32 devices in a mesh: dp: 4 (over y, x), context: 4 (over z), head: 2 (over core).
Axes of the slice: x: 2, y: 2, z: 4, core: 2. Of those that a mesh axis runs over, the one named last changes fastest.
Arguments:
- tokens: bfloat16 [4, 2, 512, 4096], P('dp', None, 'context', 'head'), may hold values from -7 to 7
- queries: bfloat16 [4, 2, 512, 2048], P('dp', None, 'context', 'head'), may hold values from -160 to 160
- grad_out: bfloat16 [4, 2, 512, 2048], P('dp', None, 'context', 'head'), may hold values from -6 to 6
- w_key: bfloat16 [4096, 256], P('context', 'head'), may hold values from -0.09375 to 0.09375
- w_value: bfloat16 [4096, 256], P('context', 'head'), may hold values from -0.09375 to 0.09375
- block_len: int32 [4], P('dp'), may hold values from 8 to 32, as said below
Outputs:
- grad_query: bfloat16 [4, 2, 512, 2048], P('dp', None, 'context', 'head')
- grad_x: bfloat16 [4, 2, 512, 4096], P('dp', None, 'context', 'head')
- grad_wkey: float32 [4096, 256], P('context', 'head')
- grad_wvalue: float32 [4096, 256], P('context', 'head')
The draws below stay inside these ranges and needn't reach their ends.
Inputs may be any that keep to these rules, and one draw needn't show every extreme that they name: `block_len`: each entry is 8, 16 or 32.
All inputs are finite; a program needn't handle non-finite values.
Results may differ from the reference program's by a relative error of at most 0.025.
Values may be sent and summed in bfloat16 or wider, within the bound.
A program may use at most 64 MiB of HBM per device.

```python
import math
import jax
import jax.numpy as jnp
from jax import lax

D = 4096
HEADS = 16
KV_HEADS = 2
HEAD_DIM = 128
CL_DEV = 128
LC = 512
REPLICAS = 4
N_CONTEXT = 4


def shared_arrays(key):
    token_key, weight_key, query_key = jax.random.split(jax.random.fold_in(key, 11), 3)
    length = CL_DEV * N_CONTEXT
    tokens = jnp.clip(jax.random.normal(token_key, (REPLICAS, 2, length, D), jnp.float32), -6.0, 6.0)
    w_key = jnp.clip(jax.random.normal(weight_key, (D, KV_HEADS * HEAD_DIM), jnp.float32), -6.0, 6.0) / math.sqrt(D)
    queries = jnp.clip(jax.random.normal(query_key, (REPLICAS, 2, length, HEADS * HEAD_DIM), jnp.float32), -6.0, 6.0)
    return (tokens, w_key, queries)


def draw_tokens(key, part):
    return shared_arrays(key)[0].astype(jnp.bfloat16)


def draw_w_key(key, part):
    return shared_arrays(key)[1].astype(jnp.bfloat16)


def draw_queries(key, part):
    return shared_arrays(key)[2].astype(jnp.bfloat16)


def draw_block_len(key, part):
    order = jax.random.permutation(jax.random.fold_in(key, 7), jnp.arange(REPLICAS, dtype=jnp.int32))
    exponent = 3 + order % 3
    return jnp.left_shift(jnp.ones((REPLICAS,), jnp.int32), exponent.astype(jnp.int32))


def level_of(own_key, dims, shards, low, top_value):
    loudness, own = 1.0, jax.random.fold_in(own_key, 6)
    for axis_at, parts in shards:
        draws = jnp.exp(jax.random.uniform(jax.random.fold_in(own, axis_at), (parts,), jnp.float32, low / len(shards), top_value / len(shards)))
        loudness = loudness * jnp.repeat(draws, dims[axis_at] // parts).reshape([-1 if axis == axis_at else 1 for axis in range(len(dims))])
    return loudness


def normal_values(key, dims, deviation, bound, cuts=(), kind=jnp.bfloat16):
    result = jax.random.normal(key, dims, jnp.float32) * deviation
    if len(cuts) > 0:
        result = level_of(key, dims, cuts, -0.22, 0.18) * result
    return jnp.clip(result, min=-bound, max=bound).astype(kind)


def setup_inputs(seed: int = 0) -> dict:
    arg_keys = jax.random.split(jax.random.key(seed), 7)
    tokens = draw_tokens(jax.random.fold_in(arg_keys[6], 71), 0)
    queries = draw_queries(jax.random.fold_in(arg_keys[6], 71), 0)
    grad_out = normal_values(arg_keys[2], (REPLICAS, 2, LC, HEADS * HEAD_DIM), 1.0, 6.0, ((0, 4), (2, 4), (3, 2)))
    w_key = draw_w_key(jax.random.fold_in(arg_keys[6], 71), 0)
    w_value = normal_values(arg_keys[4], (D, KV_HEADS * HEAD_DIM), D ** -0.5, 0.09375, ((0, 4), (1, 2)))
    block_len = draw_block_len(jax.random.fold_in(arg_keys[6], 71), 0)
    return {"tokens": tokens, "queries": queries, "grad_out": grad_out, "w_key": w_key, "w_value": w_value, "block_len": block_len}


masked_score = -1e+30

def rounded(values):
    return lax.optimization_barrier(values.astype(jnp.bfloat16)).astype(jnp.float32)

def matmul(left, right):
    return jnp.dot(left, right, precision=lax.Precision.HIGHEST)

def tile_einsum(form, left, right):
    return jnp.einsum(form, left, right, precision=lax.Precision.HIGHEST)

def one_head(q_clean, q_noisy, g_clean, g_noisy, k_clean, v_clean, k_noisy, v_noisy, block_size):
    score_scale = 1.0 / math.sqrt(HEAD_DIM)
    length = CL_DEV * N_CONTEXT
    position = jnp.arange(length, dtype=jnp.int32) // block_size
    see_clean = position[None, :] <= position[:, None]
    see_cross = position[None, :] < position[:, None]
    local_block = jnp.arange(CL_DEV, dtype=jnp.int32) // block_size
    see_own = local_block[None, :] == local_block[:, None]
    tile_shape = (N_CONTEXT, CL_DEV, HEAD_DIM)
    qn_tiles = q_noisy.reshape(tile_shape)
    gn_tiles = g_noisy.reshape(tile_shape)
    kn_tiles = k_noisy.reshape(tile_shape)
    vn_tiles = v_noisy.reshape(tile_shape)
    s_cc = jnp.where(see_clean, matmul(q_clean, k_clean.T) * score_scale, masked_score)
    s_nc = jnp.where(see_cross, matmul(q_noisy, k_clean.T) * score_scale, masked_score)
    s_nn = jnp.where(see_own, tile_einsum('tqd,tkd->tqk', qn_tiles, kn_tiles) * score_scale, masked_score)
    peak_c = lax.optimization_barrier(jnp.max(s_cc, axis=1))
    lse_c = peak_c + jnp.log(lax.optimization_barrier(jnp.sum(jnp.exp(s_cc - peak_c[:, None]), axis=1)))
    peak_n = jnp.maximum(lax.optimization_barrier(jnp.max(s_nc, axis=1)), lax.optimization_barrier(jnp.max(s_nn, axis=2)).reshape(length))
    peak_tiles = peak_n.reshape(N_CONTEXT, CL_DEV)
    total_n = lax.optimization_barrier(jnp.sum(jnp.exp(s_nc - peak_n[:, None]), axis=1))
    total_n = total_n + lax.optimization_barrier(jnp.sum(jnp.exp(s_nn - peak_tiles[:, :, None]), axis=2)).reshape(length)
    lse_n = peak_n + jnp.log(total_n)
    p_cc = jnp.exp(s_cc - lse_c[:, None])
    p_nc = jnp.exp(s_nc - lse_n[:, None])
    p_nn = jnp.exp(s_nn - lse_n.reshape(N_CONTEXT, CL_DEV)[:, :, None])
    half_cc = rounded(p_cc)
    half_nc = rounded(p_nc)
    half_nn = rounded(p_nn)
    out_c = matmul(half_cc, v_clean)
    out_n = matmul(half_nc, v_clean) + tile_einsum('tqk,tkd->tqd', half_nn, vn_tiles).reshape(length, HEAD_DIM)
    delta_c = lax.optimization_barrier(jnp.sum(g_clean * out_c, axis=1))
    delta_n = lax.optimization_barrier(jnp.sum(g_noisy * out_n, axis=1))
    ds_cc = rounded(p_cc * (matmul(g_clean, v_clean.T) - delta_c[:, None]))
    ds_nc = rounded(p_nc * (matmul(g_noisy, v_clean.T) - delta_n[:, None]))
    dp_nn = tile_einsum('tqd,tkd->tqk', gn_tiles, vn_tiles)
    ds_nn = rounded(p_nn * (dp_nn - delta_n.reshape(N_CONTEXT, CL_DEV)[:, :, None]))
    dq_c = matmul(ds_cc, k_clean) * score_scale
    dq_n = (matmul(ds_nc, k_clean) + tile_einsum('tqk,tkd->tqd', ds_nn, kn_tiles).reshape(length, HEAD_DIM)) * score_scale
    dk_c = (matmul(ds_cc.T, q_clean) + matmul(ds_nc.T, q_noisy)) * score_scale
    dv_c = matmul(half_cc.T, g_clean) + matmul(half_nc.T, g_noisy)
    dk_n = tile_einsum('tqk,tqd->tkd', ds_nn, qn_tiles).reshape(length, HEAD_DIM) * score_scale
    dv_n = tile_einsum('tqk,tqd->tkd', half_nn, gn_tiles).reshape(length, HEAD_DIM)
    return (jnp.stack([dq_c, dq_n]), jnp.stack([dk_c, dk_n]), jnp.stack([dv_c, dv_n]))

def reference(tokens, queries, grad_out, w_key, w_value, block_len):
    length = CL_DEV * N_CONTEXT
    group_size = HEADS // KV_HEADS
    flat_tokens = tokens.reshape(-1, D)
    key_flat = jnp.dot(flat_tokens, w_key, preferred_element_type=jnp.float32).astype(jnp.bfloat16)
    value_flat = jnp.dot(flat_tokens, w_value, preferred_element_type=jnp.float32).astype(jnp.bfloat16)

    def by_head(array, head_count):
        shaped = array.astype(jnp.float32).reshape(REPLICAS, 2, length, head_count, HEAD_DIM)
        return shaped.transpose(0, 3, 1, 2, 4).reshape(REPLICAS * head_count, 2, length, HEAD_DIM)
    key_heads = by_head(key_flat, KV_HEADS)
    value_heads = by_head(value_flat, KV_HEADS)
    query_heads = by_head(queries, HEADS)
    grad_heads = by_head(grad_out, HEADS)
    items = jnp.arange(REPLICAS * HEADS, dtype=jnp.int32)

    def run_item(index):
        replica = index // HEADS
        kv_index = replica * KV_HEADS + index % HEADS // group_size
        q_head = query_heads[index]
        g_head = grad_heads[index]
        k_head = key_heads[kv_index]
        v_head = value_heads[kv_index]
        return one_head(q_head[0], q_head[1], g_head[0], g_head[1], k_head[0], v_head[0], k_head[1], v_head[1], block_len[replica])
    dq_items, dk_items, dv_items = lax.map(run_item, items)
    grad_query = dq_items.reshape(REPLICAS, HEADS, 2, length, HEAD_DIM).transpose(0, 2, 3, 1, 4)
    grad_query = grad_query.reshape(REPLICAS, 2, length, HEADS * HEAD_DIM).astype(jnp.bfloat16)

    def group_sum(items_grad):
        summed = items_grad.reshape(REPLICAS, KV_HEADS, group_size, 2, length, HEAD_DIM).sum(axis=2)
        summed = summed.transpose(0, 2, 3, 1, 4).reshape(REPLICAS * 2 * length, KV_HEADS * HEAD_DIM)
        return summed.astype(jnp.bfloat16)
    grad_key = group_sum(dk_items)
    grad_value = group_sum(dv_items)
    grad_x = jnp.dot(grad_key, w_key.T, preferred_element_type=jnp.float32)
    grad_x = grad_x + jnp.dot(grad_value, w_value.T, preferred_element_type=jnp.float32)
    grad_x = grad_x.astype(jnp.bfloat16).reshape(tokens.shape)
    grad_wkey = jnp.dot(flat_tokens.T, grad_key, preferred_element_type=jnp.float32)
    grad_wvalue = jnp.dot(flat_tokens.T, grad_value, preferred_element_type=jnp.float32)
    return (grad_query, grad_x, grad_wkey, grad_wvalue)
```

```python
import functools
import math

import jax
import jax.numpy as jnp
from jax import lax
from jax.experimental import pallas as pl
from jax.experimental.pallas import tpu as pltpu
from jax.sharding import PartitionSpec as P

HEAD_DIM = 128
MASKED = -1e30
VMEM_LIMIT = 56 * 1024 * 1024
MESH = pl.DeviceIdType.MESH
NT = (((1,), (1,)), ((), ()))


def near_first(count):
    order = []
    for step in range(1, count):
        for offset in (step, count - step):
            if offset not in order:
                order.append(offset)
    return order


def line_order(me, n):
    low, high = me, n - 1 - me
    both = jnp.minimum(low, high)
    longer = jnp.where(low < high, 1, -1)
    order = []
    for k in range(1, n):
        near_side = 1 if k % 2 else -1
        peer = jnp.where(k <= 2 * both, me + near_side * ((k + 1) // 2), me + longer * (k - both))
        order.append((k, peer))
    return order


def dot(left, right):
    return jnp.dot(left, right, preferred_element_type=jnp.float32)


def dot_nt(left, right):
    return lax.dot_general(left, right, NT, preferred_element_type=jnp.float32)


def fused_kernel(
    n, m, share, early,
    blk_ref, tok_ref, qin_ref, gin_ref, wk_ref, wv_ref,
    dq_ref, gx_ref, gwk_ref, gwv_ref,
    q_ref, g_ref, tokf, wf, wo, kv, kvn, kt, knt, dkv, dn, pgp, pin, pga, pgo, tokd, gsum, rp, rin, rall,
    loc_sem, tok_sem, wz_s, wz_r, wd_s, wd_r, wx_s, wx_r, wo_sem, kv_s, kv_r,
    td_s, td_r, tf_s, tf_r, pp_s, pp_r, pn_s, pn_r, pc_s, pc_r, po_sem, rs_s, rs_r, ra_s, ra_r,
):
    me_dp = lax.axis_index("dp")
    me = lax.axis_index("context")
    head = lax.axis_index("head")
    other = 1 - head
    rows2, features = tok_ref.shape
    rows = rows2 // 2
    wrows = wk_ref.shape[0]
    half = n // 2
    score_scale = 1.0 / math.sqrt(HEAD_DIM)
    sends = []

    def copy_of(src, dst, send_sem, recv_sem, **device):
        return pltpu.make_async_remote_copy(
            src_ref=src, dst_ref=dst, send_sem=send_sem, recv_sem=recv_sem,
            device_id=device, device_id_type=MESH,
        )

    def put(src, dst, send_sem, recv_sem, **device):
        copy = copy_of(src, dst, send_sem, recv_sem, **device)
        copy.start()
        sends.append((None, copy))

    def put_if(condition, src, dst, send_sem, recv_sem, **device):
        copy = copy_of(src, dst, send_sem, recv_sem, **device)
        pl.when(condition)(copy.start)
        sends.append((condition, copy))

    def arrived(dst, send_sem, recv_sem):
        copy_of(dst, dst, send_sem, recv_sem, head=other).wait_recv()

    near = line_order(me, n)
    far = near[::-1]
    dp_peers = [(off, lax.rem(me_dp + off, m)) for off in near_first(m)]

    two_step = m == 4 and share % 32 == 0
    if two_step:
        low = lax.rem(me_dp, 2)
        w_peers = [(0, me_dp + 1 - 2 * low), (1, lax.rem(me_dp + 2, 4))]
    else:
        w_peers = [(at, peer) for at, (_, peer) in enumerate(dp_peers)]

    own_copies = [
        pltpu.make_async_copy(wk_ref, wf.at[me, :, pl.ds(0, HEAD_DIM)], loc_sem.at[0]),
        pltpu.make_async_copy(wv_ref, wf.at[me, :, pl.ds(HEAD_DIM, HEAD_DIM)], loc_sem.at[1]),
        pltpu.make_async_copy(tok_ref, tokf.at[head], loc_sem.at[2]),
        pltpu.make_async_copy(qin_ref, q_ref, loc_sem.at[4]),
        pltpu.make_async_copy(gin_ref, g_ref, loc_sem.at[5]),
    ]
    for copy in own_copies:
        copy.start()

    barrier = pltpu.get_barrier_semaphore()
    for _, peer in near:
        pl.semaphore_signal(barrier, inc=1, device_id={"context": peer}, device_id_type=MESH)
    for _, peer in dp_peers:
        pl.semaphore_signal(barrier, inc=1, device_id={"dp": peer}, device_id_type=MESH)
    pl.semaphore_signal(barrier, inc=1, device_id={"head": other}, device_id_type=MESH)
    pl.semaphore_wait(barrier, n + m - 1)

    shared_base = pl.multiple_of(me_dp * share, 16)
    chunks = 2 if two_step else 1
    piece_rows = share // chunks

    def w_piece(owner, base, chunk):
        return wf.at[owner, pl.ds(pl.multiple_of(base + chunk * piece_rows, 16), piece_rows)]

    direct_rows = wrows - m * share
    direct = pl.ds(m * share, direct_rows)
    own_copies[0].wait()
    own_copies[1].wait()
    for chunk in range(chunks):
        part = w_piece(me, shared_base, chunk)
        for side in (1, -1):
            peer = me + side
            put_if(
                (peer >= 0) & (peer < n), part, part,
                wz_s.at[0, chunk, (side + 1) // 2], wz_r.at[me, chunk], context=peer,
            )
    own_copies[2].wait()
    put(tokf.at[head], tokf.at[head], tok_sem.at[0], tok_sem.at[1], head=other)
    if direct_rows:
        for k, peer in near:
            part = wf.at[me, direct]
            put(part, part, wd_s.at[k], wd_r.at[me], context=peer)

    def token_block(owner):
        column = pl.multiple_of(lax.rem(owner, half) * wrows, 128)
        return owner // half, pl.ds(column, wrows)

    def token_rows(core, part):
        start = 0 if part == 0 else early
        count = early if part == 0 else rows - early
        return pl.ds(pl.multiple_of(core * rows + start, 16), count)

    def token_copy(part, off, peer):
        span = token_rows(head, part)
        side, columns = token_block(peer)
        return copy_of(
            tokf.at[side, span, columns], tokd.at[me, span],
            td_s.at[part, off], td_r.at[part, me], context=peer,
        )

    my_side, my_columns = token_block(me)
    def w_forward(src):
        for dp_at, peer in w_peers:
            base = peer * share
            part = w_piece(src, base, dp_at)
            arrived(part, wx_s.at[src, dp_at, dp_at], wx_r.at[src, dp_at, dp_at])
            to = w_peers[1 - dp_at][1]
            put(part, part, wx_s.at[src, 2, dp_at], wx_r.at[src, 2, dp_at], dp=to)

    for k, src in near:
        onward = jnp.where(src > me, me - 1, me + 1)
        for chunk in range(chunks):
            part = w_piece(src, shared_base, chunk)
            arrived(part, wz_s.at[k, chunk, 0], wz_r.at[src, chunk])
            put_if(
                (onward >= 0) & (onward < n), part, part,
                wz_s.at[k, chunk, 0], wz_r.at[src, chunk], context=onward,
            )
            for dp_at, peer in w_peers:
                put(part, part, wx_s.at[src, dp_at, chunk], wx_r.at[src, dp_at, chunk], dp=peer)
        if two_step and k > 1:
            w_forward(near[k - 2][1])
    arrived(tokf.at[other], tok_sem.at[0], tok_sem.at[1])
    for k, peer in far:
        copy = token_copy(0, k, peer)
        copy.start()
        sends.append((None, copy))
    for k, peer in far:
        copy = token_copy(1, k, peer)
        pl.when(peer < me)(copy.start)
        sends.append((None, copy))
    own_tokens = pltpu.make_async_copy(tokf.at[my_side, :, my_columns], tokd.at[me], loc_sem.at[3])
    own_tokens.start()
    if two_step:
        w_forward(near[-1][1])

    projected = dot(tokf[my_side, :, my_columns], wf[me])
    for k, src in near:
        if direct_rows:
            arrived(wf.at[src, direct], wd_s.at[k], wd_r.at[src])
        if two_step:
            for dp_at, peer in w_peers:
                part = w_piece(src, peer * share, 1 - dp_at)
                arrived(part, wx_s.at[src, dp_at, 1 - dp_at], wx_r.at[src, dp_at, 1 - dp_at])
                part = w_piece(src, (3 - me_dp) * share, dp_at)
                arrived(part, wx_s.at[src, 2, dp_at], wx_r.at[src, 2, dp_at])
        else:
            for dp_at, peer in w_peers:
                origin = lax.rem(me_dp + m - dp_peers[dp_at][0], m)
                part = w_piece(src, origin * share, 0)
                arrived(part, wx_s.at[src, dp_at, 0], wx_r.at[src, dp_at, 0])
        side, columns = token_block(src)
        projected += dot(tokf[side, :, columns], wf[src])
    pairs = projected.astype(jnp.bfloat16)
    my_rows = pl.ds(pl.multiple_of(me * rows, rows), rows)
    kv[my_rows, :] = pairs[:rows]
    kvn[...] = pairs[rows:]
    for k, peer in far:
        put_if(peer > me, kv.at[my_rows], kv.at[my_rows], kv_s.at[k], kv_r.at[me], context=peer)
    put(wf.at[pl.ds(other * half, half)], wo, wo_sem.at[0], wo_sem.at[1], head=other)

    block = blk_ref[0]
    total_rows = n * rows
    lane = lax.broadcasted_iota(jnp.int32, (1, rows2), 1)
    noisy_lane = lane >= rows
    position = me * rows + jnp.where(noisy_lane, lane - rows, lane)
    block_start = position & (-block)
    limit = jnp.where(noisy_lane, block_start, block_start + block)
    dkv[...] = jnp.zeros_like(dkv)
    dn[...] = jnp.zeros_like(dn)
    knt[...] = kvn[:, :HEAD_DIM].T
    own_copies[3].wait()
    own_copies[4].wait()
    for k, src in near:
        span = pl.ds(pl.multiple_of(src * rows, rows), rows)

        @pl.when(src < me)
        def _(span=span, k=k, src=src):
            arrived(kv.at[span], kv_s.at[k], kv_r.at[src])

        @pl.when(src > me)
        def _(span=span):
            kv[span, :] = jnp.zeros((rows, 2 * HEAD_DIM), jnp.bfloat16)
    for k, peer in far:
        pl.when(peer > me)(token_copy(1, k, peer).start)
    kt[...] = kv[:, :HEAD_DIM].T

    def head_turn(turn, carry):
        columns = pl.ds(pl.multiple_of(turn * HEAD_DIM, HEAD_DIM), HEAD_DIM)
        q = q_ref[:, columns]
        g = g_ref[:, columns]
        keys = kv[:, :HEAD_DIM]
        values = kv[:, HEAD_DIM:]
        own_keys = kvn[:, :HEAD_DIM]
        own_values = kvn[:, HEAD_DIM:]
        key_pos = lax.broadcasted_iota(jnp.int32, (total_rows, rows2), 0)
        near = lax.broadcasted_iota(jnp.int32, (rows, rows), 0)
        same = (near ^ lax.broadcasted_iota(jnp.int32, (rows, rows), 1)) < block
        s = jnp.where(key_pos < limit, dot_nt(keys, q) * score_scale, MASKED)
        s_own = jnp.where(same, dot_nt(own_keys, q[rows:]) * score_scale, MASKED)
        peak = jnp.max(s, axis=0, keepdims=True)
        peak_own = jnp.maximum(peak[:, rows:], jnp.max(s_own, axis=0, keepdims=True))
        peak = jnp.concatenate([peak[:, :rows], peak_own], axis=1)
        e = jnp.exp(s - peak)
        e_own = jnp.exp(s_own - peak_own)
        total = jnp.sum(e, axis=0, keepdims=True)
        total_own = total[:, rows:] + jnp.sum(e_own, axis=0, keepdims=True)
        inverse = 1.0 / jnp.concatenate([total[:, :rows], total_own], axis=1)
        p = e * inverse
        p_own = e_own * inverse[:, rows:]
        p_half = p.astype(jnp.bfloat16)
        p_half_own = p_own.astype(jnp.bfloat16)
        gp = dot_nt(values, g)
        gp_own = dot_nt(own_values, g[rows:])
        delta = jnp.sum(p_half.astype(jnp.float32) * gp, axis=0, keepdims=True)
        delta_own = delta[:, rows:] + jnp.sum(
            p_half_own.astype(jnp.float32) * gp_own, axis=0, keepdims=True
        )
        delta = jnp.concatenate([delta[:, :rows], delta_own], axis=1)
        ds = (p * (gp - delta)).astype(jnp.bfloat16)
        ds_own = (p_own * (gp_own - delta_own)).astype(jnp.bfloat16)
        dkv[:, :HEAD_DIM] += dot(ds, q)
        dkv[:, HEAD_DIM:] += dot(p_half, g)
        dn[:, :HEAD_DIM] += dot(ds_own, q[rows:])
        dn[:, HEAD_DIM:] += dot(p_half_own, g[rows:])
        dq = dot(kt[...], ds)
        dq_own = dq[:, rows:] + dot(knt[...], ds_own)
        dq_ref[:rows, columns] = (dq[:, :rows] * score_scale).T.astype(jnp.bfloat16)
        dq_ref[rows:, columns] = (dq_own * score_scale).T.astype(jnp.bfloat16)
        return carry

    lax.fori_loop(0, q_ref.shape[1] // HEAD_DIM, head_turn, 0)

    pair_scale = jnp.where(
        lax.broadcasted_iota(jnp.int32, (1, 2 * HEAD_DIM), 1) < HEAD_DIM, score_scale, 1.0
    )
    for block_at in range(n):
        pgp[block_at] = (dkv[block_at * rows : (block_at + 1) * rows] * pair_scale).astype(jnp.bfloat16)
    clean, noisy = pl.ds(0, rows), pl.ds(rows, rows)
    for k, peer in far:
        put_if(peer < me, pgp.at[peer], pin.at[me], pp_s.at[k], pp_r.at[me], context=peer)
    pga[me, noisy] = (dn[...] * pair_scale).astype(jnp.bfloat16)
    part = pga.at[me, noisy]

    def noisy_copy(k, peer):
        return copy_of(part, part, pn_s.at[k], pn_r.at[me], context=peer)

    for k, peer in far:
        copy = noisy_copy(k, peer)
        pl.when(peer > me)(copy.start)
        sends.append((None, copy))
    put(part, pgo.at[noisy], po_sem.at[0], po_sem.at[1], head=other)
    dkv[my_rows, :] *= pair_scale

    def token_onward(k, src, piece):
        span = token_rows(head, piece)
        held = tokd.at[src, span]
        arrived(held, td_s.at[piece, k], td_r.at[piece, src])
        copy = copy_of(held, held, tf_s.at[piece, k], tf_r.at[piece, src], head=other)
        copy.start()

    for k, src in near:
        token_onward(k, src, 0)
        sends.append((None, copy_of(
            tokd.at[src, token_rows(head, 0)], tokd.at[src, token_rows(head, 0)],
            tf_s.at[0, k], tf_r.at[0, src], head=other,
        )))
    for k, src in near:

        @pl.when(src > me)
        def _(k=k, src=src):
            arrived(pin.at[src], pp_s.at[k], pp_r.at[src])
            dkv[my_rows, :] += pin[src].astype(jnp.float32)

    pga[me, clean] = dkv[my_rows, :].astype(jnp.bfloat16)
    whole = pga.at[me, clean]
    for k, peer in far:
        put(whole, whole, pc_s.at[k], pc_r.at[me], context=peer)
    for k, peer in far:
        pl.when(peer < me)(noisy_copy(k, peer).start)
    put(whole, pgo.at[clean], po_sem.at[2], po_sem.at[3], head=other)

    for k, src in near:
        token_onward(k, src, 1)
        sends.append((None, copy_of(
            tokd.at[src, token_rows(head, 1)], tokd.at[src, token_rows(head, 1)],
            tf_s.at[1, k], tf_r.at[1, src], head=other,
        )))
    own_tokens.wait()
    arrived(wo, wo_sem.at[0], wo_sem.at[1])
    arrived(pgo.at[noisy], po_sem.at[0], po_sem.at[1])
    arrived(pgo.at[clean], po_sem.at[2], po_sem.at[3])

    for at in range(half):
        gx_ref[:, at * wrows : (at + 1) * wrows] = (
            dot_nt(pga[me], wf[head * half + at]) + dot_nt(pgo[...], wo[at])
        ).astype(jnp.bfloat16)

    gw = dot(pga[me].T, tokd[me])
    for k, src in near:
        for piece in range(2):
            span = token_rows(other, piece)
            arrived(tokd.at[src, span], tf_s.at[piece, k], tf_r.at[piece, src])
        arrived(pga.at[src, noisy], pn_s.at[k], pn_r.at[src])
        arrived(pga.at[src, clean], pc_s.at[k], pc_r.at[src])
        gw += dot(pga[src].T, tokd[src])

    slab = gw.shape[0] // m
    for at in range(m):
        gsum[at] = gw[at * slab : (at + 1) * slab]
        rp[at] = gw[at * slab : (at + 1) * slab].astype(jnp.bfloat16)
    for off, peer in dp_peers:
        put(rp.at[peer], rin.at[me_dp], rs_s.at[off], rs_r.at[me_dp], dp=peer)
    slab_sum = gsum[me_dp]
    for off, src in dp_peers:
        arrived(rin.at[src], rs_s.at[off], rs_r.at[src])
        slab_sum += rin[src].astype(jnp.float32)
    rall[me_dp] = slab_sum.astype(jnp.bfloat16)
    for off, peer in dp_peers:
        put(rall.at[me_dp], rall.at[me_dp], ra_s.at[off], ra_r.at[me_dp], dp=peer)
    for off, src in dp_peers:
        arrived(rall.at[src], ra_s.at[off], ra_r.at[src])
    for at in range(m):
        gsum[at] = rall[at].astype(jnp.float32)
    gwk_ref[...] = gsum[: m // 2].reshape(HEAD_DIM, wrows).T
    gwv_ref[...] = gsum[m // 2 :].reshape(HEAD_DIM, wrows).T
    for condition, copy in sends:
        if condition is None:
            copy.wait_send()
        else:
            pl.when(condition)(copy.wait_send)


def store_kernel(dq_in, gx_in, gwk_in, gwv_in, dq_out, gx_out, gwk_out, gwv_out, sem):
    pairs = ((gx_in, gx_out), (dq_in, dq_out), (gwk_in, gwk_out), (gwv_in, gwv_out))
    copies = [pltpu.make_async_copy(src, dst, sem.at[at]) for at, (src, dst) in enumerate(pairs)]
    for copy in copies:
        copy.start()
    for copy in copies:
        copy.wait()


def per_device(tokens, queries, grad_out, w_key, w_value, block_len):
    n = lax.axis_size("context")
    m = lax.axis_size("dp")
    rows = tokens.shape[2]
    features = tokens.shape[3]
    wrows, width = w_key.shape
    q_width = queries.shape[3]
    share = wrows // m // 16 * 16
    early = max(16, rows // 64 * 16)
    half = n // 2
    pair = 2 * width
    bf16, f32 = jnp.bfloat16, jnp.float32
    vmem = pl.BlockSpec(memory_space=pltpu.VMEM)
    dma = pltpu.SemaphoreType.DMA
    hbm = pl.BlockSpec(memory_space=pltpu.HBM)
    slab = pair // m
    results = (
        ((2 * rows, q_width), bf16),
        ((2 * rows, features), bf16),
        ((wrows, width), f32),
        ((wrows, width), f32),
    )
    dq, gx, gwk, gwv = pl.pallas_call(
        functools.partial(fused_kernel, n, m, share, early),
        out_shape=tuple(pltpu.VMEM(*result) for result in results),
        in_specs=[pl.BlockSpec(memory_space=pltpu.SMEM)] + [hbm] * 5,
        out_specs=(vmem, vmem, vmem, vmem),
        scratch_shapes=[
            pltpu.VMEM((2 * rows, q_width), bf16),
            pltpu.VMEM((2 * rows, q_width), bf16),
            pltpu.VMEM((2, 2 * rows, features), bf16),
            pltpu.VMEM((n, wrows, pair), bf16),
            pltpu.VMEM((half, wrows, pair), bf16),
            pltpu.VMEM((n * rows, pair), bf16),
            pltpu.VMEM((rows, pair), bf16),
            pltpu.VMEM((width, n * rows), bf16),
            pltpu.VMEM((width, rows), bf16),
            pltpu.VMEM((n * rows, pair), f32),
            pltpu.VMEM((rows, pair), f32),
            pltpu.VMEM((n, rows, pair), bf16),
            pltpu.VMEM((n, rows, pair), bf16),
            pltpu.VMEM((n, 2 * rows, pair), bf16),
            pltpu.VMEM((2 * rows, pair), bf16),
            pltpu.VMEM((n, 2 * rows, wrows), bf16),
            pltpu.VMEM((m, slab, wrows), f32),
            pltpu.VMEM((m, slab, wrows), bf16),
            pltpu.VMEM((m, slab, wrows), bf16),
            pltpu.VMEM((m, slab, wrows), bf16),
            dma((6,)), dma((2,)), dma((n, 2, 2)), dma((n, 2)), dma((n,)), dma((n,)),
            dma((n, m, 2)), dma((n, m, 2)), dma((2,)), dma((n,)), dma((n,)),
            dma((2, n)), dma((2, n)), dma((2, n)), dma((2, n)),
            dma((n,)), dma((n,)), dma((n,)), dma((n,)), dma((n,)), dma((n,)),
            dma((4,)), dma((m,)), dma((m,)), dma((m,)), dma((m,)),
        ],
        compiler_params=pltpu.CompilerParams(
            collective_id=0, has_side_effects=True, vmem_limit_bytes=VMEM_LIMIT
        ),
    )(
        block_len,
        tokens.reshape(2 * rows, features),
        queries.reshape(2 * rows, q_width),
        grad_out.reshape(2 * rows, q_width),
        w_key,
        w_value,
    )
    dq, gx, gwk, gwv = pl.pallas_call(
        store_kernel,
        out_shape=tuple(jax.ShapeDtypeStruct(*result) for result in results),
        in_specs=[vmem] * 4,
        out_specs=(hbm, hbm, hbm, hbm),
        scratch_shapes=[dma((4,))],
    )(*(pltpu.with_memory_space_constraint(x, pltpu.VMEM) for x in (dq, gx, gwk, gwv)))
    return (
        dq.reshape(queries.shape),
        gx.reshape(tokens.shape),
        gwk,
        gwv,
    )


def solution(mesh):
    placed = (
        P("dp", None, "context", "head"),
        P("dp", None, "context", "head"),
        P("dp", None, "context", "head"),
        P("context", "head"),
        P("context", "head"),
        P("dp"),
    )
    return jax.shard_map(
        per_device,
        mesh=mesh,
        in_specs=placed,
        out_specs=(
            P("dp", None, "context", "head"),
            P("dp", None, "context", "head"),
            P("context", "head"),
            P("context", "head"),
        ),
        check_vma=False,
    )
```

```python
import functools
import math

import jax
import jax.numpy as jnp
from jax import lax
from jax.experimental import pallas as pl
from jax.experimental.pallas import tpu as pltpu
from jax.sharding import PartitionSpec as P

HEAD_DIM = 128
MASKED = -1e30
VMEM_LIMIT = 56 * 1024 * 1024
MESH = pl.DeviceIdType.MESH
NT = (((1,), (1,)), ((), ()))


def line_order(me, n):
    low, high = me, n - 1 - me
    both = jnp.minimum(low, high)
    longer = jnp.where(low < high, 1, -1)
    order = []
    for k in range(1, n):
        near_side = 1 if k % 2 else -1
        peer = jnp.where(k <= 2 * both, me + near_side * ((k + 1) // 2), me + longer * (k - both))
        order.append((k, peer))
    return order


def dot(left, right):
    return jnp.dot(left, right, preferred_element_type=jnp.float32)


def dot_nt(left, right):
    return lax.dot_general(left, right, NT, preferred_element_type=jnp.float32)


def fused_kernel(
    n, m, share,
    blk_ref, tok_ref, q_in, g_in, wk_ref, wv_ref,
    dq_ref, gx_ref, gwk_ref, gwv_ref,
    qg, tokf, wf, wo, kv, kvn, kt, knt, dkv, dn, pgp, pin, pga, pgo, tokd, tokn,
    gsum, rp, rin, rall, fp, fin, foreign_own, zout, zin,
    loc_sem, pair_sem, kv_credit, pin_credit, tok_sem, wz_s, wz_r, wd_s, wd_r, wx_s, wx_r, wo_sem, kv_s, kv_r,
    t1_s, t1_r, f1_s, f1_r, t2_s, t2_r, f2_s, f2_r, pp_s, pp_r, pg_s, pn_r, pc_r, po_sem,
    rf_s, rf_r, z_sem, rs_s, rs_r, ra_s, ra_r,
):
    me_dp = lax.axis_index("dp")
    me = lax.axis_index("context")
    head = lax.axis_index("head")
    other = 1 - head
    rows2, features = tok_ref.shape
    rows = rows2 // 2
    wrows = wk_ref.shape[0]
    half = n // 2
    score_scale = 1.0 / math.sqrt(HEAD_DIM)
    drains = []

    def copy_of(src, dst, send_sem, recv_sem, **device):
        return pltpu.make_async_remote_copy(
            src_ref=src, dst_ref=dst, send_sem=send_sem, recv_sem=recv_sem,
            device_id=device, device_id_type=MESH,
        )

    def put(src, dst, send_sem, recv_sem, **device):
        copy_of(src, dst, send_sem, recv_sem, **device).start()

    def put_if(condition, src, dst, send_sem, recv_sem, **device):
        pl.when(condition)(copy_of(src, dst, send_sem, recv_sem, **device).start)

    def arrived(dst, recv_sem):
        copy_of(dst, dst, loc_sem.at[0], recv_sem, head=other).wait_recv()

    def drain(whole, send_sem, condition=None):
        drains.append((condition, copy_of(whole, whole, send_sem, loc_sem.at[0], head=other)))

    def slot(src, dst):
        return lax.rem(src - dst + n - 1, n)

    def inside(place):
        return (place >= 0) & (place < n)

    def dp_slot(src, dst):
        return lax.rem(src - dst + m - 1, m)

    near = line_order(me, n)
    far = near[::-1]
    sides = (me + 1, me - 1)
    dp_peers = [lax.rem(me_dp + off, m) for off in range(1, m)]

    two_step = m == 4 and share % 32 == 0
    if two_step:
        low = lax.rem(me_dp, 2)
        w_peers = [(0, me_dp + 1 - 2 * low), (1, lax.rem(me_dp + 2, 4))]
    else:
        w_peers = list(enumerate(dp_peers))

    w_copies = [
        pltpu.make_async_copy(wk_ref, wf.at[me, :, pl.ds(0, HEAD_DIM)], loc_sem.at[0]),
        pltpu.make_async_copy(wv_ref, wf.at[me, :, pl.ds(HEAD_DIM, HEAD_DIM)], loc_sem.at[0]),
    ]
    own_half = pltpu.make_async_copy(tok_ref, tokf.at[head], loc_sem.at[1])
    row_copies = [
        pltpu.make_async_copy(q_in, qg.at[0], loc_sem.at[2]),
        pltpu.make_async_copy(g_in, qg.at[1], loc_sem.at[2]),
    ]
    for copy in w_copies + [own_half] + row_copies:
        copy.start()
    barrier = pltpu.get_barrier_semaphore()
    for _, peer in near:
        pl.semaphore_signal(barrier, inc=1, device_id={"context": peer}, device_id_type=MESH)
    for peer in dp_peers:
        pl.semaphore_signal(barrier, inc=1, device_id={"dp": peer}, device_id_type=MESH)
    pl.semaphore_signal(barrier, inc=1, device_id={"head": other}, device_id_type=MESH)
    pl.semaphore_wait(barrier, n + m - 1)

    def cores_meet():
        pl.semaphore_signal(pair_sem, inc=1, device_id={"head": other}, device_id_type=MESH)
        pl.semaphore_wait(pair_sem, 1)

    shared_base = pl.multiple_of(me_dp * share, 16)
    chunks = 2 if two_step else 1
    piece_rows = share // chunks

    def w_piece(owner, base, chunk):
        return wf.at[owner, pl.ds(pl.multiple_of(base + chunk * piece_rows, 16), piece_rows)]

    direct_rows = wrows - m * share
    direct = pl.ds(m * share, direct_rows)
    pltpu.make_async_copy(wf.at[me], wf.at[me], loc_sem.at[0]).wait()
    share_rows = wf.at[0, pl.ds(0, share)]
    for chunk in range(chunks):
        part = w_piece(me, shared_base, chunk)
        for at, peer in enumerate(sides):
            put_if(inside(peer), part, part, wz_s.at[at], wz_r.at[slot(me, peer), chunk], context=peer)
    for at, peer in enumerate(sides):
        drain(share_rows, wz_s.at[at], inside(peer))
    own_half.wait()
    put(tokf.at[head], tokf.at[head], tok_sem.at[0], tok_sem.at[1], head=other)
    drain(tokf.at[head], tok_sem.at[0])
    if direct_rows:
        for k, peer in near:
            part = wf.at[me, direct]
            put(part, part, wd_s.at[k - 1], wd_r.at[slot(me, peer)], context=peer)
            drain(part, wd_s.at[k - 1])

    def token_block(owner):
        column = pl.multiple_of(lax.rem(owner, half) * wrows, 128)
        return owner // half, pl.ds(column, wrows)

    quarter = rows // 4
    base = me // half * half
    place = me - base
    mates = [base + lax.rem(place + k, half) for k in range(1, half)]
    cross = [jnp.where(me < half, half + k, half - 1 - k) for k in range(half)]
    partner = lax.rem(me + half, n)
    outer = (me == 0) | (me == n - 1)
    inner = (me > 0) & (me < n - 1)

    def mate_slot(src, dst):
        return lax.rem(src - dst + half - 1, half)

    def cross_rows(core, part):
        return pl.ds(pl.multiple_of(core * 2 * quarter + part * quarter, 16), quarter)

    def mate_rows(core, part):
        if part == 0:
            return pl.ds(pl.multiple_of(core * rows, 16), rows)
        return pl.ds(pl.multiple_of(core * 2 * quarter, 16), 2 * quarter)

    def cross_copy(part, peer):
        span = cross_rows(head, part)
        side, columns = token_block(peer)
        return copy_of(
            tokf.at[side, span, columns], tokd.at[me, span],
            t1_s.at[part], t1_r.at[part, lax.rem(me, half)], context=peer,
        )

    def mate_copy(part, peer):
        if part == 0:
            side, columns = token_block(peer)
            span = mate_rows(head, 0)
            held = tokd.at[me, span]
        else:
            side, columns = token_block(lax.rem(peer + half, n))
            span = pl.ds(pl.multiple_of(rows + head * 2 * quarter, 16), 2 * quarter)
            held = tokn.at[place, mate_rows(head, 1)]
        return copy_of(
            tokf.at[side, span, columns], held,
            t2_s.at[part], t2_r.at[part, mate_slot(me, peer)], context=peer,
        )

    my_side, my_columns = token_block(me)

    def w_forward(src):
        for dp_at, peer in w_peers:
            part = w_piece(src, peer * share, dp_at)
            arrived(part, wx_r.at[slot(src, me), 2 * dp_at + dp_at])
            to = w_peers[1 - dp_at][1]
            put(part, part, wx_s.at[slot(src, me)], wx_r.at[slot(src, me), 4 + dp_at], dp=to)

    for k, src in near:
        onward = jnp.where(src > me, me - 1, me + 1)
        for chunk in range(chunks):
            part = w_piece(src, shared_base, chunk)
            arrived(part, wz_r.at[slot(src, me), chunk])
            put_if(inside(onward), part, part, wz_s.at[1 + k], wz_r.at[slot(src, onward), chunk], context=onward)
            for dp_at, peer in w_peers:
                put(part, part, wx_s.at[slot(src, me)], wx_r.at[slot(src, me), chunks * dp_at + chunk], dp=peer)
        drain(share_rows, wz_s.at[1 + k], inside(onward))
        drain(wf.at[0, pl.ds(0, (m - 1) * share)], wx_s.at[slot(src, me)])
        if k == 1:
            arrived(tokf.at[other], tok_sem.at[1])
            for peer in mates:
                for part in range(2):
                    pl.when(outer)(mate_copy(part, peer).start)
        if two_step and k > 1:
            w_forward(near[k - 2][1])
    cores_meet()
    for peer in cross[::-1]:
        cross_copy(0, peer).start()
    for peer in cross[::-1]:
        pl.when(peer < me)(cross_copy(1, peer).start)
    for peer in mates:
        pl.when(inner)(mate_copy(1, peer).start)
        pl.when((peer < me) & inner)(mate_copy(0, peer).start)
    own_tokens = pltpu.make_async_copy(tokf.at[my_side, :, my_columns], tokd.at[me], loc_sem.at[3])
    own_tokens.start()
    for part in range(2):
        held = tokd.at[pl.ds(0, half), pl.ds(0, quarter)]
        drain(held, t1_s.at[part])
        drain(held, f1_s.at[part])
    for part, held in enumerate((tokd.at[pl.ds(0, half - 1), pl.ds(0, rows)], tokn.at[pl.ds(0, half - 1), pl.ds(0, 2 * quarter)])):
        drain(held, t2_s.at[part])
        drain(held, f2_s.at[part])
    if two_step:
        w_forward(near[-1][1])

    projected = dot(tokf[my_side, :, my_columns], wf[me])
    for k, src in near:
        if direct_rows:
            arrived(wf.at[src, direct], wd_r.at[slot(src, me)])
        if two_step:
            for dp_at, peer in w_peers:
                part = w_piece(src, peer * share, 1 - dp_at)
                arrived(part, wx_r.at[slot(src, me), 2 * dp_at + 1 - dp_at])
                part = w_piece(src, (3 - me_dp) * share, dp_at)
                arrived(part, wx_r.at[slot(src, me), 4 + dp_at])
        else:
            for off in range(1, m):
                part = w_piece(src, lax.rem(me_dp + m - off, m) * share, 0)
                arrived(part, wx_r.at[slot(src, me), off - 1])
        side, columns = token_block(src)
        projected += dot(tokf[side, :, columns], wf[src])
    pairs = projected.astype(jnp.bfloat16)
    my_rows = pl.ds(pl.multiple_of(me * rows, rows), rows)
    kv[my_rows, :] = pairs[:rows]
    kvn[...] = pairs[rows:]
    for k, peer in far:
        put_if(peer > me, kv.at[my_rows], kv.at[my_rows], kv_s.at[k - 1], kv_r.at[slot(me, peer)], context=peer)
        drain(kv.at[my_rows], kv_s.at[k - 1], peer > me)
    put(wf.at[pl.ds(other * half, half)], wo, wo_sem.at[0], wo_sem.at[1], head=other)
    drain(wo, wo_sem.at[0])

    block = blk_ref[0]
    total_rows = n * rows
    lane = lax.broadcasted_iota(jnp.int32, (1, rows2), 1)
    noisy_lane = lane >= rows
    position = me * rows + jnp.where(noisy_lane, lane - rows, lane)
    block_start = position & (-block)
    limit = jnp.where(noisy_lane, block_start, block_start + block)
    dkv[...] = jnp.zeros_like(dkv)
    dn[...] = jnp.zeros_like(dn)
    knt[...] = kvn[:, :HEAD_DIM].T
    pltpu.make_async_copy(qg, qg, loc_sem.at[2]).wait()
    for k, src in near:
        span = pl.ds(pl.multiple_of(src * rows, rows), rows)

        @pl.when(src < me)
        def _(span=span, src=src):
            arrived(kv.at[span], kv_r.at[slot(src, me)])

        @pl.when(src > me)
        def _(span=span):
            kv[span, :] = jnp.zeros((rows, 2 * HEAD_DIM), jnp.bfloat16)
    for _, peer in near:

        @pl.when(peer < me)
        def _(peer=peer):
            pl.semaphore_signal(kv_credit, inc=1, device_id={"context": peer}, device_id_type=MESH)

    kt[...] = kv[:, :HEAD_DIM].T

    steps = 4 if n % 4 == 0 else 1
    step_rows = total_rows // steps

    def head_turns(first, last):
        for step in range(steps):

            @pl.when(me // (n // steps) == step)
            def _(step=step):
                turn_of = functools.partial(head_turn, (step + 1) * step_rows)
                lax.fori_loop(first, last, turn_of, 0)

    def head_turn(extent, turn, carry):
        open_rows = extent - step_rows
        columns = pl.ds(pl.multiple_of(turn * HEAD_DIM, HEAD_DIM), HEAD_DIM)
        q = qg[0, :, columns]
        g = qg[1, :, columns]
        keys = kv[:extent, :HEAD_DIM]
        values = kv[:extent, HEAD_DIM:]
        own_keys = kvn[:, :HEAD_DIM]
        own_values = kvn[:, HEAD_DIM:]
        key_pos = open_rows + lax.broadcasted_iota(jnp.int32, (step_rows, rows2), 0)
        near = lax.broadcasted_iota(jnp.int32, (rows, rows), 0)
        same = (near ^ lax.broadcasted_iota(jnp.int32, (rows, rows), 1)) < block
        s = dot_nt(keys, q) * score_scale
        s_edge = jnp.where(key_pos < limit, s[open_rows:], MASKED)
        s = jnp.concatenate([s[:open_rows], s_edge], axis=0) if open_rows else s_edge
        s_own = jnp.where(same, dot_nt(own_keys, q[rows:]) * score_scale, MASKED)
        peak = jnp.max(s, axis=0, keepdims=True)
        peak_own = jnp.maximum(peak[:, rows:], jnp.max(s_own, axis=0, keepdims=True))
        peak = jnp.concatenate([peak[:, :rows], peak_own], axis=1)
        e = jnp.exp(s - peak)
        e_own = jnp.exp(s_own - peak_own)
        total = jnp.sum(e, axis=0, keepdims=True)
        total_own = total[:, rows:] + jnp.sum(e_own, axis=0, keepdims=True)
        inverse = 1.0 / jnp.concatenate([total[:, :rows], total_own], axis=1)
        p = e * inverse
        p_own = e_own * inverse[:, rows:]
        p_half = p.astype(jnp.bfloat16)
        p_half_own = p_own.astype(jnp.bfloat16)
        gp = dot_nt(values, g)
        gp_own = dot_nt(own_values, g[rows:])
        delta = jnp.sum(p_half.astype(jnp.float32) * gp, axis=0, keepdims=True)
        delta_own = delta[:, rows:] + jnp.sum(
            p_half_own.astype(jnp.float32) * gp_own, axis=0, keepdims=True
        )
        delta = jnp.concatenate([delta[:, :rows], delta_own], axis=1)
        ds = (p * (gp - delta)).astype(jnp.bfloat16)
        ds_own = (p_own * (gp_own - delta_own)).astype(jnp.bfloat16)
        dkv[:extent, :HEAD_DIM] += dot(ds, q)
        dkv[:extent, HEAD_DIM:] += dot(p_half, g)
        dn[:, :HEAD_DIM] += dot(ds_own, q[rows:])
        dn[:, HEAD_DIM:] += dot(p_half_own, g[rows:])
        dq = dot(kt[:, :extent], ds)
        dq_own = dq[:, rows:] + dot(knt[...], ds_own)
        dq_ref[:rows, columns] = (dq[:, :rows] * score_scale).T.astype(jnp.bfloat16)
        dq_ref[rows:, columns] = (dq_own * score_scale).T.astype(jnp.bfloat16)
        return carry

    turns = qg.shape[2] // HEAD_DIM
    head_turns(0, turns * 5 // 8)

    @pl.when(me < n - 1)
    def _():
        pl.semaphore_wait(kv_credit, n - 1 - me)

    for peer in cross[::-1]:
        pl.when(peer > me)(cross_copy(1, peer).start)
    head_turns(turns * 5 // 8, turns)

    pair_scale = jnp.where(
        lax.broadcasted_iota(jnp.int32, (1, 2 * HEAD_DIM), 1) < HEAD_DIM, score_scale, 1.0
    )
    clean, noisy = pl.ds(0, rows), pl.ds(rows, rows)
    pga[me, noisy] = (dn[...] * pair_scale).astype(jnp.bfloat16)
    for peer in mates:
        part = pga.at[me, noisy]
        put(part, part, pg_s.at[0], pn_r.at[mate_slot(me, peer)], context=peer)
    for block_at in range(n):
        pgp[block_at] = (dkv[block_at * rows : (block_at + 1) * rows] * pair_scale).astype(jnp.bfloat16)
    for k, peer in far:
        put_if(peer < me, pgp.at[peer], pin.at[me], pp_s.at[k - 1], pp_r.at[slot(me, peer)], context=peer)
        drain(pgp.at[peer], pp_s.at[k - 1], peer < me)


    def clean_copy(peer):
        part = pga.at[me, clean]
        return copy_of(part, part, pg_s.at[1], pc_r.at[slot(me, peer)], context=peer)

    for peer in mates:
        pl.when((peer > me) & inner)(mate_copy(0, peer).start)
    put(pga.at[me, noisy], pgo.at[noisy], po_sem.at[0], po_sem.at[1], head=other)
    dkv[my_rows, :] *= pair_scale

    def cross_onward(src, part):
        held = tokd.at[src, cross_rows(head, part)]
        arrived(held, t1_r.at[part, lax.rem(src, half)])
        put(held, held, f1_s.at[part], f1_r.at[part, lax.rem(src, half)], head=other)

    def mate_held(src, core, part):
        return tokd.at[src, mate_rows(core, 0)] if part == 0 else tokn.at[src - base, mate_rows(core, 1)]

    def mate_onward(src, part):
        held = mate_held(src, head, part)
        arrived(held, t2_r.at[part, mate_slot(src, me)])
        put(held, held, f2_s.at[part], f2_r.at[part, mate_slot(src, me)], head=other)

    for src in mates:
        mate_onward(src, 1)
    for src in cross:
        cross_onward(src, 0)
    foreign_side, foreign_columns = token_block(partner)
    gf = dot(pga[me, noisy].T, tokf[foreign_side, rows:, foreign_columns])
    for src in mates:
        arrived(mate_held(src, other, 1), f2_r.at[1, mate_slot(src, me)])
        arrived(pga.at[src, noisy], pn_r.at[mate_slot(src, me)])
        gf += dot(pga[src, noisy].T, tokn[src - base])
    slab = gf.shape[0] // m
    for at in range(m):
        gsum[at] = gf[at * slab : (at + 1) * slab]
        fp[at] = gf[at * slab : (at + 1) * slab].astype(jnp.bfloat16)
    foreign_own[...] = gsum[me_dp]
    for peer in dp_peers:
        put(fp.at[peer], fin.at[me_dp], rf_s.at[0], rf_r.at[dp_slot(me_dp, peer)], dp=peer)
    drain(fp.at[pl.ds(0, m - 1)], rf_s.at[0])
    for k, src in near:

        @pl.when(src > me)
        def _(src=src):
            arrived(pin.at[src], pp_r.at[slot(src, me)])
            dkv[my_rows, :] += pin[src].astype(jnp.float32)

    for _, peer in near:

        @pl.when((me == 0) & (peer > 1))
        def _(peer=peer):
            pl.semaphore_signal(pin_credit, inc=1, device_id={"context": peer}, device_id_type=MESH)

    pga[me, clean] = dkv[my_rows, :].astype(jnp.bfloat16)
    for k, peer in far:
        pl.when(peer > me)(clean_copy(peer).start)
    for k, peer in near:
        pl.when((peer < me) & (peer > 0))(clean_copy(peer).start)

    @pl.when(me > 1)
    def _():
        pl.semaphore_wait(pin_credit, 1)

    for k, peer in near:
        pl.when((peer < me) & (peer == 0))(clean_copy(peer).start)
    put(pga.at[me, clean], pgo.at[clean], po_sem.at[0], po_sem.at[2], head=other)
    drain(pga.at[pl.ds(0, half - 1), noisy], pg_s.at[0])
    drain(pga.at[pl.ds(0, n - 1), clean], pg_s.at[1])
    drain(pga.at[me], po_sem.at[0])

    own_tokens.wait()
    for src in mates:
        mate_onward(src, 0)
    for src in cross:
        cross_onward(src, 1)
    gw = dot(pga[me].T, tokd[me])
    for src in mates:
        arrived(mate_held(src, other, 0), f2_r.at[0, mate_slot(src, me)])
        arrived(pga.at[src, clean], pc_r.at[slot(src, me)])
        gw += dot(pga[src].T, tokd[src])
    for src in cross:
        for part in range(2):
            arrived(tokd.at[src, cross_rows(other, part)], f1_r.at[part, lax.rem(src, half)])
        arrived(pga.at[src, clean], pc_r.at[slot(src, me)])
        gw += dot(pga[src, clean].T, tokd[src, clean])

    for at in range(m):
        gsum[at] = gw[at * slab : (at + 1) * slab]
        rp[at] = gw[at * slab : (at + 1) * slab].astype(jnp.bfloat16)
    for peer in dp_peers:
        put(rp.at[peer], rin.at[me_dp], rs_s.at[0], rs_r.at[dp_slot(me_dp, peer)], dp=peer)
    drain(rp.at[pl.ds(0, m - 1)], rs_s.at[0])
    foreign_sum = foreign_own[...]
    for src in dp_peers:
        arrived(fin.at[src], rf_r.at[dp_slot(src, me_dp)])
        foreign_sum += fin[src].astype(jnp.float32)
    zout[...] = foreign_sum.astype(jnp.bfloat16)
    put(zout, zin, z_sem.at[0], z_sem.at[1], context=partner)
    drain(zout, z_sem.at[0])
    arrived(wo, wo_sem.at[1])
    arrived(pgo.at[noisy], po_sem.at[1])
    arrived(pgo.at[clean], po_sem.at[2])
    for at in range(half):
        gx_ref[:, at * wrows : (at + 1) * wrows] = (
            dot_nt(pga[me], wf[head * half + at]) + dot_nt(pgo[...], wo[at])
        ).astype(jnp.bfloat16)

    slab_sum = gsum[me_dp]
    for src in dp_peers:
        arrived(rin.at[src], rs_r.at[dp_slot(src, me_dp)])
        slab_sum += rin[src].astype(jnp.float32)
    arrived(zin, z_sem.at[1])
    slab_sum += zin[...].astype(jnp.float32)
    rall[me_dp] = slab_sum.astype(jnp.bfloat16)
    for peer in dp_peers:
        put(rall.at[me_dp], rall.at[me_dp], ra_s.at[0], ra_r.at[dp_slot(me_dp, peer)], dp=peer)
    drain(rall.at[pl.ds(0, m - 1)], ra_s.at[0])
    for src in dp_peers:
        arrived(rall.at[src], ra_r.at[dp_slot(src, me_dp)])
    for at in range(m):
        gsum[at] = rall[at].astype(jnp.float32)
    gwk_ref[...] = gsum[: m // 2].reshape(HEAD_DIM, wrows).T
    gwv_ref[...] = gsum[m // 2 :].reshape(HEAD_DIM, wrows).T
    for condition, copy in drains:
        if condition is None:
            copy.wait_send()
        else:
            pl.when(condition)(copy.wait_send)


def store_kernel(dq_in, gx_in, gwk_in, gwv_in, dq_out, gx_out, gwk_out, gwv_out, sem):
    pairs = ((gx_in, gx_out), (dq_in, dq_out), (gwk_in, gwk_out), (gwv_in, gwv_out))
    copies = [pltpu.make_async_copy(src, dst, sem.at[at]) for at, (src, dst) in enumerate(pairs)]
    for copy in copies:
        copy.start()
    for copy in copies:
        copy.wait()


def per_device(tokens, queries, grad_out, w_key, w_value, block_len):
    n = lax.axis_size("context")
    m = lax.axis_size("dp")
    rows = tokens.shape[2]
    features = tokens.shape[3]
    wrows, width = w_key.shape
    q_width = queries.shape[3]
    share = wrows // m // 16 * 16
    direct_slots = n - 1 if wrows > m * share else 1
    half = n // 2
    pair = 2 * width
    bf16, f32 = jnp.bfloat16, jnp.float32
    vmem = pl.BlockSpec(memory_space=pltpu.VMEM)
    dma = pltpu.SemaphoreType.DMA
    hbm = pl.BlockSpec(memory_space=pltpu.HBM)
    slab = pair // m
    results = (
        ((2 * rows, q_width), bf16),
        ((2 * rows, features), bf16),
        ((wrows, width), f32),
        ((wrows, width), f32),
    )
    dq, gx, gwk, gwv = pl.pallas_call(
        functools.partial(fused_kernel, n, m, share),
        out_shape=tuple(pltpu.VMEM(*result) for result in results),
        in_specs=[pl.BlockSpec(memory_space=pltpu.SMEM)] + [hbm] * 5,
        out_specs=(vmem, vmem, vmem, vmem),
        scratch_shapes=[
            pltpu.VMEM((2, 2 * rows, q_width), bf16),
            pltpu.VMEM((2, 2 * rows, features), bf16),
            pltpu.VMEM((n, wrows, pair), bf16),
            pltpu.VMEM((half, wrows, pair), bf16),
            pltpu.VMEM((n * rows, pair), bf16),
            pltpu.VMEM((rows, pair), bf16),
            pltpu.VMEM((width, n * rows), bf16),
            pltpu.VMEM((width, rows), bf16),
            pltpu.VMEM((n * rows, pair), f32),
            pltpu.VMEM((rows, pair), f32),
            pltpu.VMEM((n, rows, pair), bf16),
            pltpu.VMEM((n, rows, pair), bf16),
            pltpu.VMEM((n, 2 * rows, pair), bf16),
            pltpu.VMEM((2 * rows, pair), bf16),
            pltpu.VMEM((n, 2 * rows, wrows), bf16),
            pltpu.VMEM((half, rows, wrows), bf16),
            pltpu.VMEM((m, slab, wrows), f32),
            pltpu.VMEM((m, slab, wrows), bf16),
            pltpu.VMEM((m, slab, wrows), bf16),
            pltpu.VMEM((m, slab, wrows), bf16),
            pltpu.VMEM((m, slab, wrows), bf16),
            pltpu.VMEM((m, slab, wrows), bf16),
            pltpu.VMEM((slab, wrows), f32),
            pltpu.VMEM((slab, wrows), bf16),
            pltpu.VMEM((slab, wrows), bf16),
            dma((4,)), pltpu.SemaphoreType.REGULAR, pltpu.SemaphoreType.REGULAR, pltpu.SemaphoreType.REGULAR, dma((2,)),
            dma((n + 1,)), dma((n - 1, 2)), dma((direct_slots,)), dma((direct_slots,)),
            dma((n - 1,)), dma((n - 1, max(6, m - 1))), dma((2,)), dma((n - 1,)), dma((n - 1,)),
            dma((2,)), dma((2, half)), dma((2,)), dma((2, half)),
            dma((2,)), dma((2, half - 1)), dma((2,)), dma((2, half - 1)), dma((n - 1,)), dma((n - 1,)),
            dma((2,)), dma((half - 1,)), dma((n - 1,)), dma((3,)),
            dma((1,)), dma((m - 1,)), dma((2,)), dma((1,)), dma((m - 1,)), dma((1,)), dma((m - 1,)),
        ],
        compiler_params=pltpu.CompilerParams(
            collective_id=0, has_side_effects=True, vmem_limit_bytes=VMEM_LIMIT
        ),
    )(
        block_len,
        tokens.reshape(2 * rows, features),
        queries.reshape(2 * rows, q_width),
        grad_out.reshape(2 * rows, q_width),
        w_key,
        w_value,
    )
    dq, gx, gwk, gwv = pl.pallas_call(
        store_kernel,
        out_shape=tuple(jax.ShapeDtypeStruct(*result) for result in results),
        in_specs=[vmem] * 4,
        out_specs=(hbm, hbm, hbm, hbm),
        scratch_shapes=[dma((4,))],
    )(*(pltpu.with_memory_space_constraint(x, pltpu.VMEM) for x in (dq, gx, gwk, gwv)))
    return (
        dq.reshape(queries.shape),
        gx.reshape(tokens.shape),
        gwk,
        gwv,
    )


def solution(mesh):
    placed = (
        P("dp", None, "context", "head"),
        P("dp", None, "context", "head"),
        P("dp", None, "context", "head"),
        P("context", "head"),
        P("context", "head"),
        P("dp"),
    )
    return jax.shard_map(
        per_device,
        mesh=mesh,
        in_specs=placed,
        out_specs=(
            P("dp", None, "context", "head"),
            P("dp", None, "context", "head"),
            P("context", "head"),
            P("context", "head"),
        ),
        check_vma=False,
    )
```

```python
import functools
import math

import jax
import jax.numpy as jnp
from jax import lax
from jax.experimental import pallas as pl
from jax.experimental.pallas import tpu as pltpu
from jax.sharding import PartitionSpec as P

HEAD_DIM = 128
MASKED = -1e30
VMEM_LIMIT = 56 * 1024 * 1024
MESH = pl.DeviceIdType.MESH
NT = (((1,), (1,)), ((), ()))


def line_order(me, n):
    low, high = me, n - 1 - me
    both = jnp.minimum(low, high)
    longer = jnp.where(low < high, 1, -1)
    order = []
    for k in range(1, n):
        near_side = 1 if k % 2 else -1
        peer = jnp.where(k <= 2 * both, me + near_side * ((k + 1) // 2), me + longer * (k - both))
        order.append((k, peer))
    return order


def dot(left, right):
    return jnp.dot(left, right, preferred_element_type=jnp.float32)


def dot_nt(left, right):
    return lax.dot_general(left, right, NT, preferred_element_type=jnp.float32)


def fused_kernel(
    n, m, share, pack,
    blk_ref, tok_ref, q_in, g_in, wk_ref, wv_ref,
    dq_ref, gx_ref, gwk_ref, gwv_ref,
    qg, tokf, wf, wo, kv, kvn, kt, knt, dkv, dn, pgp, pin, pga, pgo, tokd, tokn,
    gsum, rp, rin, rall, fp, fin, foreign_own, zout, zin,
    loc_sem, pair_sem, kv_credit, tok_sem, wz_s, wz_r, wd_s, wd_r, wx_s, wx_r, wo_sem, kv_s, kv_r,
    t1_s, t1_r, f1_s, f1_r, t2_s, t2_r, f2_s, f2_r, pp_s, pp_r, pg_s, pn_r, pc_r, po_sem,
    rf_s, rf_r, z_sem, rs_s, rs_r, ra_s, ra_r,
):
    me_dp = lax.axis_index("dp")
    me = lax.axis_index("context")
    head = lax.axis_index("head")
    other = 1 - head
    rows2, features = tok_ref.shape
    rows = rows2 // 2
    wrows = wk_ref.shape[0]
    half = n // 2
    score_scale = 1.0 / math.sqrt(HEAD_DIM)
    drains = []

    def copy_of(src, dst, send_sem, recv_sem, **device):
        return pltpu.make_async_remote_copy(
            src_ref=src, dst_ref=dst, send_sem=send_sem, recv_sem=recv_sem,
            device_id=device, device_id_type=MESH,
        )

    def put(src, dst, send_sem, recv_sem, **device):
        copy_of(src, dst, send_sem, recv_sem, **device).start()

    def put_if(condition, src, dst, send_sem, recv_sem, **device):
        pl.when(condition)(copy_of(src, dst, send_sem, recv_sem, **device).start)

    def arrived(dst, recv_sem):
        copy_of(dst, dst, loc_sem.at[0], recv_sem, head=other).wait_recv()

    def drain(whole, send_sem, condition=None):
        drains.append((condition, copy_of(whole, whole, send_sem, loc_sem.at[0], head=other)))

    def slot(src, dst):
        return lax.rem(src - dst + n - 1, n)

    def inside(place):
        return (place >= 0) & (place < n)

    def dp_slot(src, dst):
        return lax.rem(src - dst + m - 1, m)

    near = line_order(me, n)
    far = near[::-1]
    sides = (me + 1, me - 1)
    dp_peers = [lax.rem(me_dp + off, m) for off in range(1, m)]

    two_step = m == 4 and share % 32 == 0
    if two_step:
        low = lax.rem(me_dp, 2)
        w_peers = [(0, me_dp + 1 - 2 * low), (1, lax.rem(me_dp + 2, 4))]
    else:
        w_peers = list(enumerate(dp_peers))

    w_copies = [
        pltpu.make_async_copy(wk_ref, wf.at[me, :, pl.ds(0, HEAD_DIM)], loc_sem.at[0]),
        pltpu.make_async_copy(wv_ref, wf.at[me, :, pl.ds(HEAD_DIM, HEAD_DIM)], loc_sem.at[0]),
    ]
    own_half = pltpu.make_async_copy(tok_ref, tokf.at[head], loc_sem.at[1])
    row_copies = [
        pltpu.make_async_copy(q_in, qg.at[0], loc_sem.at[2]),
        pltpu.make_async_copy(g_in, qg.at[1], loc_sem.at[2]),
    ]
    for copy in w_copies + [own_half] + row_copies:
        copy.start()
    barrier = pltpu.get_barrier_semaphore()
    for _, peer in near:
        pl.semaphore_signal(barrier, inc=1, device_id={"context": peer}, device_id_type=MESH)
    for peer in dp_peers:
        pl.semaphore_signal(barrier, inc=1, device_id={"dp": peer}, device_id_type=MESH)
    pl.semaphore_signal(barrier, inc=1, device_id={"head": other}, device_id_type=MESH)
    pl.semaphore_wait(barrier, n + m - 1)

    def cores_meet():
        pl.semaphore_signal(pair_sem, inc=1, device_id={"head": other}, device_id_type=MESH)
        pl.semaphore_wait(pair_sem, 1)

    shared_base = pl.multiple_of(me_dp * share, 16)
    chunks = 2 if two_step else 1
    piece_rows = share // chunks

    def w_piece(owner, base, chunk):
        return wf.at[owner, pl.ds(pl.multiple_of(base + chunk * piece_rows, 16), piece_rows)]

    direct_rows = wrows - m * share
    direct = pl.ds(m * share, direct_rows)
    pltpu.make_async_copy(wf.at[me], wf.at[me], loc_sem.at[0]).wait()
    share_rows = wf.at[0, pl.ds(0, share)]
    for chunk in range(chunks):
        part = w_piece(me, shared_base, chunk)
        for at, peer in enumerate(sides):
            put_if(inside(peer), part, part, wz_s.at[at], wz_r.at[slot(me, peer), chunk], context=peer)
    for at, peer in enumerate(sides):
        drain(share_rows, wz_s.at[at], inside(peer))
    own_half.wait()
    put(tokf.at[head], tokf.at[head], tok_sem.at[0], tok_sem.at[1], head=other)
    drain(tokf.at[head], tok_sem.at[0])
    if direct_rows:
        for k, peer in near:
            part = wf.at[me, direct]
            put(part, part, wd_s.at[k - 1], wd_r.at[slot(me, peer)], context=peer)
            drain(part, wd_s.at[k - 1])

    def token_block(owner):
        column = pl.multiple_of(lax.rem(owner, half) * wrows, 128)
        return owner // half, pl.ds(column, wrows)

    quarter = rows // 4
    base = me // half * half
    place = me - base
    mates = [base + lax.rem(place + k, half) for k in range(1, half)]
    cross = [jnp.where(me < half, half + k, half - 1 - k) for k in range(half)]
    partner = lax.rem(me + half, n)
    outer = (me == 0) | (me == n - 1)
    inner = (me > 0) & (me < n - 1)

    def mate_slot(src, dst):
        return lax.rem(src - dst + half - 1, half)

    def cross_rows(core, part):
        return pl.ds(pl.multiple_of(core * 2 * quarter + part * quarter, 16), quarter)

    def mate_rows(core, part):
        if part == 0:
            return pl.ds(pl.multiple_of(core * rows, 16), rows)
        return pl.ds(pl.multiple_of(core * 2 * quarter, 16), 2 * quarter)

    def cross_copy(part, peer):
        span = cross_rows(head, part)
        side, columns = token_block(peer)
        return copy_of(
            tokf.at[side, span, columns], tokd.at[me, span],
            t1_s.at[part], t1_r.at[part, lax.rem(me, half)], context=peer,
        )

    def mate_copy(part, peer):
        if part == 0:
            side, columns = token_block(peer)
            span = mate_rows(head, 0)
            held = tokd.at[me, span]
        else:
            side, columns = token_block(lax.rem(peer + half, n))
            span = pl.ds(pl.multiple_of(rows + head * 2 * quarter, 16), 2 * quarter)
            held = tokn.at[place, mate_rows(head, 1)]
        return copy_of(
            tokf.at[side, span, columns], held,
            t2_s.at[part], t2_r.at[part, mate_slot(me, peer)], context=peer,
        )

    my_side, my_columns = token_block(me)

    def w_forward(src):
        for dp_at, peer in w_peers:
            part = w_piece(src, peer * share, dp_at)
            arrived(part, wx_r.at[slot(src, me), 2 * dp_at + dp_at])
            to = w_peers[1 - dp_at][1]
            put(part, part, wx_s.at[slot(src, me)], wx_r.at[slot(src, me), 4 + dp_at], dp=to)

    for k, src in near:
        onward = jnp.where(src > me, me - 1, me + 1)
        for chunk in range(chunks):
            part = w_piece(src, shared_base, chunk)
            arrived(part, wz_r.at[slot(src, me), chunk])
            put_if(inside(onward), part, part, wz_s.at[1 + k], wz_r.at[slot(src, onward), chunk], context=onward)
            for dp_at, peer in w_peers:
                put(part, part, wx_s.at[slot(src, me)], wx_r.at[slot(src, me), chunks * dp_at + chunk], dp=peer)
        drain(share_rows, wz_s.at[1 + k], inside(onward))
        drain(wf.at[0, pl.ds(0, (m - 1) * share)], wx_s.at[slot(src, me)])
        if k == 1:
            arrived(tokf.at[other], tok_sem.at[1])
            for peer in mates:
                for part in range(2):
                    pl.when(outer)(mate_copy(part, peer).start)
        if two_step and k > 1:
            w_forward(near[k - 2][1])
    cores_meet()
    for peer in cross[::-1]:
        cross_copy(0, peer).start()
    for peer in cross[::-1]:
        pl.when(peer < me)(cross_copy(1, peer).start)
    for peer in mates:
        pl.when(inner)(mate_copy(1, peer).start)
        pl.when((peer < me) & inner)(mate_copy(0, peer).start)
    own_tokens = pltpu.make_async_copy(tokf.at[my_side, :, my_columns], tokd.at[me], loc_sem.at[3])
    own_tokens.start()
    for part in range(2):
        held = tokd.at[pl.ds(0, half), pl.ds(0, quarter)]
        drain(held, t1_s.at[part])
        drain(held, f1_s.at[part])
    for part, held in enumerate((tokd.at[pl.ds(0, half - 1), pl.ds(0, rows)], tokn.at[pl.ds(0, half - 1), pl.ds(0, 2 * quarter)])):
        drain(held, t2_s.at[part])
        drain(held, f2_s.at[part])
    if two_step:
        w_forward(near[-1][1])

    projected = dot(tokf[my_side, :, my_columns], wf[me])
    for k, src in near:
        if direct_rows:
            arrived(wf.at[src, direct], wd_r.at[slot(src, me)])
        if two_step:
            for dp_at, peer in w_peers:
                part = w_piece(src, peer * share, 1 - dp_at)
                arrived(part, wx_r.at[slot(src, me), 2 * dp_at + 1 - dp_at])
                part = w_piece(src, (3 - me_dp) * share, dp_at)
                arrived(part, wx_r.at[slot(src, me), 4 + dp_at])
        else:
            for off in range(1, m):
                part = w_piece(src, lax.rem(me_dp + m - off, m) * share, 0)
                arrived(part, wx_r.at[slot(src, me), off - 1])
        side, columns = token_block(src)
        projected += dot(tokf[side, :, columns], wf[src])
    pairs = projected.astype(jnp.bfloat16)
    my_rows = pl.ds(pl.multiple_of(me * rows, rows), rows)
    kv[my_rows, :] = pairs[:rows]
    kvn[...] = pairs[rows:]
    for k, peer in far:
        put_if(peer > me, kv.at[my_rows], kv.at[my_rows], kv_s.at[k - 1], kv_r.at[slot(me, peer)], context=peer)
        drain(kv.at[my_rows], kv_s.at[k - 1], peer > me)
    put(wf.at[pl.ds(other * half, half)], wo, wo_sem.at[0], wo_sem.at[1], head=other)
    drain(wo, wo_sem.at[0])

    block = blk_ref[0]
    total_rows = n * rows
    lane = lax.broadcasted_iota(jnp.int32, (1, pack * rows2), 1)
    noisy_lane = lane >= pack * rows
    position = me * rows + lane % rows
    block_start = position & (-block)
    limit = jnp.where(noisy_lane, block_start, block_start + block)
    dkv[...] = jnp.zeros_like(dkv)
    dn[...] = jnp.zeros_like(dn)
    knt[...] = kvn[:, :HEAD_DIM].T
    pltpu.make_async_copy(qg, qg, loc_sem.at[2]).wait()
    for k, src in near:
        span = pl.ds(pl.multiple_of(src * rows, rows), rows)

        @pl.when(src < me)
        def _(span=span, src=src):
            arrived(kv.at[span], kv_r.at[slot(src, me)])

        @pl.when(src > me)
        def _(span=span):
            kv[span, :] = jnp.zeros((rows, 2 * HEAD_DIM), jnp.bfloat16)
    for _, peer in near:

        @pl.when(peer < me)
        def _(peer=peer):
            pl.semaphore_signal(kv_credit, inc=1, device_id={"context": peer}, device_id_type=MESH)

    kt[...] = kv[:, :HEAD_DIM].T

    steps = 4 if n % 4 == 0 else 1
    step_rows = total_rows // steps

    def head_turns(first, last):
        for step in range(steps):

            @pl.when(me // (n // steps) == step)
            def _(step=step):
                turn_of = functools.partial(head_turn, (step + 1) * step_rows)
                lax.fori_loop(first, last, turn_of, 0)

    wide = pack * rows

    def head_turn(extent, turn, carry):
        open_rows = extent - step_rows
        spans = [
            pl.ds(pl.multiple_of((turn * pack + at) * HEAD_DIM, HEAD_DIM), HEAD_DIM) for at in range(pack)
        ]

        def stacked(which):
            held = [qg[which, :, span] for span in spans]
            return jnp.concatenate([x[:rows] for x in held] + [x[rows:] for x in held], axis=0)

        q = stacked(0)
        g = stacked(1)
        keys = kv[:extent, :HEAD_DIM]
        values = kv[:extent, HEAD_DIM:]
        own_keys = kvn[:, :HEAD_DIM]
        own_values = kvn[:, HEAD_DIM:]
        key_pos = open_rows + lax.broadcasted_iota(jnp.int32, (step_rows, 2 * wide), 0)
        near_key = lax.broadcasted_iota(jnp.int32, (rows, wide), 0)
        near_row = lax.broadcasted_iota(jnp.int32, (rows, wide), 1) % rows
        same = (near_key ^ near_row) < block
        s = dot_nt(keys, q)
        s_edge = jnp.where(key_pos < limit, s[open_rows:], MASKED)
        s = jnp.concatenate([s[:open_rows], s_edge], axis=0) if open_rows else s_edge
        s_own = jnp.where(same, dot_nt(own_keys, q[wide:]), MASKED)
        peak = jnp.max(s, axis=0, keepdims=True)
        peak_own = jnp.maximum(peak[:, wide:], jnp.max(s_own, axis=0, keepdims=True))
        peak = jnp.concatenate([peak[:, :wide], peak_own], axis=1)
        e = jnp.exp((s - peak) * score_scale)
        e_own = jnp.exp((s_own - peak_own) * score_scale)
        total = jnp.sum(e, axis=0, keepdims=True)
        total_own = total[:, wide:] + jnp.sum(e_own, axis=0, keepdims=True)
        inverse = 1.0 / jnp.concatenate([total[:, :wide], total_own], axis=1)
        p = e * inverse
        p_own = e_own * inverse[:, wide:]
        p_half = p.astype(jnp.bfloat16)
        p_half_own = p_own.astype(jnp.bfloat16)
        weighted = p * dot_nt(values, g)
        weighted_own = p_own * dot_nt(own_values, g[wide:])
        delta = jnp.sum(weighted, axis=0, keepdims=True)
        delta_own = delta[:, wide:] + jnp.sum(weighted_own, axis=0, keepdims=True)
        delta = jnp.concatenate([delta[:, :wide], delta_own], axis=1)
        ds = (weighted - p * delta).astype(jnp.bfloat16)
        ds_own = (weighted_own - p_own * delta_own).astype(jnp.bfloat16)
        dkv[:extent, :HEAD_DIM] += dot(ds, q)
        dkv[:extent, HEAD_DIM:] += dot(p_half, g)
        dn[:, :HEAD_DIM] += dot(ds_own, q[wide:])
        dn[:, HEAD_DIM:] += dot(p_half_own, g[wide:])
        dq = dot(kt[:, :extent], ds)
        dq_own = dq[:, wide:] + dot(knt[...], ds_own)
        for at, span in enumerate(spans):
            lanes = slice(at * rows, (at + 1) * rows)
            dq_ref[:rows, span] = (dq[:, lanes] * score_scale).T.astype(jnp.bfloat16)
            dq_ref[rows:, span] = (dq_own[:, lanes] * score_scale).T.astype(jnp.bfloat16)
        return carry

    turns = qg.shape[2] // HEAD_DIM // pack
    head_turns(0, turns // 2)

    @pl.when(me < n - 1)
    def _():
        pl.semaphore_wait(kv_credit, n - 1 - me)

    for peer in cross[::-1]:
        pl.when(peer > me)(cross_copy(1, peer).start)
    head_turns(turns // 2, turns)

    pair_scale = jnp.where(
        lax.broadcasted_iota(jnp.int32, (1, 2 * HEAD_DIM), 1) < HEAD_DIM, score_scale, 1.0
    )
    clean, noisy = pl.ds(0, rows), pl.ds(rows, rows)
    pga[me, noisy] = (dn[...] * pair_scale).astype(jnp.bfloat16)
    for peer in mates:
        part = pga.at[me, noisy]
        put(part, part, pg_s.at[0], pn_r.at[mate_slot(me, peer)], context=peer)
    for block_at in range(n):
        pgp[block_at] = (dkv[block_at * rows : (block_at + 1) * rows] * pair_scale).astype(jnp.bfloat16)
    for k, peer in far:
        put_if(peer < me, pgp.at[peer], pin.at[me], pp_s.at[k - 1], pp_r.at[slot(me, peer)], context=peer)
        drain(pgp.at[peer], pp_s.at[k - 1], peer < me)


    def clean_copy(peer):
        part = pga.at[me, clean]
        return copy_of(part, part, pg_s.at[1], pc_r.at[slot(me, peer)], context=peer)

    for peer in mates:
        pl.when((peer > me) & inner)(mate_copy(0, peer).start)
    put(pga.at[me, noisy], pgo.at[noisy], po_sem.at[0], po_sem.at[1], head=other)
    dkv[my_rows, :] *= pair_scale

    def cross_onward(src, part):
        held = tokd.at[src, cross_rows(head, part)]
        arrived(held, t1_r.at[part, lax.rem(src, half)])
        put(held, held, f1_s.at[part], f1_r.at[part, lax.rem(src, half)], head=other)

    def mate_held(src, core, part):
        return tokd.at[src, mate_rows(core, 0)] if part == 0 else tokn.at[src - base, mate_rows(core, 1)]

    def mate_onward(src, part):
        held = mate_held(src, head, part)
        arrived(held, t2_r.at[part, mate_slot(src, me)])
        put(held, held, f2_s.at[part], f2_r.at[part, mate_slot(src, me)], head=other)

    for src in mates:
        mate_onward(src, 1)
    for src in cross:
        cross_onward(src, 0)
    foreign_side, foreign_columns = token_block(partner)
    gf = dot(pga[me, noisy].T, tokf[foreign_side, rows:, foreign_columns])
    for src in mates:
        arrived(mate_held(src, other, 1), f2_r.at[1, mate_slot(src, me)])
        arrived(pga.at[src, noisy], pn_r.at[mate_slot(src, me)])
        gf += dot(pga[src, noisy].T, tokn[src - base])
    slab = gf.shape[0] // m
    for at in range(m):
        gsum[at] = gf[at * slab : (at + 1) * slab]
        fp[at] = gf[at * slab : (at + 1) * slab].astype(jnp.bfloat16)
    foreign_own[...] = gsum[me_dp]
    for peer in dp_peers:
        put(fp.at[peer], fin.at[me_dp], rf_s.at[0], rf_r.at[dp_slot(me_dp, peer)], dp=peer)
    drain(fp.at[pl.ds(0, m - 1)], rf_s.at[0])
    for k, src in near:

        @pl.when(src > me)
        def _(src=src):
            arrived(pin.at[src], pp_r.at[slot(src, me)])
            dkv[my_rows, :] += pin[src].astype(jnp.float32)

    pga[me, clean] = dkv[my_rows, :].astype(jnp.bfloat16)
    for k, peer in far:
        pl.when(peer > me)(clean_copy(peer).start)
    for k, peer in far:
        pl.when((peer < me))(clean_copy(peer).start)


    put(pga.at[me, clean], pgo.at[clean], po_sem.at[0], po_sem.at[2], head=other)
    drain(pga.at[pl.ds(0, half - 1), noisy], pg_s.at[0])
    drain(pga.at[pl.ds(0, n - 1), clean], pg_s.at[1])
    drain(pga.at[me], po_sem.at[0])

    own_tokens.wait()
    for src in mates:
        mate_onward(src, 0)
    for src in cross:
        cross_onward(src, 1)
    gw = dot(pga[me].T, tokd[me])
    for src in mates:
        arrived(mate_held(src, other, 0), f2_r.at[0, mate_slot(src, me)])
        arrived(pga.at[src, clean], pc_r.at[slot(src, me)])
        gw += dot(pga[src].T, tokd[src])
    for src in cross:
        for part in range(2):
            arrived(tokd.at[src, cross_rows(other, part)], f1_r.at[part, lax.rem(src, half)])
        arrived(pga.at[src, clean], pc_r.at[slot(src, me)])
        gw += dot(pga[src, clean].T, tokd[src, clean])

    for at in range(m):
        gsum[at] = gw[at * slab : (at + 1) * slab]
        rp[at] = gw[at * slab : (at + 1) * slab].astype(jnp.bfloat16)
    parts = 2 if slab % 32 == 0 else 1

    def slab_part(part):
        return pl.ds(part * (slab // parts), slab // parts)

    for part in range(parts):
        span = slab_part(part)
        for peer in dp_peers:
            put(rp.at[peer, span], rin.at[me_dp, span], rs_s.at[0], rs_r.at[part, dp_slot(me_dp, peer)], dp=peer)
    drain(rp.at[pl.ds(0, m - 1)], rs_s.at[0])
    foreign_sum = foreign_own[...]
    for src in dp_peers:
        arrived(fin.at[src], rf_r.at[dp_slot(src, me_dp)])
        foreign_sum += fin[src].astype(jnp.float32)
    zout[...] = foreign_sum.astype(jnp.bfloat16)
    for part in range(parts):
        span = slab_part(part)
        put(zout.at[span], zin.at[span], z_sem.at[0], z_sem.at[1 + part], context=partner)
    drain(zout, z_sem.at[0])
    arrived(wo, wo_sem.at[1])
    arrived(pgo.at[noisy], po_sem.at[1])
    arrived(pgo.at[clean], po_sem.at[2])
    for at in range(half):
        gx_ref[:, at * wrows : (at + 1) * wrows] = (
            dot_nt(pga[me], wf[head * half + at]) + dot_nt(pgo[...], wo[at])
        ).astype(jnp.bfloat16)

    for part in range(parts):
        span = slab_part(part)
        slab_sum = gsum[me_dp, span]
        for src in dp_peers:
            arrived(rin.at[src, span], rs_r.at[part, dp_slot(src, me_dp)])
            slab_sum += rin[src, span].astype(jnp.float32)
        arrived(zin.at[span], z_sem.at[1 + part])
        slab_sum += zin[span].astype(jnp.float32)
        rall[me_dp, span] = slab_sum.astype(jnp.bfloat16)
        for peer in dp_peers:
            held = rall.at[me_dp, span]
            put(held, held, ra_s.at[0], ra_r.at[part, dp_slot(me_dp, peer)], dp=peer)
    drain(rall.at[pl.ds(0, m - 1)], ra_s.at[0])
    for part in range(parts):
        span = slab_part(part)
        for src in dp_peers:
            arrived(rall.at[src, span], ra_r.at[part, dp_slot(src, me_dp)])
    for at in range(m):
        gsum[at] = rall[at].astype(jnp.float32)
    gwk_ref[...] = gsum[: m // 2].reshape(HEAD_DIM, wrows).T
    gwv_ref[...] = gsum[m // 2 :].reshape(HEAD_DIM, wrows).T
    for condition, copy in drains:
        if condition is None:
            copy.wait_send()
        else:
            pl.when(condition)(copy.wait_send)


def store_kernel(dq_in, gx_in, gwk_in, gwv_in, dq_out, gx_out, gwk_out, gwv_out, sem):
    pairs = ((gx_in, gx_out), (dq_in, dq_out), (gwk_in, gwk_out), (gwv_in, gwv_out))
    copies = [pltpu.make_async_copy(src, dst, sem.at[at]) for at, (src, dst) in enumerate(pairs)]
    for copy in copies:
        copy.start()
    for copy in copies:
        copy.wait()


def per_device(tokens, queries, grad_out, w_key, w_value, block_len):
    n = lax.axis_size("context")
    m = lax.axis_size("dp")
    rows = tokens.shape[2]
    features = tokens.shape[3]
    wrows, width = w_key.shape
    q_width = queries.shape[3]
    share = wrows // m // 16 * 16
    direct_slots = n - 1 if wrows > m * share else 1
    half = n // 2
    pair = 2 * width
    bf16, f32 = jnp.bfloat16, jnp.float32
    vmem = pl.BlockSpec(memory_space=pltpu.VMEM)
    dma = pltpu.SemaphoreType.DMA
    heads = q_width // HEAD_DIM
    pack = math.gcd(heads, max(1, min(4, 2048 // (n * rows))))
    hbm = pl.BlockSpec(memory_space=pltpu.HBM)
    slab = pair // m
    results = (
        ((2 * rows, q_width), bf16),
        ((2 * rows, features), bf16),
        ((wrows, width), f32),
        ((wrows, width), f32),
    )
    dq, gx, gwk, gwv = pl.pallas_call(
        functools.partial(fused_kernel, n, m, share, pack),
        out_shape=tuple(pltpu.VMEM(*result) for result in results),
        in_specs=[pl.BlockSpec(memory_space=pltpu.SMEM)] + [hbm] * 5,
        out_specs=(vmem, vmem, vmem, vmem),
        scratch_shapes=[
            pltpu.VMEM((2, 2 * rows, q_width), bf16),
            pltpu.VMEM((2, 2 * rows, features), bf16),
            pltpu.VMEM((n, wrows, pair), bf16),
            pltpu.VMEM((half, wrows, pair), bf16),
            pltpu.VMEM((n * rows, pair), bf16),
            pltpu.VMEM((rows, pair), bf16),
            pltpu.VMEM((width, n * rows), bf16),
            pltpu.VMEM((width, rows), bf16),
            pltpu.VMEM((n * rows, pair), f32),
            pltpu.VMEM((rows, pair), f32),
            pltpu.VMEM((n, rows, pair), bf16),
            pltpu.VMEM((n, rows, pair), bf16),
            pltpu.VMEM((n, 2 * rows, pair), bf16),
            pltpu.VMEM((2 * rows, pair), bf16),
            pltpu.VMEM((n, 2 * rows, wrows), bf16),
            pltpu.VMEM((half, rows, wrows), bf16),
            pltpu.VMEM((m, slab, wrows), f32),
            pltpu.VMEM((m, slab, wrows), bf16),
            pltpu.VMEM((m, slab, wrows), bf16),
            pltpu.VMEM((m, slab, wrows), bf16),
            pltpu.VMEM((m, slab, wrows), bf16),
            pltpu.VMEM((m, slab, wrows), bf16),
            pltpu.VMEM((slab, wrows), f32),
            pltpu.VMEM((slab, wrows), bf16),
            pltpu.VMEM((slab, wrows), bf16),
            dma((4,)), pltpu.SemaphoreType.REGULAR, pltpu.SemaphoreType.REGULAR, dma((2,)),
            dma((n + 1,)), dma((n - 1, 2)), dma((direct_slots,)), dma((direct_slots,)),
            dma((n - 1,)), dma((n - 1, max(6, m - 1))), dma((2,)), dma((n - 1,)), dma((n - 1,)),
            dma((2,)), dma((2, half)), dma((2,)), dma((2, half)),
            dma((2,)), dma((2, half - 1)), dma((2,)), dma((2, half - 1)), dma((n - 1,)), dma((n - 1,)),
            dma((2,)), dma((half - 1,)), dma((n - 1,)), dma((3,)),
            dma((1,)), dma((m - 1,)), dma((3,)), dma((1,)), dma((2, m - 1)), dma((1,)), dma((2, m - 1)),
        ],
        compiler_params=pltpu.CompilerParams(
            collective_id=0, has_side_effects=True, vmem_limit_bytes=VMEM_LIMIT
        ),
    )(
        block_len,
        tokens.reshape(2 * rows, features),
        queries.reshape(2 * rows, q_width),
        grad_out.reshape(2 * rows, q_width),
        w_key,
        w_value,
    )
    dq, gx, gwk, gwv = pl.pallas_call(
        store_kernel,
        out_shape=tuple(jax.ShapeDtypeStruct(*result) for result in results),
        in_specs=[vmem] * 4,
        out_specs=(hbm, hbm, hbm, hbm),
        scratch_shapes=[dma((4,))],
    )(*(pltpu.with_memory_space_constraint(x, pltpu.VMEM) for x in (dq, gx, gwk, gwv)))
    return (
        dq.reshape(queries.shape),
        gx.reshape(tokens.shape),
        gwk,
        gwv,
    )


def solution(mesh):
    placed = (
        P("dp", None, "context", "head"),
        P("dp", None, "context", "head"),
        P("dp", None, "context", "head"),
        P("context", "head"),
        P("context", "head"),
        P("dp"),
    )
    return jax.shard_map(
        per_device,
        mesh=mesh,
        in_specs=placed,
        out_specs=(
            P("dp", None, "context", "head"),
            P("dp", None, "context", "head"),
            P("context", "head"),
            P("context", "head"),
        ),
        check_vma=False,
    )
```

```python
import functools
import math

import jax
import jax.numpy as jnp
from jax import lax
from jax.experimental import pallas as pl
from jax.experimental.pallas import tpu as pltpu
from jax.sharding import PartitionSpec as P

HEAD_DIM = 128
MASKED = -1e30
VMEM_LIMIT = 56 * 1024 * 1024
MESH = pl.DeviceIdType.MESH
NT = (((1,), (1,)), ((), ()))


def line_order(me, n):
    low, high = me, n - 1 - me
    both = jnp.minimum(low, high)
    longer = jnp.where(low < high, 1, -1)
    order = []
    for k in range(1, n):
        near_side = 1 if k % 2 else -1
        peer = jnp.where(k <= 2 * both, me + near_side * ((k + 1) // 2), me + longer * (k - both))
        order.append((k, peer))
    return order


def dot(left, right):
    return jnp.dot(left, right, preferred_element_type=jnp.float32)


def dot_nt(left, right):
    return lax.dot_general(left, right, NT, preferred_element_type=jnp.float32)


def fused_kernel(
    n, m, share, pack,
    blk_ref, tok_ref, q_in, g_in, wk_ref, wv_ref,
    dq_ref, gx_ref, gwk_ref, gwv_ref,
    qg, tokf, wf, wo, kv, kvn, kt, knt, dkv, dn, pgp, pin, pga, pgo, tokd, tokn,
    gsum, rp, rin, rall, fp, fin, foreign_own, zout, zin,
    loc_sem, pair_sem, kv_credit, sent_credit, tok_sem, wz_s, wz_r, wd_s, wd_r, wx_s, wx_r, wo_sem, kv_s, kv_r,
    t1_s, t1_r, f1_s, f1_r, t2_s, t2_r, f2_s, f2_r, pp_s, pp_r, pg_s, pn_r, pc_r, po_sem,
    rf_s, rf_r, z_sem, rs_s, rs_r, ra_s, ra_r,
):
    me_dp = lax.axis_index("dp")
    me = lax.axis_index("context")
    head = lax.axis_index("head")
    other = 1 - head
    rows2, features = tok_ref.shape
    rows = rows2 // 2
    wrows = wk_ref.shape[0]
    half = n // 2
    score_scale = 1.0 / math.sqrt(HEAD_DIM)
    drains = []

    def copy_of(src, dst, send_sem, recv_sem, **device):
        return pltpu.make_async_remote_copy(
            src_ref=src, dst_ref=dst, send_sem=send_sem, recv_sem=recv_sem,
            device_id=device, device_id_type=MESH,
        )

    def put(src, dst, send_sem, recv_sem, **device):
        copy_of(src, dst, send_sem, recv_sem, **device).start()

    def put_if(condition, src, dst, send_sem, recv_sem, **device):
        pl.when(condition)(copy_of(src, dst, send_sem, recv_sem, **device).start)

    def arrived(dst, recv_sem):
        copy_of(dst, dst, loc_sem.at[0], recv_sem, head=other).wait_recv()

    def drain(whole, send_sem, condition=None):
        drains.append((condition, copy_of(whole, whole, send_sem, loc_sem.at[0], head=other)))

    def slot(src, dst):
        return lax.rem(src - dst + n - 1, n)

    def inside(place):
        return (place >= 0) & (place < n)

    def dp_slot(src, dst):
        return lax.rem(src - dst + m - 1, m)

    near = line_order(me, n)
    far = near[::-1]
    sides = (me + 1, me - 1)
    ring_peers = [lax.rem(me_dp + off, m) for off in range(1, m)]
    dp_peers = [jnp.where(k < me_dp, k, k + 1) for k in range(m - 1)]

    two_step = m == 4 and share % 32 == 0
    if two_step:
        low = lax.rem(me_dp, 2)
        w_peers = [(0, me_dp + 1 - 2 * low), (1, lax.rem(me_dp + 2, 4))]
    else:
        w_peers = list(enumerate(ring_peers))

    w_copies = [
        pltpu.make_async_copy(wk_ref, wf.at[me, :, pl.ds(0, HEAD_DIM)], loc_sem.at[0]),
        pltpu.make_async_copy(wv_ref, wf.at[me, :, pl.ds(HEAD_DIM, HEAD_DIM)], loc_sem.at[0]),
    ]
    own_half = pltpu.make_async_copy(tok_ref, tokf.at[head], loc_sem.at[1])
    row_copies = [
        pltpu.make_async_copy(q_in, qg.at[0], loc_sem.at[2]),
        pltpu.make_async_copy(g_in, qg.at[1], loc_sem.at[2]),
    ]
    for copy in w_copies + [own_half] + row_copies:
        copy.start()
    barrier = pltpu.get_barrier_semaphore()
    for _, peer in near:
        pl.semaphore_signal(barrier, inc=1, device_id={"context": peer}, device_id_type=MESH)
    for peer in dp_peers:
        pl.semaphore_signal(barrier, inc=1, device_id={"dp": peer}, device_id_type=MESH)
    pl.semaphore_signal(barrier, inc=1, device_id={"head": other}, device_id_type=MESH)
    pl.semaphore_wait(barrier, n + m - 1)

    def cores_meet():
        pl.semaphore_signal(pair_sem, inc=1, device_id={"head": other}, device_id_type=MESH)
        pl.semaphore_wait(pair_sem, 1)

    shared_base = pl.multiple_of(me_dp * share, 16)
    chunks = 2 if two_step else 1
    piece_rows = share // chunks

    def w_piece(owner, base, chunk):
        return wf.at[owner, pl.ds(pl.multiple_of(base + chunk * piece_rows, 16), piece_rows)]

    direct_rows = wrows - m * share
    direct = pl.ds(m * share, direct_rows)
    pltpu.make_async_copy(wf.at[me], wf.at[me], loc_sem.at[0]).wait()
    share_rows = wf.at[0, pl.ds(0, share)]
    for chunk in range(chunks):
        part = w_piece(me, shared_base, chunk)
        for at, peer in enumerate(sides):
            put_if(inside(peer), part, part, wz_s.at[at], wz_r.at[slot(me, peer), chunk], context=peer)
    for at, peer in enumerate(sides):
        drain(share_rows, wz_s.at[at], inside(peer))
    own_half.wait()
    put(tokf.at[head], tokf.at[head], tok_sem.at[0], tok_sem.at[1], head=other)
    drain(tokf.at[head], tok_sem.at[0])
    if direct_rows:
        for k, peer in near:
            part = wf.at[me, direct]
            put(part, part, wd_s.at[k - 1], wd_r.at[slot(me, peer)], context=peer)
            drain(part, wd_s.at[k - 1])

    def token_block(owner):
        column = pl.multiple_of(lax.rem(owner, half) * wrows, 128)
        return owner // half, pl.ds(column, wrows)

    quarter = rows // 4
    base = me // half * half
    place = me - base
    mates = [base + lax.rem(place + k, half) for k in range(1, half)]
    cross = [jnp.where(me < half, half + k, half - 1 - k) for k in range(half)]
    partner = lax.rem(me + half, n)
    outer = (me == 0) | (me == n - 1)
    inner = (me > 0) & (me < n - 1)

    def mate_slot(src, dst):
        return lax.rem(src - dst + half - 1, half)

    def cross_rows(core, part):
        return pl.ds(pl.multiple_of(core * 2 * quarter + part * quarter, 16), quarter)

    def mate_rows(core, part):
        if part == 0:
            return pl.ds(pl.multiple_of(core * rows, 16), rows)
        return pl.ds(pl.multiple_of(core * 2 * quarter, 16), 2 * quarter)

    def cross_copy(part, peer):
        span = cross_rows(head, part)
        side, columns = token_block(peer)
        return copy_of(
            tokf.at[side, span, columns], tokd.at[me, span],
            t1_s.at[part], t1_r.at[part, lax.rem(me, half)], context=peer,
        )

    def mate_copy(part, peer):
        if part == 0:
            side, columns = token_block(peer)
            span = mate_rows(head, 0)
            held = tokd.at[me, span]
        else:
            side, columns = token_block(lax.rem(peer + half, n))
            span = pl.ds(pl.multiple_of(rows + head * 2 * quarter, 16), 2 * quarter)
            held = tokn.at[place, mate_rows(head, 1)]
        return copy_of(
            tokf.at[side, span, columns], held,
            t2_s.at[part], t2_r.at[part, mate_slot(me, peer)], context=peer,
        )

    my_side, my_columns = token_block(me)

    def w_forward(src):
        for dp_at, peer in w_peers:
            part = w_piece(src, peer * share, dp_at)
            arrived(part, wx_r.at[slot(src, me), 2 * dp_at + dp_at])
            to = w_peers[1 - dp_at][1]
            put(part, part, wx_s.at[slot(src, me)], wx_r.at[slot(src, me), 4 + dp_at], dp=to)

    for k, src in near:
        onward = jnp.where(src > me, me - 1, me + 1)
        for chunk in range(chunks):
            part = w_piece(src, shared_base, chunk)
            arrived(part, wz_r.at[slot(src, me), chunk])
            put_if(inside(onward), part, part, wz_s.at[1 + k], wz_r.at[slot(src, onward), chunk], context=onward)
            for dp_at, peer in w_peers:
                put(part, part, wx_s.at[slot(src, me)], wx_r.at[slot(src, me), chunks * dp_at + chunk], dp=peer)
        drain(share_rows, wz_s.at[1 + k], inside(onward))
        drain(wf.at[0, pl.ds(0, (m - 1) * share)], wx_s.at[slot(src, me)])
        if k == 1:
            arrived(tokf.at[other], tok_sem.at[1])
            for peer in mates:
                for part in range(2):
                    pl.when(outer)(mate_copy(part, peer).start)
        if two_step and k > 1:
            w_forward(near[k - 2][1])
    cores_meet()
    for peer in cross[::-1]:
        cross_copy(0, peer).start()
    for peer in cross[::-1]:
        pl.when(peer < me)(cross_copy(1, peer).start)
    for peer in mates:
        pl.when(inner)(mate_copy(1, peer).start)
        pl.when((peer < me) & inner)(mate_copy(0, peer).start)
    own_tokens = pltpu.make_async_copy(tokf.at[my_side, :, my_columns], tokd.at[me], loc_sem.at[3])
    own_tokens.start()
    for part in range(2):
        held = tokd.at[pl.ds(0, half), pl.ds(0, quarter)]
        drain(held, t1_s.at[part])
        drain(held, f1_s.at[part])
    for part, held in enumerate((tokd.at[pl.ds(0, half - 1), pl.ds(0, rows)], tokn.at[pl.ds(0, half - 1), pl.ds(0, 2 * quarter)])):
        drain(held, t2_s.at[part])
        drain(held, f2_s.at[part])
    if two_step:
        w_forward(near[-1][1])

    projected = dot(tokf[my_side, :, my_columns], wf[me])
    for k, src in near:
        if direct_rows:
            arrived(wf.at[src, direct], wd_r.at[slot(src, me)])
        if two_step:
            for dp_at, peer in w_peers:
                part = w_piece(src, peer * share, 1 - dp_at)
                arrived(part, wx_r.at[slot(src, me), 2 * dp_at + 1 - dp_at])
                part = w_piece(src, (3 - me_dp) * share, dp_at)
                arrived(part, wx_r.at[slot(src, me), 4 + dp_at])
        else:
            for off in range(1, m):
                part = w_piece(src, lax.rem(me_dp + m - off, m) * share, 0)
                arrived(part, wx_r.at[slot(src, me), off - 1])
        side, columns = token_block(src)
        projected += dot(tokf[side, :, columns], wf[src])
    pairs = projected.astype(jnp.bfloat16)
    my_rows = pl.ds(pl.multiple_of(me * rows, rows), rows)
    kv[my_rows, :] = pairs[:rows]
    kvn[...] = pairs[rows:]
    for k, peer in far:
        put_if(peer > me, kv.at[my_rows], kv.at[my_rows], kv_s.at[k - 1], kv_r.at[slot(me, peer)], context=peer)
        drain(kv.at[my_rows], kv_s.at[k - 1], peer > me)
    put(wf.at[pl.ds(other * half, half)], wo, wo_sem.at[0], wo_sem.at[1], head=other)
    drain(wo, wo_sem.at[0])

    block = blk_ref[0]
    total_rows = n * rows
    lane = lax.broadcasted_iota(jnp.int32, (1, pack * rows2), 1)
    noisy_lane = lane >= pack * rows
    position = me * rows + lane % rows
    block_start = position & (-block)
    limit = jnp.where(noisy_lane, block_start, block_start + block)
    dkv[...] = jnp.zeros_like(dkv)
    dn[...] = jnp.zeros_like(dn)
    knt[...] = kvn[:, :HEAD_DIM].T
    pltpu.make_async_copy(qg, qg, loc_sem.at[2]).wait()
    for k, src in near:
        span = pl.ds(pl.multiple_of(src * rows, rows), rows)

        @pl.when(src < me)
        def _(span=span, src=src):
            arrived(kv.at[span], kv_r.at[slot(src, me)])

        @pl.when(src > me)
        def _(span=span):
            kv[span, :] = jnp.zeros((rows, 2 * HEAD_DIM), jnp.bfloat16)
    for _, peer in near:

        @pl.when(peer < me)
        def _(peer=peer):
            pl.semaphore_signal(kv_credit, inc=1, device_id={"context": peer}, device_id_type=MESH)

    kt[...] = kv[:, :HEAD_DIM].T

    steps = 4 if n % 4 == 0 else 1
    step_rows = total_rows // steps

    def head_turns(first, last):
        for step in range(steps):

            @pl.when(me // (n // steps) == step)
            def _(step=step):
                turn_of = functools.partial(head_turn, (step + 1) * step_rows)
                lax.fori_loop(first, last, turn_of, 0)

    wide = pack * rows

    def head_turn(extent, turn, carry):
        open_rows = extent - step_rows
        spans = [
            pl.ds(pl.multiple_of((turn * pack + at) * HEAD_DIM, HEAD_DIM), HEAD_DIM) for at in range(pack)
        ]

        def stacked(which):
            held = [qg[which, :, span] for span in spans]
            return jnp.concatenate([x[:rows] for x in held] + [x[rows:] for x in held], axis=0)

        q = stacked(0)
        g = stacked(1)
        keys = kv[:extent, :HEAD_DIM]
        values = kv[:extent, HEAD_DIM:]
        own_keys = kvn[:, :HEAD_DIM]
        own_values = kvn[:, HEAD_DIM:]
        key_pos = open_rows + lax.broadcasted_iota(jnp.int32, (step_rows, 2 * wide), 0)
        near_key = lax.broadcasted_iota(jnp.int32, (rows, wide), 0)
        near_row = lax.broadcasted_iota(jnp.int32, (rows, wide), 1) % rows
        same = (near_key ^ near_row) < block
        s = dot_nt(keys, q)
        s_edge = jnp.where(key_pos < limit, s[open_rows:], MASKED)
        s = jnp.concatenate([s[:open_rows], s_edge], axis=0) if open_rows else s_edge
        s_own = jnp.where(same, dot_nt(own_keys, q[wide:]), MASKED)
        peak = jnp.max(s, axis=0, keepdims=True)
        peak_own = jnp.maximum(peak[:, wide:], jnp.max(s_own, axis=0, keepdims=True))
        peak = jnp.concatenate([peak[:, :wide], peak_own], axis=1)
        e = jnp.exp((s - peak) * score_scale)
        e_own = jnp.exp((s_own - peak_own) * score_scale)
        total = jnp.sum(e, axis=0, keepdims=True)
        total_own = total[:, wide:] + jnp.sum(e_own, axis=0, keepdims=True)
        inverse = 1.0 / jnp.concatenate([total[:, :wide], total_own], axis=1)
        p = e * inverse
        p_own = e_own * inverse[:, wide:]
        p_half = p.astype(jnp.bfloat16)
        p_half_own = p_own.astype(jnp.bfloat16)
        weighted = p * dot_nt(values, g)
        weighted_own = p_own * dot_nt(own_values, g[wide:])
        delta = jnp.sum(weighted, axis=0, keepdims=True)
        delta_own = delta[:, wide:] + jnp.sum(weighted_own, axis=0, keepdims=True)
        delta = jnp.concatenate([delta[:, :wide], delta_own], axis=1)
        ds = (weighted - p * delta).astype(jnp.bfloat16)
        ds_own = (weighted_own - p_own * delta_own).astype(jnp.bfloat16)
        dkv[:extent, :HEAD_DIM] += dot(ds, q)
        dkv[:extent, HEAD_DIM:] += dot(p_half, g)
        dn[:, :HEAD_DIM] += dot(ds_own, q[wide:])
        dn[:, HEAD_DIM:] += dot(p_half_own, g[wide:])
        dq = dot(kt[:, :extent], ds)
        dq_own = dq[:, wide:] + dot(knt[...], ds_own)
        for at, span in enumerate(spans):
            lanes = slice(at * rows, (at + 1) * rows)
            dq_ref[:rows, span] = (dq[:, lanes] * score_scale).T.astype(jnp.bfloat16)
            dq_ref[rows:, span] = (dq_own[:, lanes] * score_scale).T.astype(jnp.bfloat16)
        return carry

    turns = qg.shape[2] // HEAD_DIM // pack
    head_turns(0, turns // 2)

    @pl.when(me < n - 1)
    def _():
        pl.semaphore_wait(kv_credit, n - 1 - me)

    for peer in cross[::-1]:
        pl.when(peer > me)(cross_copy(1, peer).start)
    head_turns(turns // 2, turns)

    pair_scale = jnp.where(
        lax.broadcasted_iota(jnp.int32, (1, 2 * HEAD_DIM), 1) < HEAD_DIM, score_scale, 1.0
    )
    clean, noisy = pl.ds(0, rows), pl.ds(rows, rows)
    pga[me, noisy] = (dn[...] * pair_scale).astype(jnp.bfloat16)
    for peer in mates:
        part = pga.at[me, noisy]
        put(part, part, pg_s.at[0], pn_r.at[mate_slot(me, peer)], context=peer)
    for block_at in range(n):
        pgp[block_at] = (dkv[block_at * rows : (block_at + 1) * rows] * pair_scale).astype(jnp.bfloat16)
    for k, peer in far:
        put_if(peer < me, pgp.at[peer], pin.at[me], pp_s.at[k - 1], pp_r.at[slot(me, peer)], context=peer)


    def clean_copy(peer):
        part = pga.at[me, clean]
        return copy_of(part, part, pg_s.at[1], pc_r.at[slot(me, peer)], context=peer)

    for peer in mates:
        pl.when((peer > me) & inner)(mate_copy(0, peer).start)
    put(pga.at[me, noisy], pgo.at[noisy], po_sem.at[0], po_sem.at[1], head=other)
    dkv[my_rows, :] *= pair_scale

    def cross_onward(src, part):
        held = tokd.at[src, cross_rows(head, part)]
        arrived(held, t1_r.at[part, lax.rem(src, half)])
        put(held, held, f1_s.at[part], f1_r.at[part, lax.rem(src, half)], head=other)

    def mate_held(src, core, part):
        return tokd.at[src, mate_rows(core, 0)] if part == 0 else tokn.at[src - base, mate_rows(core, 1)]

    def mate_onward(src, part):
        held = mate_held(src, head, part)
        arrived(held, t2_r.at[part, mate_slot(src, me)])
        put(held, held, f2_s.at[part], f2_r.at[part, mate_slot(src, me)], head=other)

    for src in mates:
        mate_onward(src, 1)
    for src in cross:
        cross_onward(src, 0)
    foreign_side, foreign_columns = token_block(partner)
    gf = dot(pga[me, noisy].T, tokf[foreign_side, rows:, foreign_columns])
    for src in mates:
        arrived(mate_held(src, other, 1), f2_r.at[1, mate_slot(src, me)])
        arrived(pga.at[src, noisy], pn_r.at[mate_slot(src, me)])
        gf += dot(pga[src, noisy].T, tokn[src - base])
    slab = gf.shape[0] // m
    for at in range(m):
        gsum[at] = gf[at * slab : (at + 1) * slab]
        fp[at] = gf[at * slab : (at + 1) * slab].astype(jnp.bfloat16)
    foreign_own[...] = gsum[me_dp]
    for peer in dp_peers:
        put(fp.at[peer], fin.at[me_dp], rf_s.at[0], rf_r.at[dp_slot(me_dp, peer)], dp=peer)
    drain(fp.at[pl.ds(0, m - 1)], rf_s.at[0])
    for k, peer in near:
        sent = copy_of(pgp.at[peer], pgp.at[peer], pp_s.at[k - 1], loc_sem.at[0], head=other)
        pl.when(peer < me)(sent.wait_send)
    for _, peer in near:

        @pl.when((peer > me) & (me > 0))
        def _(peer=peer):
            pl.semaphore_signal(sent_credit, inc=1, device_id={"context": peer}, device_id_type=MESH)

    for k, src in near:

        @pl.when(src > me)
        def _(src=src):
            arrived(pin.at[src], pp_r.at[slot(src, me)])
            dkv[my_rows, :] += pin[src].astype(jnp.float32)

    pga[me, clean] = dkv[my_rows, :].astype(jnp.bfloat16)
    for k, peer in far:
        pl.when(peer > me)(clean_copy(peer).start)

    @pl.when(me > 1)
    def _():
        pl.semaphore_wait(sent_credit, me - 1)

    for k, peer in far:
        pl.when((peer < me))(clean_copy(peer).start)


    put(pga.at[me, clean], pgo.at[clean], po_sem.at[0], po_sem.at[2], head=other)
    drain(pga.at[pl.ds(0, half - 1), noisy], pg_s.at[0])
    drain(pga.at[pl.ds(0, n - 1), clean], pg_s.at[1])
    drain(pga.at[me], po_sem.at[0])

    own_tokens.wait()
    for src in mates:
        mate_onward(src, 0)
    for src in cross:
        cross_onward(src, 1)
    gw = dot(pga[me].T, tokd[me])
    for src in mates:
        arrived(mate_held(src, other, 0), f2_r.at[0, mate_slot(src, me)])
        arrived(pga.at[src, clean], pc_r.at[slot(src, me)])
        gw += dot(pga[src].T, tokd[src])
    for src in cross:
        for part in range(2):
            arrived(tokd.at[src, cross_rows(other, part)], f1_r.at[part, lax.rem(src, half)])
        arrived(pga.at[src, clean], pc_r.at[slot(src, me)])
        gw += dot(pga[src, clean].T, tokd[src, clean])

    for at in range(m):
        gsum[at] = gw[at * slab : (at + 1) * slab]
        rp[at] = gw[at * slab : (at + 1) * slab].astype(jnp.bfloat16)
    parts = 2 if slab % 32 == 0 else 1

    def slab_part(part):
        return pl.ds(part * (slab // parts), slab // parts)

    for part in range(parts):
        span = slab_part(part)
        for peer in dp_peers:
            put(rp.at[peer, span], rin.at[me_dp, span], rs_s.at[0], rs_r.at[part, dp_slot(me_dp, peer)], dp=peer)
    drain(rp.at[pl.ds(0, m - 1)], rs_s.at[0])
    foreign_sum = foreign_own[...]
    for src in dp_peers:
        arrived(fin.at[src], rf_r.at[dp_slot(src, me_dp)])
        foreign_sum += fin[src].astype(jnp.float32)
    zout[...] = foreign_sum.astype(jnp.bfloat16)
    for part in range(parts):
        span = slab_part(part)
        put(zout.at[span], zin.at[span], z_sem.at[0], z_sem.at[1 + part], context=partner)
    drain(zout, z_sem.at[0])
    arrived(wo, wo_sem.at[1])
    arrived(pgo.at[noisy], po_sem.at[1])
    arrived(pgo.at[clean], po_sem.at[2])
    for at in range(half):
        gx_ref[:, at * wrows : (at + 1) * wrows] = (
            dot_nt(pga[me], wf[head * half + at]) + dot_nt(pgo[...], wo[at])
        ).astype(jnp.bfloat16)

    for part in range(parts):
        span = slab_part(part)
        slab_sum = gsum[me_dp, span]
        for src in dp_peers:
            arrived(rin.at[src, span], rs_r.at[part, dp_slot(src, me_dp)])
            slab_sum += rin[src, span].astype(jnp.float32)
        arrived(zin.at[span], z_sem.at[1 + part])
        slab_sum += zin[span].astype(jnp.float32)
        rall[me_dp, span] = slab_sum.astype(jnp.bfloat16)
        for peer in dp_peers:
            held = rall.at[me_dp, span]
            put(held, held, ra_s.at[0], ra_r.at[part, dp_slot(me_dp, peer)], dp=peer)
    drain(rall.at[pl.ds(0, m - 1)], ra_s.at[0])
    for part in range(parts):
        span = slab_part(part)
        for src in dp_peers:
            arrived(rall.at[src, span], ra_r.at[part, dp_slot(src, me_dp)])
    for at in range(m):
        gsum[at] = rall[at].astype(jnp.float32)
    gwk_ref[...] = gsum[: m // 2].reshape(HEAD_DIM, wrows).T
    gwv_ref[...] = gsum[m // 2 :].reshape(HEAD_DIM, wrows).T
    for condition, copy in drains:
        if condition is None:
            copy.wait_send()
        else:
            pl.when(condition)(copy.wait_send)


def store_kernel(dq_in, gx_in, gwk_in, gwv_in, dq_out, gx_out, gwk_out, gwv_out, sem):
    pairs = ((gx_in, gx_out), (dq_in, dq_out), (gwk_in, gwk_out), (gwv_in, gwv_out))
    copies = [pltpu.make_async_copy(src, dst, sem.at[at]) for at, (src, dst) in enumerate(pairs)]
    for copy in copies:
        copy.start()
    for copy in copies:
        copy.wait()


def per_device(tokens, queries, grad_out, w_key, w_value, block_len):
    n = lax.axis_size("context")
    m = lax.axis_size("dp")
    rows = tokens.shape[2]
    features = tokens.shape[3]
    wrows, width = w_key.shape
    q_width = queries.shape[3]
    share = wrows // m // 16 * 16
    direct_slots = n - 1 if wrows > m * share else 1
    half = n // 2
    pair = 2 * width
    bf16, f32 = jnp.bfloat16, jnp.float32
    vmem = pl.BlockSpec(memory_space=pltpu.VMEM)
    dma = pltpu.SemaphoreType.DMA
    heads = q_width // HEAD_DIM
    pack = math.gcd(heads, max(1, min(4, 2048 // (n * rows))))
    hbm = pl.BlockSpec(memory_space=pltpu.HBM)
    slab = pair // m
    results = (
        ((2 * rows, q_width), bf16),
        ((2 * rows, features), bf16),
        ((wrows, width), f32),
        ((wrows, width), f32),
    )
    dq, gx, gwk, gwv = pl.pallas_call(
        functools.partial(fused_kernel, n, m, share, pack),
        out_shape=tuple(pltpu.VMEM(*result) for result in results),
        in_specs=[pl.BlockSpec(memory_space=pltpu.SMEM)] + [hbm] * 5,
        out_specs=(vmem, vmem, vmem, vmem),
        scratch_shapes=[
            pltpu.VMEM((2, 2 * rows, q_width), bf16),
            pltpu.VMEM((2, 2 * rows, features), bf16),
            pltpu.VMEM((n, wrows, pair), bf16),
            pltpu.VMEM((half, wrows, pair), bf16),
            pltpu.VMEM((n * rows, pair), bf16),
            pltpu.VMEM((rows, pair), bf16),
            pltpu.VMEM((width, n * rows), bf16),
            pltpu.VMEM((width, rows), bf16),
            pltpu.VMEM((n * rows, pair), f32),
            pltpu.VMEM((rows, pair), f32),
            pltpu.VMEM((n, rows, pair), bf16),
            pltpu.VMEM((n, rows, pair), bf16),
            pltpu.VMEM((n, 2 * rows, pair), bf16),
            pltpu.VMEM((2 * rows, pair), bf16),
            pltpu.VMEM((n, 2 * rows, wrows), bf16),
            pltpu.VMEM((half, rows, wrows), bf16),
            pltpu.VMEM((m, slab, wrows), f32),
            pltpu.VMEM((m, slab, wrows), bf16),
            pltpu.VMEM((m, slab, wrows), bf16),
            pltpu.VMEM((m, slab, wrows), bf16),
            pltpu.VMEM((m, slab, wrows), bf16),
            pltpu.VMEM((m, slab, wrows), bf16),
            pltpu.VMEM((slab, wrows), f32),
            pltpu.VMEM((slab, wrows), bf16),
            pltpu.VMEM((slab, wrows), bf16),
            dma((4,)), pltpu.SemaphoreType.REGULAR, pltpu.SemaphoreType.REGULAR, pltpu.SemaphoreType.REGULAR, dma((2,)),
            dma((n + 1,)), dma((n - 1, 2)), dma((direct_slots,)), dma((direct_slots,)),
            dma((n - 1,)), dma((n - 1, max(6, m - 1))), dma((2,)), dma((n - 1,)), dma((n - 1,)),
            dma((2,)), dma((2, half)), dma((2,)), dma((2, half)),
            dma((2,)), dma((2, half - 1)), dma((2,)), dma((2, half - 1)), dma((n - 1,)), dma((n - 1,)),
            dma((2,)), dma((half - 1,)), dma((n - 1,)), dma((3,)),
            dma((1,)), dma((m - 1,)), dma((3,)), dma((1,)), dma((2, m - 1)), dma((1,)), dma((2, m - 1)),
        ],
        compiler_params=pltpu.CompilerParams(
            collective_id=0, has_side_effects=True, vmem_limit_bytes=VMEM_LIMIT
        ),
    )(
        block_len,
        tokens.reshape(2 * rows, features),
        queries.reshape(2 * rows, q_width),
        grad_out.reshape(2 * rows, q_width),
        w_key,
        w_value,
    )
    dq, gx, gwk, gwv = pl.pallas_call(
        store_kernel,
        out_shape=tuple(jax.ShapeDtypeStruct(*result) for result in results),
        in_specs=[vmem] * 4,
        out_specs=(hbm, hbm, hbm, hbm),
        scratch_shapes=[dma((4,))],
    )(*(pltpu.with_memory_space_constraint(x, pltpu.VMEM) for x in (dq, gx, gwk, gwv)))
    return (
        dq.reshape(queries.shape),
        gx.reshape(tokens.shape),
        gwk,
        gwv,
    )


def solution(mesh):
    placed = (
        P("dp", None, "context", "head"),
        P("dp", None, "context", "head"),
        P("dp", None, "context", "head"),
        P("context", "head"),
        P("context", "head"),
        P("dp"),
    )
    return jax.shard_map(
        per_device,
        mesh=mesh,
        in_specs=placed,
        out_specs=(
            P("dp", None, "context", "head"),
            P("dp", None, "context", "head"),
            P("context", "head"),
            P("context", "head"),
        ),
        check_vma=False,
    )
```

```python
import functools
import math

import jax
import jax.numpy as jnp
from jax import lax
from jax.experimental import pallas as pl
from jax.experimental.pallas import tpu as pltpu
from jax.sharding import PartitionSpec as P

HEAD_DIM = 128
MASKED = -1e30
VMEM_LIMIT = 56 * 1024 * 1024
MESH = pl.DeviceIdType.MESH
NT = (((1,), (1,)), ((), ()))


def line_order(me, n):
    low, high = me, n - 1 - me
    both = jnp.minimum(low, high)
    longer = jnp.where(low < high, 1, -1)
    order = []
    for k in range(1, n):
        near_side = 1 if k % 2 else -1
        peer = jnp.where(k <= 2 * both, me + near_side * ((k + 1) // 2), me + longer * (k - both))
        order.append((k, peer))
    return order


def dot(left, right):
    return jnp.dot(left, right, preferred_element_type=jnp.float32)


def dot_nt(left, right):
    return lax.dot_general(left, right, NT, preferred_element_type=jnp.float32)


def fused_kernel(
    n, m, share, pack,
    blk_ref, tok_ref, q_in, g_in, wk_ref, wv_ref,
    dq_ref, gx_ref, gwk_ref, gwv_ref,
    qg, tokf, wf, wo, kv, kvn, kt, knt, dkv, dn, pgp, pin, pga, pgo, tokd, tokn,
    gsum, rp, rin, rall, fp, fin, foreign_own, zout, zin,
    loc_sem, pair_sem, kv_credit, sent_credit, tok_sem, wz_s, wz_r, wd_s, wd_r, wx_s, wx_r, wo_sem, kv_s, kv_r,
    t1_s, t1_r, f1_s, f1_r, t2_s, t2_r, f2_s, f2_r, pp_s, pp_r, pg_s, pn_r, pc_r, po_sem,
    rf_s, rf_r, z_sem, rs_s, rs_r, ra_s, ra_r,
):
    me_dp = lax.axis_index("dp")
    me = lax.axis_index("context")
    head = lax.axis_index("head")
    other = 1 - head
    rows2, features = tok_ref.shape
    rows = rows2 // 2
    wrows = wk_ref.shape[0]
    half = n // 2
    score_scale = 1.0 / math.sqrt(HEAD_DIM)
    drains = []

    def copy_of(src, dst, send_sem, recv_sem, **device):
        return pltpu.make_async_remote_copy(
            src_ref=src, dst_ref=dst, send_sem=send_sem, recv_sem=recv_sem,
            device_id=device, device_id_type=MESH,
        )

    def put(src, dst, send_sem, recv_sem, **device):
        copy_of(src, dst, send_sem, recv_sem, **device).start()

    def put_if(condition, src, dst, send_sem, recv_sem, **device):
        pl.when(condition)(copy_of(src, dst, send_sem, recv_sem, **device).start)

    def arrived(dst, recv_sem):
        copy_of(dst, dst, loc_sem.at[0], recv_sem, head=other).wait_recv()

    def drain(whole, send_sem, condition=None):
        drains.append((condition, copy_of(whole, whole, send_sem, loc_sem.at[0], head=other)))

    def slot(src, dst):
        return lax.rem(src - dst + n - 1, n)

    def inside(place):
        return (place >= 0) & (place < n)

    def dp_slot(src, dst):
        return lax.rem(src - dst + m - 1, m)

    near = line_order(me, n)
    far = near[::-1]
    sides = (me + 1, me - 1)
    ring_peers = [lax.rem(me_dp + off, m) for off in range(1, m)]
    dp_peers = [jnp.where(k < me_dp, k, k + 1) for k in range(m - 1)]

    two_step = m == 4 and share % 32 == 0
    if two_step:
        low = lax.rem(me_dp, 2)
        w_peers = [(0, me_dp + 1 - 2 * low), (1, lax.rem(me_dp + 2, 4))]
    else:
        w_peers = list(enumerate(ring_peers))

    w_copies = [
        pltpu.make_async_copy(wk_ref, wf.at[me, :, pl.ds(0, HEAD_DIM)], loc_sem.at[0]),
        pltpu.make_async_copy(wv_ref, wf.at[me, :, pl.ds(HEAD_DIM, HEAD_DIM)], loc_sem.at[0]),
    ]
    own_half = pltpu.make_async_copy(tok_ref, tokf.at[head], loc_sem.at[1])
    row_copies = [
        pltpu.make_async_copy(q_in, qg.at[0], loc_sem.at[2]),
        pltpu.make_async_copy(g_in, qg.at[1], loc_sem.at[2]),
    ]
    for copy in w_copies + [own_half] + row_copies:
        copy.start()
    barrier = pltpu.get_barrier_semaphore()
    for _, peer in near:
        pl.semaphore_signal(barrier, inc=1, device_id={"context": peer}, device_id_type=MESH)
    for peer in dp_peers:
        pl.semaphore_signal(barrier, inc=1, device_id={"dp": peer}, device_id_type=MESH)
    pl.semaphore_signal(barrier, inc=1, device_id={"head": other}, device_id_type=MESH)
    pl.semaphore_wait(barrier, n + m - 1)

    def cores_meet():
        pl.semaphore_signal(pair_sem, inc=1, device_id={"head": other}, device_id_type=MESH)
        pl.semaphore_wait(pair_sem, 1)

    shared_base = pl.multiple_of(me_dp * share, 16)
    chunks = 2 if two_step else 1
    piece_rows = share // chunks

    def w_piece(owner, base, chunk):
        return wf.at[owner, pl.ds(pl.multiple_of(base + chunk * piece_rows, 16), piece_rows)]

    direct_rows = wrows - m * share
    direct = pl.ds(m * share, direct_rows)
    pltpu.make_async_copy(wf.at[me], wf.at[me], loc_sem.at[0]).wait()
    share_rows = wf.at[0, pl.ds(0, share)]
    for chunk in range(chunks):
        part = w_piece(me, shared_base, chunk)
        for at, peer in enumerate(sides):
            put_if(inside(peer), part, part, wz_s.at[at], wz_r.at[slot(me, peer), chunk], context=peer)
    for at, peer in enumerate(sides):
        drain(share_rows, wz_s.at[at], inside(peer))
    own_half.wait()
    put(tokf.at[head], tokf.at[head], tok_sem.at[0], tok_sem.at[1], head=other)
    drain(tokf.at[head], tok_sem.at[0])
    if direct_rows:
        for k, peer in near:
            part = wf.at[me, direct]
            put(part, part, wd_s.at[k - 1], wd_r.at[slot(me, peer)], context=peer)
            drain(part, wd_s.at[k - 1])

    def token_block(owner):
        column = pl.multiple_of(lax.rem(owner, half) * wrows, 128)
        return owner // half, pl.ds(column, wrows)

    quarter = rows // 4
    base = me // half * half
    place = me - base
    mates = [base + lax.rem(place + k, half) for k in range(1, half)]
    cross = [jnp.where(me < half, half + k, half - 1 - k) for k in range(half)]
    partner = lax.rem(me + half, n)
    outer = (me == 0) | (me == n - 1)
    inner = (me > 0) & (me < n - 1)

    def mate_slot(src, dst):
        return lax.rem(src - dst + half - 1, half)

    def cross_rows(core, part):
        return pl.ds(pl.multiple_of(core * 2 * quarter + part * quarter, 16), quarter)

    def mate_rows(core, part):
        if part == 0:
            return pl.ds(pl.multiple_of(core * rows, 16), rows)
        return pl.ds(pl.multiple_of(core * 2 * quarter, 16), 2 * quarter)

    def cross_copy(part, peer):
        span = cross_rows(head, part)
        side, columns = token_block(peer)
        return copy_of(
            tokf.at[side, span, columns], tokd.at[me, span],
            t1_s.at[part], t1_r.at[part, lax.rem(me, half)], context=peer,
        )

    def mate_copy(part, peer):
        if part == 0:
            side, columns = token_block(peer)
            span = mate_rows(head, 0)
            held = tokd.at[me, span]
        else:
            side, columns = token_block(lax.rem(peer + half, n))
            span = pl.ds(pl.multiple_of(rows + head * 2 * quarter, 16), 2 * quarter)
            held = tokn.at[place, mate_rows(head, 1)]
        return copy_of(
            tokf.at[side, span, columns], held,
            t2_s.at[part], t2_r.at[part, mate_slot(me, peer)], context=peer,
        )

    my_side, my_columns = token_block(me)

    def w_forward(src):
        for dp_at, peer in w_peers:
            part = w_piece(src, peer * share, dp_at)
            arrived(part, wx_r.at[slot(src, me), 2 * dp_at + dp_at])
            to = w_peers[1 - dp_at][1]
            put(part, part, wx_s.at[slot(src, me)], wx_r.at[slot(src, me), 4 + dp_at], dp=to)

    for k, src in near:
        onward = jnp.where(src > me, me - 1, me + 1)
        for chunk in range(chunks):
            part = w_piece(src, shared_base, chunk)
            arrived(part, wz_r.at[slot(src, me), chunk])
            put_if(inside(onward), part, part, wz_s.at[1 + k], wz_r.at[slot(src, onward), chunk], context=onward)
            for dp_at, peer in w_peers:
                put(part, part, wx_s.at[slot(src, me)], wx_r.at[slot(src, me), chunks * dp_at + chunk], dp=peer)
        drain(share_rows, wz_s.at[1 + k], inside(onward))
        drain(wf.at[0, pl.ds(0, (m - 1) * share)], wx_s.at[slot(src, me)])
        if k == 1:
            arrived(tokf.at[other], tok_sem.at[1])
            for peer in mates:
                for part in range(2):
                    pl.when(outer)(mate_copy(part, peer).start)
        if two_step and k > 1:
            w_forward(near[k - 2][1])
    cores_meet()
    for peer in cross[::-1]:
        cross_copy(0, peer).start()
    for peer in cross[::-1]:
        pl.when(peer < me)(cross_copy(1, peer).start)
    for peer in mates:
        pl.when(inner)(mate_copy(1, peer).start)
        pl.when((peer < me) & inner)(mate_copy(0, peer).start)
    own_tokens = pltpu.make_async_copy(tokf.at[my_side, :, my_columns], tokd.at[me], loc_sem.at[3])
    own_tokens.start()
    for part in range(2):
        held = tokd.at[pl.ds(0, half), pl.ds(0, quarter)]
        drain(held, t1_s.at[part])
        drain(held, f1_s.at[part])
    for part, held in enumerate((tokd.at[pl.ds(0, half - 1), pl.ds(0, rows)], tokn.at[pl.ds(0, half - 1), pl.ds(0, 2 * quarter)])):
        drain(held, t2_s.at[part])
        drain(held, f2_s.at[part])
    if two_step:
        w_forward(near[-1][1])

    projected = dot(tokf[my_side, :, my_columns], wf[me])
    for k, src in near:
        if direct_rows:
            arrived(wf.at[src, direct], wd_r.at[slot(src, me)])
        if two_step:
            for dp_at, peer in w_peers:
                part = w_piece(src, peer * share, 1 - dp_at)
                arrived(part, wx_r.at[slot(src, me), 2 * dp_at + 1 - dp_at])
                part = w_piece(src, (3 - me_dp) * share, dp_at)
                arrived(part, wx_r.at[slot(src, me), 4 + dp_at])
        else:
            for off in range(1, m):
                part = w_piece(src, lax.rem(me_dp + m - off, m) * share, 0)
                arrived(part, wx_r.at[slot(src, me), off - 1])
        side, columns = token_block(src)
        projected += dot(tokf[side, :, columns], wf[src])
    pairs = projected.astype(jnp.bfloat16)
    my_rows = pl.ds(pl.multiple_of(me * rows, rows), rows)
    kv[my_rows, :] = pairs[:rows]
    kvn[...] = pairs[rows:]
    for k, peer in far:
        put_if(peer > me, kv.at[my_rows], kv.at[my_rows], kv_s.at[k - 1], kv_r.at[slot(me, peer)], context=peer)
        drain(kv.at[my_rows], kv_s.at[k - 1], peer > me)
    put(wf.at[pl.ds(other * half, half)], wo, wo_sem.at[0], wo_sem.at[1], head=other)
    drain(wo, wo_sem.at[0])

    block = blk_ref[0]
    total_rows = n * rows
    lane = lax.broadcasted_iota(jnp.int32, (1, pack * rows2), 1)
    noisy_lane = lane >= pack * rows
    position = me * rows + lane % rows
    block_start = position & (-block)
    limit = jnp.where(noisy_lane, block_start, block_start + block)
    dkv[...] = jnp.zeros_like(dkv)
    dn[...] = jnp.zeros_like(dn)
    knt[...] = kvn[:, :HEAD_DIM].T
    pltpu.make_async_copy(qg, qg, loc_sem.at[2]).wait()
    for k, src in near:
        span = pl.ds(pl.multiple_of(src * rows, rows), rows)

        @pl.when(src < me)
        def _(span=span, src=src):
            arrived(kv.at[span], kv_r.at[slot(src, me)])

        @pl.when(src > me)
        def _(span=span):
            kv[span, :] = jnp.zeros((rows, 2 * HEAD_DIM), jnp.bfloat16)
    for _, peer in near:

        @pl.when(peer < me)
        def _(peer=peer):
            pl.semaphore_signal(kv_credit, inc=1, device_id={"context": peer}, device_id_type=MESH)

    kt[...] = kv[:, :HEAD_DIM].T

    steps = 4 if n % 4 == 0 else 1
    step_rows = total_rows // steps

    def head_turns(first, last):
        for step in range(steps):

            @pl.when(me // (n // steps) == step)
            def _(step=step):
                turn_of = functools.partial(head_turn, (step + 1) * step_rows)
                lax.fori_loop(first, last, turn_of, 0)

    wide = pack * rows
    exp2_scale = score_scale * math.log2(math.e)

    def head_turn(extent, turn, carry):
        open_rows = extent - step_rows
        spans = [
            pl.ds(pl.multiple_of((turn * pack + at) * HEAD_DIM, HEAD_DIM), HEAD_DIM) for at in range(pack)
        ]

        def stacked(which):
            held = [qg[which, :, span] for span in spans]
            return jnp.concatenate([x[:rows] for x in held] + [x[rows:] for x in held], axis=0)

        q = stacked(0)
        g = stacked(1)
        keys = kv[:extent, :HEAD_DIM]
        values = kv[:extent, HEAD_DIM:]
        own_keys = kvn[:, :HEAD_DIM]
        own_values = kvn[:, HEAD_DIM:]
        key_pos = open_rows + lax.broadcasted_iota(jnp.int32, (step_rows, 2 * wide), 0)
        near_key = lax.broadcasted_iota(jnp.int32, (rows, wide), 0)
        near_row = lax.broadcasted_iota(jnp.int32, (rows, wide), 1) % rows
        same = (near_key ^ near_row) < block
        s = dot_nt(keys, q)
        s_edge = jnp.where(key_pos < limit, s[open_rows:], MASKED)
        s = jnp.concatenate([s[:open_rows], s_edge], axis=0) if open_rows else s_edge
        s_own = jnp.where(same, dot_nt(own_keys, q[wide:]), MASKED)
        peak = jnp.max(s, axis=0, keepdims=True)
        peak_own = jnp.maximum(peak[:, wide:], jnp.max(s_own, axis=0, keepdims=True))
        peak = jnp.concatenate([peak[:, :wide], peak_own], axis=1)
        e = jnp.exp2((s - peak) * exp2_scale)
        e_own = jnp.exp2((s_own - peak_own) * exp2_scale)
        total = jnp.sum(e, axis=0, keepdims=True)
        total_own = total[:, wide:] + jnp.sum(e_own, axis=0, keepdims=True)
        inverse = 1.0 / jnp.concatenate([total[:, :wide], total_own], axis=1)
        p = e * inverse
        p_own = e_own * inverse[:, wide:]
        p_half = p.astype(jnp.bfloat16)
        p_half_own = p_own.astype(jnp.bfloat16)
        weighted = p * dot_nt(values, g)
        weighted_own = p_own * dot_nt(own_values, g[wide:])
        delta = jnp.sum(weighted, axis=0, keepdims=True)
        delta_own = delta[:, wide:] + jnp.sum(weighted_own, axis=0, keepdims=True)
        delta = jnp.concatenate([delta[:, :wide], delta_own], axis=1)
        ds = (weighted - p * delta).astype(jnp.bfloat16)
        ds_own = (weighted_own - p_own * delta_own).astype(jnp.bfloat16)
        dkv[:extent, :HEAD_DIM] += dot(ds, q)
        dkv[:extent, HEAD_DIM:] += dot(p_half, g)
        dn[:, :HEAD_DIM] += dot(ds_own, q[wide:])
        dn[:, HEAD_DIM:] += dot(p_half_own, g[wide:])
        dq = dot(kt[:, :extent], ds)
        dq_own = dq[:, wide:] + dot(knt[...], ds_own)
        for at, span in enumerate(spans):
            lanes = slice(at * rows, (at + 1) * rows)
            dq_ref[:rows, span] = (dq[:, lanes] * score_scale).T.astype(jnp.bfloat16)
            dq_ref[rows:, span] = (dq_own[:, lanes] * score_scale).T.astype(jnp.bfloat16)
        return carry

    turns = qg.shape[2] // HEAD_DIM // pack
    head_turns(0, turns // 2)

    @pl.when(me < n - 1)
    def _():
        pl.semaphore_wait(kv_credit, n - 1 - me)

    for peer in cross[::-1]:
        pl.when(peer > me)(cross_copy(1, peer).start)
    head_turns(turns // 2, turns)

    pair_scale = jnp.where(
        lax.broadcasted_iota(jnp.int32, (1, 2 * HEAD_DIM), 1) < HEAD_DIM, score_scale, 1.0
    )
    clean, noisy = pl.ds(0, rows), pl.ds(rows, rows)
    pga[me, noisy] = (dn[...] * pair_scale).astype(jnp.bfloat16)
    for block_at in range(n):
        pgp[block_at] = (dkv[block_at * rows : (block_at + 1) * rows] * pair_scale).astype(jnp.bfloat16)
    for at, (k, peer) in enumerate(far):
        if at == n - 2:
            for mate in mates:
                part = pga.at[me, noisy]
                put(part, part, pg_s.at[0], pn_r.at[mate_slot(me, mate)], context=mate)
        put_if(peer < me, pgp.at[peer], pin.at[me], pp_s.at[k - 1], pp_r.at[slot(me, peer)], context=peer)


    def clean_copy(peer):
        part = pga.at[me, clean]
        return copy_of(part, part, pg_s.at[1], pc_r.at[slot(me, peer)], context=peer)

    for peer in mates:
        pl.when((peer > me) & inner)(mate_copy(0, peer).start)
    put(pga.at[me, noisy], pgo.at[noisy], po_sem.at[0], po_sem.at[1], head=other)
    dkv[my_rows, :] *= pair_scale

    def cross_onward(src, part):
        held = tokd.at[src, cross_rows(head, part)]
        arrived(held, t1_r.at[part, lax.rem(src, half)])
        put(held, held, f1_s.at[part], f1_r.at[part, lax.rem(src, half)], head=other)

    def mate_held(src, core, part):
        return tokd.at[src, mate_rows(core, 0)] if part == 0 else tokn.at[src - base, mate_rows(core, 1)]

    def mate_onward(src, part):
        held = mate_held(src, head, part)
        arrived(held, t2_r.at[part, mate_slot(src, me)])
        put(held, held, f2_s.at[part], f2_r.at[part, mate_slot(src, me)], head=other)

    for src in mates:
        mate_onward(src, 1)
    for src in cross:
        cross_onward(src, 0)
    for k, peer in near:
        sent = copy_of(pgp.at[peer], pgp.at[peer], pp_s.at[k - 1], loc_sem.at[0], head=other)
        pl.when(peer < me)(sent.wait_send)
    for _, peer in near:

        @pl.when((peer > me) & (me > 0))
        def _(peer=peer):
            pl.semaphore_signal(sent_credit, inc=1, device_id={"context": peer}, device_id_type=MESH)

    foreign_side, foreign_columns = token_block(partner)
    gf = dot(pga[me, noisy].T, tokf[foreign_side, rows:, foreign_columns])
    for src in mates:
        arrived(mate_held(src, other, 1), f2_r.at[1, mate_slot(src, me)])
        arrived(pga.at[src, noisy], pn_r.at[mate_slot(src, me)])
        gf += dot(pga[src, noisy].T, tokn[src - base])
    slab = gf.shape[0] // m
    for at in range(m):
        gsum[at] = gf[at * slab : (at + 1) * slab]
        fp[at] = gf[at * slab : (at + 1) * slab].astype(jnp.bfloat16)
    foreign_own[...] = gsum[me_dp]
    for peer in dp_peers:
        put(fp.at[peer], fin.at[me_dp], rf_s.at[0], rf_r.at[dp_slot(me_dp, peer)], dp=peer)
    drain(fp.at[pl.ds(0, m - 1)], rf_s.at[0])
    for k, src in near:

        @pl.when(src > me)
        def _(src=src):
            arrived(pin.at[src], pp_r.at[slot(src, me)])
            dkv[my_rows, :] += pin[src].astype(jnp.float32)

    pga[me, clean] = dkv[my_rows, :].astype(jnp.bfloat16)
    for k, peer in far:
        pl.when(peer > me)(clean_copy(peer).start)

    @pl.when(me > 1)
    def _():
        pl.semaphore_wait(sent_credit, me - 1)

    for k, peer in far:
        pl.when((peer < me))(clean_copy(peer).start)


    put(pga.at[me, clean], pgo.at[clean], po_sem.at[0], po_sem.at[2], head=other)
    drain(pga.at[pl.ds(0, half - 1), noisy], pg_s.at[0])
    drain(pga.at[pl.ds(0, n - 1), clean], pg_s.at[1])
    drain(pga.at[me], po_sem.at[0])

    own_tokens.wait()
    for src in mates:
        mate_onward(src, 0)
    for src in cross:
        cross_onward(src, 1)
    gw = dot(pga[me].T, tokd[me])
    for src in mates:
        arrived(mate_held(src, other, 0), f2_r.at[0, mate_slot(src, me)])
        arrived(pga.at[src, clean], pc_r.at[slot(src, me)])
        gw += dot(pga[src].T, tokd[src])
    for src in cross:
        for part in range(2):
            arrived(tokd.at[src, cross_rows(other, part)], f1_r.at[part, lax.rem(src, half)])
        arrived(pga.at[src, clean], pc_r.at[slot(src, me)])
        gw += dot(pga[src, clean].T, tokd[src, clean])

    for at in range(m):
        gsum[at] = gw[at * slab : (at + 1) * slab]
        rp[at] = gw[at * slab : (at + 1) * slab].astype(jnp.bfloat16)
    parts = 2 if slab % 32 == 0 else 1

    def slab_part(part):
        return pl.ds(part * (slab // parts), slab // parts)

    for part in range(parts):
        span = slab_part(part)
        for peer in dp_peers:
            put(rp.at[peer, span], rin.at[me_dp, span], rs_s.at[0], rs_r.at[part, dp_slot(me_dp, peer)], dp=peer)
    drain(rp.at[pl.ds(0, m - 1)], rs_s.at[0])
    foreign_sum = foreign_own[...]
    for src in dp_peers:
        arrived(fin.at[src], rf_r.at[dp_slot(src, me_dp)])
        foreign_sum += fin[src].astype(jnp.float32)
    zout[...] = foreign_sum.astype(jnp.bfloat16)
    for part in range(parts):
        span = slab_part(part)
        put(zout.at[span], zin.at[span], z_sem.at[0], z_sem.at[1 + part], context=partner)
    drain(zout, z_sem.at[0])
    arrived(wo, wo_sem.at[1])
    arrived(pgo.at[noisy], po_sem.at[1])
    arrived(pgo.at[clean], po_sem.at[2])
    for at in range(half):
        gx_ref[:, at * wrows : (at + 1) * wrows] = (
            dot_nt(pga[me], wf[head * half + at]) + dot_nt(pgo[...], wo[at])
        ).astype(jnp.bfloat16)

    for part in range(parts):
        span = slab_part(part)
        slab_sum = gsum[me_dp, span]
        for src in dp_peers:
            arrived(rin.at[src, span], rs_r.at[part, dp_slot(src, me_dp)])
            slab_sum += rin[src, span].astype(jnp.float32)
        arrived(zin.at[span], z_sem.at[1 + part])
        slab_sum += zin[span].astype(jnp.float32)
        rall[me_dp, span] = slab_sum.astype(jnp.bfloat16)
        for peer in dp_peers:
            held = rall.at[me_dp, span]
            put(held, held, ra_s.at[0], ra_r.at[part, dp_slot(me_dp, peer)], dp=peer)
    drain(rall.at[pl.ds(0, m - 1)], ra_s.at[0])
    for part in range(parts):
        span = slab_part(part)
        for src in dp_peers:
            arrived(rall.at[src, span], ra_r.at[part, dp_slot(src, me_dp)])
    for at in range(m):
        gsum[at] = rall[at].astype(jnp.float32)
    gwk_ref[...] = gsum[: m // 2].reshape(HEAD_DIM, wrows).T
    gwv_ref[...] = gsum[m // 2 :].reshape(HEAD_DIM, wrows).T
    for condition, copy in drains:
        if condition is None:
            copy.wait_send()
        else:
            pl.when(condition)(copy.wait_send)


def store_kernel(dq_in, gx_in, gwk_in, gwv_in, dq_out, gx_out, gwk_out, gwv_out, sem):
    pairs = ((gx_in, gx_out), (dq_in, dq_out), (gwk_in, gwk_out), (gwv_in, gwv_out))
    copies = [pltpu.make_async_copy(src, dst, sem.at[at]) for at, (src, dst) in enumerate(pairs)]
    for copy in copies:
        copy.start()
    for copy in copies:
        copy.wait()


def per_device(tokens, queries, grad_out, w_key, w_value, block_len):
    n = lax.axis_size("context")
    m = lax.axis_size("dp")
    rows = tokens.shape[2]
    features = tokens.shape[3]
    wrows, width = w_key.shape
    q_width = queries.shape[3]
    share = wrows // m // 16 * 16
    direct_slots = n - 1 if wrows > m * share else 1
    half = n // 2
    pair = 2 * width
    bf16, f32 = jnp.bfloat16, jnp.float32
    vmem = pl.BlockSpec(memory_space=pltpu.VMEM)
    dma = pltpu.SemaphoreType.DMA
    heads = q_width // HEAD_DIM
    pack = math.gcd(heads, max(1, min(4, 2048 // (n * rows))))
    hbm = pl.BlockSpec(memory_space=pltpu.HBM)
    slab = pair // m
    results = (
        ((2 * rows, q_width), bf16),
        ((2 * rows, features), bf16),
        ((wrows, width), f32),
        ((wrows, width), f32),
    )
    dq, gx, gwk, gwv = pl.pallas_call(
        functools.partial(fused_kernel, n, m, share, pack),
        out_shape=tuple(pltpu.VMEM(*result) for result in results),
        in_specs=[pl.BlockSpec(memory_space=pltpu.SMEM)] + [hbm] * 5,
        out_specs=(vmem, vmem, vmem, vmem),
        scratch_shapes=[
            pltpu.VMEM((2, 2 * rows, q_width), bf16),
            pltpu.VMEM((2, 2 * rows, features), bf16),
            pltpu.VMEM((n, wrows, pair), bf16),
            pltpu.VMEM((half, wrows, pair), bf16),
            pltpu.VMEM((n * rows, pair), bf16),
            pltpu.VMEM((rows, pair), bf16),
            pltpu.VMEM((width, n * rows), bf16),
            pltpu.VMEM((width, rows), bf16),
            pltpu.VMEM((n * rows, pair), f32),
            pltpu.VMEM((rows, pair), f32),
            pltpu.VMEM((n, rows, pair), bf16),
            pltpu.VMEM((n, rows, pair), bf16),
            pltpu.VMEM((n, 2 * rows, pair), bf16),
            pltpu.VMEM((2 * rows, pair), bf16),
            pltpu.VMEM((n, 2 * rows, wrows), bf16),
            pltpu.VMEM((half, rows, wrows), bf16),
            pltpu.VMEM((m, slab, wrows), f32),
            pltpu.VMEM((m, slab, wrows), bf16),
            pltpu.VMEM((m, slab, wrows), bf16),
            pltpu.VMEM((m, slab, wrows), bf16),
            pltpu.VMEM((m, slab, wrows), bf16),
            pltpu.VMEM((m, slab, wrows), bf16),
            pltpu.VMEM((slab, wrows), f32),
            pltpu.VMEM((slab, wrows), bf16),
            pltpu.VMEM((slab, wrows), bf16),
            dma((4,)), pltpu.SemaphoreType.REGULAR, pltpu.SemaphoreType.REGULAR, pltpu.SemaphoreType.REGULAR, dma((2,)),
            dma((n + 1,)), dma((n - 1, 2)), dma((direct_slots,)), dma((direct_slots,)),
            dma((n - 1,)), dma((n - 1, max(6, m - 1))), dma((2,)), dma((n - 1,)), dma((n - 1,)),
            dma((2,)), dma((2, half)), dma((2,)), dma((2, half)),
            dma((2,)), dma((2, half - 1)), dma((2,)), dma((2, half - 1)), dma((n - 1,)), dma((n - 1,)),
            dma((2,)), dma((half - 1,)), dma((n - 1,)), dma((3,)),
            dma((1,)), dma((m - 1,)), dma((3,)), dma((1,)), dma((2, m - 1)), dma((1,)), dma((2, m - 1)),
        ],
        compiler_params=pltpu.CompilerParams(
            collective_id=0, has_side_effects=True, vmem_limit_bytes=VMEM_LIMIT
        ),
    )(
        block_len,
        tokens.reshape(2 * rows, features),
        queries.reshape(2 * rows, q_width),
        grad_out.reshape(2 * rows, q_width),
        w_key,
        w_value,
    )
    dq, gx, gwk, gwv = pl.pallas_call(
        store_kernel,
        out_shape=tuple(jax.ShapeDtypeStruct(*result) for result in results),
        in_specs=[vmem] * 4,
        out_specs=(hbm, hbm, hbm, hbm),
        scratch_shapes=[dma((4,))],
    )(*(pltpu.with_memory_space_constraint(x, pltpu.VMEM) for x in (dq, gx, gwk, gwv)))
    return (
        dq.reshape(queries.shape),
        gx.reshape(tokens.shape),
        gwk,
        gwv,
    )


def solution(mesh):
    placed = (
        P("dp", None, "context", "head"),
        P("dp", None, "context", "head"),
        P("dp", None, "context", "head"),
        P("context", "head"),
        P("context", "head"),
        P("dp"),
    )
    return jax.shard_map(
        per_device,
        mesh=mesh,
        in_specs=placed,
        out_specs=(
            P("dp", None, "context", "head"),
            P("dp", None, "context", "head"),
            P("context", "head"),
            P("context", "head"),
        ),
        check_vma=False,
    )
```

```python
import functools
import math

import jax
import jax.numpy as jnp
from jax import lax
from jax.experimental import pallas as pl
from jax.experimental.pallas import tpu as pltpu
from jax.sharding import PartitionSpec as P

HEAD_DIM = 128
MASKED = -1e30
VMEM_LIMIT = 56 * 1024 * 1024
MESH = pl.DeviceIdType.MESH
NT = (((1,), (1,)), ((), ()))


def line_order(me, n):
    low, high = me, n - 1 - me
    both = jnp.minimum(low, high)
    longer = jnp.where(low < high, 1, -1)
    order = []
    for k in range(1, n):
        near_side = 1 if k % 2 else -1
        peer = jnp.where(k <= 2 * both, me + near_side * ((k + 1) // 2), me + longer * (k - both))
        order.append((k, peer))
    return order


def dot(left, right):
    return jnp.dot(left, right, preferred_element_type=jnp.float32)


def dot_nt(left, right):
    return lax.dot_general(left, right, NT, preferred_element_type=jnp.float32)


def fused_kernel(
    n, m, share, pack,
    blk_ref, tok_ref, q_in, g_in, wk_ref, wv_ref,
    dq_ref, gx_ref, gwk_ref, gwv_ref,
    qg, tokf, wf, wo, kv, kvn, kt, knt, dkv, dn, pgp, pin, pga, pgo, tokd, tokn,
    gsum, rp, rin, rall, fp, fin, foreign_own, zout, zin,
    loc_sem, pair_sem, kv_credit, sent_credit, tok_sem, wz_s, wz_r, wd_s, wd_r, wx_s, wx_r, wo_sem, kv_s, kv_r,
    t1_s, t1_r, f1_s, f1_r, t2_s, t2_r, f2_s, f2_r, pp_s, pp_r, pg_s, pn_r, pc_r, po_sem,
    rf_s, rf_r, z_sem, rs_s, rs_r, ra_s, ra_r,
):
    me_dp = lax.axis_index("dp")
    me = lax.axis_index("context")
    head = lax.axis_index("head")
    other = 1 - head
    rows2, features = tok_ref.shape
    rows = rows2 // 2
    wrows = wk_ref.shape[0]
    half = n // 2
    score_scale = 1.0 / math.sqrt(HEAD_DIM)
    drains = []

    def copy_of(src, dst, send_sem, recv_sem, **device):
        return pltpu.make_async_remote_copy(
            src_ref=src, dst_ref=dst, send_sem=send_sem, recv_sem=recv_sem,
            device_id=device, device_id_type=MESH,
        )

    def put(src, dst, send_sem, recv_sem, **device):
        copy_of(src, dst, send_sem, recv_sem, **device).start()

    def put_if(condition, src, dst, send_sem, recv_sem, **device):
        pl.when(condition)(copy_of(src, dst, send_sem, recv_sem, **device).start)

    def arrived(dst, recv_sem):
        copy_of(dst, dst, loc_sem.at[0], recv_sem, head=other).wait_recv()

    def drain(whole, send_sem, condition=None):
        drains.append((condition, copy_of(whole, whole, send_sem, loc_sem.at[0], head=other)))

    def slot(src, dst):
        return lax.rem(src - dst + n - 1, n)

    def inside(place):
        return (place >= 0) & (place < n)

    def dp_slot(src, dst):
        return lax.rem(src - dst + m - 1, m)

    near = line_order(me, n)
    far = near[::-1]
    sides = (me + 1, me - 1)
    ring_peers = [lax.rem(me_dp + off, m) for off in range(1, m)]
    dp_peers = [jnp.where(k < me_dp, k, k + 1) for k in range(m - 1)]
    if m == 4:
        dp_peers = [me_dp + 1 - 2 * lax.rem(me_dp, 2), lax.rem(me_dp + 2, 4), 3 - me_dp]

    two_step = m == 4 and share % 32 == 0
    if two_step:
        low = lax.rem(me_dp, 2)
        w_peers = [(0, me_dp + 1 - 2 * low), (1, lax.rem(me_dp + 2, 4))]
    else:
        w_peers = list(enumerate(ring_peers))

    w_copies = [
        pltpu.make_async_copy(wk_ref, wf.at[me, :, pl.ds(0, HEAD_DIM)], loc_sem.at[0]),
        pltpu.make_async_copy(wv_ref, wf.at[me, :, pl.ds(HEAD_DIM, HEAD_DIM)], loc_sem.at[0]),
    ]
    own_half = pltpu.make_async_copy(tok_ref, tokf.at[head], loc_sem.at[1])
    row_copies = [
        pltpu.make_async_copy(q_in, qg.at[0], loc_sem.at[2]),
        pltpu.make_async_copy(g_in, qg.at[1], loc_sem.at[2]),
    ]
    for copy in w_copies + [own_half] + row_copies:
        copy.start()
    barrier = pltpu.get_barrier_semaphore()
    for _, peer in near:
        pl.semaphore_signal(barrier, inc=1, device_id={"context": peer}, device_id_type=MESH)
    for peer in dp_peers:
        pl.semaphore_signal(barrier, inc=1, device_id={"dp": peer}, device_id_type=MESH)
    pl.semaphore_signal(barrier, inc=1, device_id={"head": other}, device_id_type=MESH)
    pl.semaphore_wait(barrier, n + m - 1)

    def cores_meet():
        pl.semaphore_signal(pair_sem, inc=1, device_id={"head": other}, device_id_type=MESH)
        pl.semaphore_wait(pair_sem, 1)

    shared_base = pl.multiple_of(me_dp * share, 16)
    chunks = 2 if two_step else 1
    piece_rows = share // chunks

    def w_piece(owner, base, chunk):
        return wf.at[owner, pl.ds(pl.multiple_of(base + chunk * piece_rows, 16), piece_rows)]

    direct_rows = wrows - m * share
    direct = pl.ds(m * share, direct_rows)
    pltpu.make_async_copy(wf.at[me], wf.at[me], loc_sem.at[0]).wait()
    share_rows = wf.at[0, pl.ds(0, share)]
    for chunk in range(chunks):
        part = w_piece(me, shared_base, chunk)
        for at, peer in enumerate(sides):
            put_if(inside(peer), part, part, wz_s.at[at], wz_r.at[slot(me, peer), chunk], context=peer)
    for at, peer in enumerate(sides):
        drain(share_rows, wz_s.at[at], inside(peer))
    own_half.wait()
    put(tokf.at[head], tokf.at[head], tok_sem.at[0], tok_sem.at[1], head=other)
    drain(tokf.at[head], tok_sem.at[0])
    if direct_rows:
        for k, peer in near:
            part = wf.at[me, direct]
            put(part, part, wd_s.at[k - 1], wd_r.at[slot(me, peer)], context=peer)
            drain(part, wd_s.at[k - 1])

    def token_block(owner):
        column = pl.multiple_of(lax.rem(owner, half) * wrows, 128)
        return owner // half, pl.ds(column, wrows)

    quarter = rows // 4
    base = me // half * half
    place = me - base
    mates = [base + lax.rem(place + k, half) for k in range(1, half)]
    cross = [jnp.where(me < half, half + k, half - 1 - k) for k in range(half)]
    partner = lax.rem(me + half, n)
    outer = (me == 0) | (me == n - 1)
    inner = (me > 0) & (me < n - 1)

    def mate_slot(src, dst):
        return lax.rem(src - dst + half - 1, half)

    def cross_rows(core, part):
        return pl.ds(pl.multiple_of(core * 2 * quarter + part * quarter, 16), quarter)

    def mate_rows(core, part):
        if part < 2:
            return pl.ds(pl.multiple_of(core * rows + part * 2 * quarter, 16), 2 * quarter)
        return pl.ds(pl.multiple_of(core * 2 * quarter, 16), 2 * quarter)

    def cross_copy(part, peer):
        span = cross_rows(head, part)
        side, columns = token_block(peer)
        return copy_of(
            tokf.at[side, span, columns], tokd.at[me, span],
            t1_s.at[part], t1_r.at[part, lax.rem(me, half)], context=peer,
        )

    def mate_copy(part, peer):
        if part < 2:
            side, columns = token_block(peer)
            span = mate_rows(head, part)
            held = tokd.at[me, span]
        else:
            side, columns = token_block(lax.rem(peer + half, n))
            span = pl.ds(pl.multiple_of(rows + head * 2 * quarter, 16), 2 * quarter)
            held = tokn.at[place, mate_rows(head, 2)]
        return copy_of(
            tokf.at[side, span, columns], held,
            t2_s.at[part], t2_r.at[part, mate_slot(me, peer)], context=peer,
        )

    my_side, my_columns = token_block(me)

    def w_forward(src):
        for dp_at, peer in w_peers:
            part = w_piece(src, peer * share, dp_at)
            arrived(part, wx_r.at[slot(src, me), 2 * dp_at + dp_at])
            to = w_peers[1 - dp_at][1]
            put(part, part, wx_s.at[slot(src, me)], wx_r.at[slot(src, me), 4 + dp_at], dp=to)

    for k, src in near:
        onward = jnp.where(src > me, me - 1, me + 1)
        for chunk in range(chunks):
            part = w_piece(src, shared_base, chunk)
            arrived(part, wz_r.at[slot(src, me), chunk])
            put_if(inside(onward), part, part, wz_s.at[1 + k], wz_r.at[slot(src, onward), chunk], context=onward)
            for dp_at, peer in w_peers:
                put(part, part, wx_s.at[slot(src, me)], wx_r.at[slot(src, me), chunks * dp_at + chunk], dp=peer)
        drain(share_rows, wz_s.at[1 + k], inside(onward))
        drain(wf.at[0, pl.ds(0, (m - 1) * share)], wx_s.at[slot(src, me)])
        if k == 1:
            arrived(tokf.at[other], tok_sem.at[1])
            for peer in mates:
                for part in range(3):
                    pl.when(outer)(mate_copy(part, peer).start)
        if two_step and k > 1:
            w_forward(near[k - 2][1])
    cores_meet()
    for peer in cross[::-1]:
        cross_copy(0, peer).start()
    for peer in cross[::-1]:
        pl.when(peer < me)(cross_copy(1, peer).start)
    for peer in mates:
        pl.when(inner)(mate_copy(2, peer).start)
        for part in range(2):
            pl.when((peer < me) & inner)(mate_copy(part, peer).start)
    own_tokens = pltpu.make_async_copy(tokf.at[my_side, :, my_columns], tokd.at[me], loc_sem.at[3])
    own_tokens.start()
    for part in range(2):
        held = tokd.at[pl.ds(0, half), pl.ds(0, quarter)]
        drain(held, t1_s.at[part])
        drain(held, f1_s.at[part])
    for part in range(3):
        held = tokn.at[pl.ds(0, half - 1), pl.ds(0, 2 * quarter)]
        drain(held, t2_s.at[part])
        drain(held, f2_s.at[part])
    if two_step:
        w_forward(near[-1][1])

    projected = dot(tokf[my_side, :, my_columns], wf[me])
    for k, src in near:
        if direct_rows:
            arrived(wf.at[src, direct], wd_r.at[slot(src, me)])
        if two_step:
            for dp_at, peer in w_peers:
                part = w_piece(src, peer * share, 1 - dp_at)
                arrived(part, wx_r.at[slot(src, me), 2 * dp_at + 1 - dp_at])
                part = w_piece(src, (3 - me_dp) * share, dp_at)
                arrived(part, wx_r.at[slot(src, me), 4 + dp_at])
        else:
            for off in range(1, m):
                part = w_piece(src, lax.rem(me_dp + m - off, m) * share, 0)
                arrived(part, wx_r.at[slot(src, me), off - 1])
        side, columns = token_block(src)
        projected += dot(tokf[side, :, columns], wf[src])
    pairs = projected.astype(jnp.bfloat16)
    my_rows = pl.ds(pl.multiple_of(me * rows, rows), rows)
    kv[my_rows, :] = pairs[:rows]
    kvn[...] = pairs[rows:]
    for k, peer in far:
        put_if(peer > me, kv.at[my_rows], kv.at[my_rows], kv_s.at[k - 1], kv_r.at[slot(me, peer)], context=peer)
        drain(kv.at[my_rows], kv_s.at[k - 1], peer > me)
    put(wf.at[pl.ds(other * half, half)], wo, wo_sem.at[0], wo_sem.at[1], head=other)
    drain(wo, wo_sem.at[0])

    block = blk_ref[0]
    total_rows = n * rows
    lane = lax.broadcasted_iota(jnp.int32, (1, pack * rows2), 1)
    noisy_lane = lane >= pack * rows
    position = me * rows + lane % rows
    block_start = position & (-block)
    limit = jnp.where(noisy_lane, block_start, block_start + block)
    dkv[...] = jnp.zeros_like(dkv)
    dn[...] = jnp.zeros_like(dn)
    knt[...] = kvn[:, :HEAD_DIM].T
    pltpu.make_async_copy(qg, qg, loc_sem.at[2]).wait()
    for k, src in near:
        span = pl.ds(pl.multiple_of(src * rows, rows), rows)

        @pl.when(src < me)
        def _(span=span, src=src):
            arrived(kv.at[span], kv_r.at[slot(src, me)])

        @pl.when(src > me)
        def _(span=span):
            kv[span, :] = jnp.zeros((rows, 2 * HEAD_DIM), jnp.bfloat16)
    for _, peer in near:

        @pl.when(peer < me)
        def _(peer=peer):
            pl.semaphore_signal(kv_credit, inc=1, device_id={"context": peer}, device_id_type=MESH)

    for peer in mates:
        pl.when((peer > me) & inner)(mate_copy(0, peer).start)
    kt[...] = kv[:, :HEAD_DIM].T

    steps = 4 if n % 4 == 0 else 1
    step_rows = total_rows // steps

    def head_turns(first, last):
        for step in range(steps):

            @pl.when(me // (n // steps) == step)
            def _(step=step):
                turn_of = functools.partial(head_turn, (step + 1) * step_rows)
                lax.fori_loop(first, last, turn_of, 0)

    wide = pack * rows
    exp2_scale = score_scale * math.log2(math.e)

    def head_turn(extent, turn, carry):
        open_rows = extent - step_rows
        spans = [
            pl.ds(pl.multiple_of((turn * pack + at) * HEAD_DIM, HEAD_DIM), HEAD_DIM) for at in range(pack)
        ]

        def stacked(which):
            held = [qg[which, :, span] for span in spans]
            return jnp.concatenate([x[:rows] for x in held] + [x[rows:] for x in held], axis=0)

        q = stacked(0)
        g = stacked(1)
        keys = kv[:extent, :HEAD_DIM]
        values = kv[:extent, HEAD_DIM:]
        own_keys = kvn[:, :HEAD_DIM]
        own_values = kvn[:, HEAD_DIM:]
        key_pos = open_rows + lax.broadcasted_iota(jnp.int32, (step_rows, 2 * wide), 0)
        near_key = lax.broadcasted_iota(jnp.int32, (rows, wide), 0)
        near_row = lax.broadcasted_iota(jnp.int32, (rows, wide), 1) % rows
        same = (near_key ^ near_row) < block
        s = dot_nt(keys, q)
        s_edge = jnp.where(key_pos < limit, s[open_rows:], MASKED)
        s = jnp.concatenate([s[:open_rows], s_edge], axis=0) if open_rows else s_edge
        s_own = jnp.where(same, dot_nt(own_keys, q[wide:]), MASKED)
        peak = jnp.max(s, axis=0, keepdims=True)
        peak_own = jnp.maximum(peak[:, wide:], jnp.max(s_own, axis=0, keepdims=True))
        peak = jnp.concatenate([peak[:, :wide], peak_own], axis=1)
        e = jnp.exp2((s - peak) * exp2_scale)
        e_own = jnp.exp2((s_own - peak_own) * exp2_scale)
        total = jnp.sum(e, axis=0, keepdims=True)
        total_own = total[:, wide:] + jnp.sum(e_own, axis=0, keepdims=True)
        inverse = 1.0 / jnp.concatenate([total[:, :wide], total_own], axis=1)
        p = e * inverse
        p_own = e_own * inverse[:, wide:]
        p_half = p.astype(jnp.bfloat16)
        p_half_own = p_own.astype(jnp.bfloat16)
        weighted = p * dot_nt(values, g)
        weighted_own = p_own * dot_nt(own_values, g[wide:])
        delta = jnp.sum(weighted, axis=0, keepdims=True)
        delta_own = delta[:, wide:] + jnp.sum(weighted_own, axis=0, keepdims=True)
        delta = jnp.concatenate([delta[:, :wide], delta_own], axis=1)
        ds = (weighted - p * delta).astype(jnp.bfloat16)
        ds_own = (weighted_own - p_own * delta_own).astype(jnp.bfloat16)
        dkv[:extent, :HEAD_DIM] += dot(ds, q)
        dkv[:extent, HEAD_DIM:] += dot(p_half, g)
        dn[:, :HEAD_DIM] += dot(ds_own, q[wide:])
        dn[:, HEAD_DIM:] += dot(p_half_own, g[wide:])
        dq = dot(kt[:, :extent], ds)
        dq_own = dq[:, wide:] + dot(knt[...], ds_own)
        for at, span in enumerate(spans):
            lanes = slice(at * rows, (at + 1) * rows)
            dq_ref[:rows, span] = (dq[:, lanes] * score_scale).T.astype(jnp.bfloat16)
            dq_ref[rows:, span] = (dq_own[:, lanes] * score_scale).T.astype(jnp.bfloat16)
        return carry

    turns = qg.shape[2] // HEAD_DIM // pack
    head_turns(0, turns // 2)

    @pl.when(me < n - 1)
    def _():
        pl.semaphore_wait(kv_credit, n - 1 - me)

    for peer in cross[::-1]:
        pl.when(peer > me)(cross_copy(1, peer).start)
    head_turns(turns // 2, turns)

    pair_scale = jnp.where(
        lax.broadcasted_iota(jnp.int32, (1, 2 * HEAD_DIM), 1) < HEAD_DIM, score_scale, 1.0
    )
    clean, noisy = pl.ds(0, rows), pl.ds(rows, rows)
    pga[me, noisy] = (dn[...] * pair_scale).astype(jnp.bfloat16)
    for block_at in range(n):
        pgp[block_at] = (dkv[block_at * rows : (block_at + 1) * rows] * pair_scale).astype(jnp.bfloat16)
    for at, (k, peer) in enumerate(far):
        if at == n - 2:
            for mate in mates:
                part = pga.at[me, noisy]
                put(part, part, pg_s.at[0], pn_r.at[mate_slot(me, mate)], context=mate)
        put_if(peer < me, pgp.at[peer], pin.at[me], pp_s.at[k - 1], pp_r.at[slot(me, peer)], context=peer)


    def clean_copy(peer):
        part = pga.at[me, clean]
        return copy_of(part, part, pg_s.at[1], pc_r.at[slot(me, peer)], context=peer)

    for peer in mates:
        pl.when((peer > me) & inner)(mate_copy(1, peer).start)
    put(pga.at[me, noisy], pgo.at[noisy], po_sem.at[0], po_sem.at[1], head=other)
    dkv[my_rows, :] *= pair_scale

    def cross_onward(src, part):
        held = tokd.at[src, cross_rows(head, part)]
        arrived(held, t1_r.at[part, lax.rem(src, half)])
        put(held, held, f1_s.at[part], f1_r.at[part, lax.rem(src, half)], head=other)

    def mate_held(src, core, part):
        return tokd.at[src, mate_rows(core, part)] if part < 2 else tokn.at[src - base, mate_rows(core, 2)]

    def mate_onward(src, part):
        held = mate_held(src, head, part)
        arrived(held, t2_r.at[part, mate_slot(src, me)])
        put(held, held, f2_s.at[part], f2_r.at[part, mate_slot(src, me)], head=other)

    for src in mates:
        mate_onward(src, 2)
    for src in cross:
        cross_onward(src, 0)
    def own_clean():
        for k, src in near:

            @pl.when(src > me)
            def _(src=src):
                arrived(pin.at[src], pp_r.at[slot(src, me)])
                dkv[my_rows, :] += pin[src].astype(jnp.float32)

        pga[me, clean] = dkv[my_rows, :].astype(jnp.bfloat16)
        for k, peer in far:
            pl.when(peer > me)(clean_copy(peer).start)

    pl.when(me == 0)(own_clean)
    for k, peer in near:
        sent = copy_of(pgp.at[peer], pgp.at[peer], pp_s.at[k - 1], loc_sem.at[0], head=other)
        pl.when((peer < me) & (me < n - 1))(sent.wait_send)
        drain(pgp.at[peer], pp_s.at[k - 1], (peer < me) & (me == n - 1))
    for _, peer in near:

        @pl.when((peer > me) & (me > 0))
        def _(peer=peer):
            pl.semaphore_signal(sent_credit, inc=1, device_id={"context": peer}, device_id_type=MESH)

    foreign_side, foreign_columns = token_block(partner)
    gf = dot(pga[me, noisy].T, tokf[foreign_side, rows:, foreign_columns])
    for src in mates:
        arrived(mate_held(src, other, 2), f2_r.at[2, mate_slot(src, me)])
        arrived(pga.at[src, noisy], pn_r.at[mate_slot(src, me)])
        gf += dot(pga[src, noisy].T, tokn[src - base])
    slab = gf.shape[0] // m
    for at in range(m):
        gsum[at] = gf[at * slab : (at + 1) * slab]
        fp[at] = gf[at * slab : (at + 1) * slab].astype(jnp.bfloat16)
    foreign_own[...] = gsum[me_dp]
    for peer in dp_peers:
        put(fp.at[peer], fin.at[me_dp], rf_s.at[0], rf_r.at[dp_slot(me_dp, peer)], dp=peer)
    drain(fp.at[pl.ds(0, m - 1)], rf_s.at[0])
    pl.when(me > 0)(own_clean)

    @pl.when(me > 1)
    def _():
        pl.semaphore_wait(sent_credit, me - 1)

    for k, peer in far:
        pl.when((peer < me))(clean_copy(peer).start)


    put(pga.at[me, clean], pgo.at[clean], po_sem.at[0], po_sem.at[2], head=other)
    drain(pga.at[pl.ds(0, half - 1), noisy], pg_s.at[0])
    drain(pga.at[pl.ds(0, n - 1), clean], pg_s.at[1])
    drain(pga.at[me], po_sem.at[0])

    own_tokens.wait()
    for src in mates:
        for part in range(2):
            mate_onward(src, part)
    for src in cross:
        cross_onward(src, 1)
    gw = dot(pga[me].T, tokd[me])
    for src in mates:
        for part in range(2):
            arrived(mate_held(src, other, part), f2_r.at[part, mate_slot(src, me)])
        arrived(pga.at[src, clean], pc_r.at[slot(src, me)])
        gw += dot(pga[src].T, tokd[src])
    for src in cross:
        for part in range(2):
            arrived(tokd.at[src, cross_rows(other, part)], f1_r.at[part, lax.rem(src, half)])
        arrived(pga.at[src, clean], pc_r.at[slot(src, me)])
        gw += dot(pga[src, clean].T, tokd[src, clean])

    for at in range(m):
        gsum[at] = gw[at * slab : (at + 1) * slab]
        rp[at] = gw[at * slab : (at + 1) * slab].astype(jnp.bfloat16)
    parts = 2 if slab % 32 == 0 else 1

    def slab_part(part):
        return pl.ds(part * (slab // parts), slab // parts)

    for part in range(parts):
        span = slab_part(part)
        for peer in dp_peers:
            put(rp.at[peer, span], rin.at[me_dp, span], rs_s.at[0], rs_r.at[part, dp_slot(me_dp, peer)], dp=peer)
    drain(rp.at[pl.ds(0, m - 1)], rs_s.at[0])
    foreign_sum = foreign_own[...]
    for src in dp_peers:
        arrived(fin.at[src], rf_r.at[dp_slot(src, me_dp)])
        foreign_sum += fin[src].astype(jnp.float32)
    zout[...] = foreign_sum.astype(jnp.bfloat16)
    for part in range(parts):
        span = slab_part(part)
        put(zout.at[span], zin.at[span], z_sem.at[0], z_sem.at[1 + part], context=partner)
    drain(zout, z_sem.at[0])
    arrived(wo, wo_sem.at[1])
    arrived(pgo.at[noisy], po_sem.at[1])
    arrived(pgo.at[clean], po_sem.at[2])
    for at in range(half):
        gx_ref[:, at * wrows : (at + 1) * wrows] = (
            dot_nt(pga[me], wf[head * half + at]) + dot_nt(pgo[...], wo[at])
        ).astype(jnp.bfloat16)

    for part in range(parts):
        span = slab_part(part)
        slab_sum = gsum[me_dp, span]
        for src in dp_peers:
            arrived(rin.at[src, span], rs_r.at[part, dp_slot(src, me_dp)])
            slab_sum += rin[src, span].astype(jnp.float32)
        arrived(zin.at[span], z_sem.at[1 + part])
        slab_sum += zin[span].astype(jnp.float32)
        rall[me_dp, span] = slab_sum.astype(jnp.bfloat16)
        for peer in dp_peers:
            held = rall.at[me_dp, span]
            put(held, held, ra_s.at[0], ra_r.at[part, dp_slot(me_dp, peer)], dp=peer)
    drain(rall.at[pl.ds(0, m - 1)], ra_s.at[0])
    for part in range(parts):
        span = slab_part(part)
        for src in dp_peers:
            arrived(rall.at[src, span], ra_r.at[part, dp_slot(src, me_dp)])
    for at in range(m):
        gsum[at] = rall[at].astype(jnp.float32)
    gwk_ref[...] = gsum[: m // 2].reshape(HEAD_DIM, wrows).T
    gwv_ref[...] = gsum[m // 2 :].reshape(HEAD_DIM, wrows).T
    for condition, copy in drains:
        if condition is None:
            copy.wait_send()
        else:
            pl.when(condition)(copy.wait_send)


def store_kernel(dq_in, gx_in, gwk_in, gwv_in, dq_out, gx_out, gwk_out, gwv_out, sem):
    pairs = ((gx_in, gx_out), (dq_in, dq_out), (gwk_in, gwk_out), (gwv_in, gwv_out))
    copies = [pltpu.make_async_copy(src, dst, sem.at[at]) for at, (src, dst) in enumerate(pairs)]
    for copy in copies:
        copy.start()
    for copy in copies:
        copy.wait()


def per_device(tokens, queries, grad_out, w_key, w_value, block_len):
    n = lax.axis_size("context")
    m = lax.axis_size("dp")
    rows = tokens.shape[2]
    features = tokens.shape[3]
    wrows, width = w_key.shape
    q_width = queries.shape[3]
    share = wrows // m // 16 * 16
    direct_slots = n - 1 if wrows > m * share else 1
    half = n // 2
    pair = 2 * width
    bf16, f32 = jnp.bfloat16, jnp.float32
    vmem = pl.BlockSpec(memory_space=pltpu.VMEM)
    dma = pltpu.SemaphoreType.DMA
    heads = q_width // HEAD_DIM
    pack = math.gcd(heads, max(1, min(4, 2048 // (n * rows))))
    hbm = pl.BlockSpec(memory_space=pltpu.HBM)
    slab = pair // m
    results = (
        ((2 * rows, q_width), bf16),
        ((2 * rows, features), bf16),
        ((wrows, width), f32),
        ((wrows, width), f32),
    )
    dq, gx, gwk, gwv = pl.pallas_call(
        functools.partial(fused_kernel, n, m, share, pack),
        out_shape=tuple(pltpu.VMEM(*result) for result in results),
        in_specs=[pl.BlockSpec(memory_space=pltpu.SMEM)] + [hbm] * 5,
        out_specs=(vmem, vmem, vmem, vmem),
        scratch_shapes=[
            pltpu.VMEM((2, 2 * rows, q_width), bf16),
            pltpu.VMEM((2, 2 * rows, features), bf16),
            pltpu.VMEM((n, wrows, pair), bf16),
            pltpu.VMEM((half, wrows, pair), bf16),
            pltpu.VMEM((n * rows, pair), bf16),
            pltpu.VMEM((rows, pair), bf16),
            pltpu.VMEM((width, n * rows), bf16),
            pltpu.VMEM((width, rows), bf16),
            pltpu.VMEM((n * rows, pair), f32),
            pltpu.VMEM((rows, pair), f32),
            pltpu.VMEM((n, rows, pair), bf16),
            pltpu.VMEM((n, rows, pair), bf16),
            pltpu.VMEM((n, 2 * rows, pair), bf16),
            pltpu.VMEM((2 * rows, pair), bf16),
            pltpu.VMEM((n, 2 * rows, wrows), bf16),
            pltpu.VMEM((half, rows, wrows), bf16),
            pltpu.VMEM((m, slab, wrows), f32),
            pltpu.VMEM((m, slab, wrows), bf16),
            pltpu.VMEM((m, slab, wrows), bf16),
            pltpu.VMEM((m, slab, wrows), bf16),
            pltpu.VMEM((m, slab, wrows), bf16),
            pltpu.VMEM((m, slab, wrows), bf16),
            pltpu.VMEM((slab, wrows), f32),
            pltpu.VMEM((slab, wrows), bf16),
            pltpu.VMEM((slab, wrows), bf16),
            dma((4,)), pltpu.SemaphoreType.REGULAR, pltpu.SemaphoreType.REGULAR, pltpu.SemaphoreType.REGULAR, dma((2,)),
            dma((n + 1,)), dma((n - 1, 2)), dma((direct_slots,)), dma((direct_slots,)),
            dma((n - 1,)), dma((n - 1, max(6, m - 1))), dma((2,)), dma((n - 1,)), dma((n - 1,)),
            dma((2,)), dma((2, half)), dma((2,)), dma((2, half)),
            dma((3,)), dma((3, half - 1)), dma((3,)), dma((3, half - 1)), dma((n - 1,)), dma((n - 1,)),
            dma((2,)), dma((half - 1,)), dma((n - 1,)), dma((3,)),
            dma((1,)), dma((m - 1,)), dma((3,)), dma((1,)), dma((2, m - 1)), dma((1,)), dma((2, m - 1)),
        ],
        compiler_params=pltpu.CompilerParams(
            collective_id=0, has_side_effects=True, vmem_limit_bytes=VMEM_LIMIT
        ),
    )(
        block_len,
        tokens.reshape(2 * rows, features),
        queries.reshape(2 * rows, q_width),
        grad_out.reshape(2 * rows, q_width),
        w_key,
        w_value,
    )
    dq, gx, gwk, gwv = pl.pallas_call(
        store_kernel,
        out_shape=tuple(jax.ShapeDtypeStruct(*result) for result in results),
        in_specs=[vmem] * 4,
        out_specs=(hbm, hbm, hbm, hbm),
        scratch_shapes=[dma((4,))],
    )(*(pltpu.with_memory_space_constraint(x, pltpu.VMEM) for x in (dq, gx, gwk, gwv)))
    return (
        dq.reshape(queries.shape),
        gx.reshape(tokens.shape),
        gwk,
        gwv,
    )


def solution(mesh):
    placed = (
        P("dp", None, "context", "head"),
        P("dp", None, "context", "head"),
        P("dp", None, "context", "head"),
        P("context", "head"),
        P("context", "head"),
        P("dp"),
    )
    return jax.shard_map(
        per_device,
        mesh=mesh,
        in_specs=placed,
        out_specs=(
            P("dp", None, "context", "head"),
            P("dp", None, "context", "head"),
            P("context", "head"),
            P("context", "head"),
        ),
        check_vma=False,
    )
```

```python
import functools
import math

import jax
import jax.numpy as jnp
from jax import lax
from jax.experimental import pallas as pl
from jax.experimental.pallas import tpu as pltpu
from jax.sharding import PartitionSpec as P

HEAD_DIM = 128
MASKED = -1e30
VMEM_LIMIT = 56 * 1024 * 1024
MESH = pl.DeviceIdType.MESH
NT = (((1,), (1,)), ((), ()))


def line_order(me, n):
    low, high = me, n - 1 - me
    both = jnp.minimum(low, high)
    longer = jnp.where(low < high, 1, -1)
    order = []
    for k in range(1, n):
        near_side = 1 if k % 2 else -1
        peer = jnp.where(k <= 2 * both, me + near_side * ((k + 1) // 2), me + longer * (k - both))
        order.append((k, peer))
    return order


def dot(left, right):
    return jnp.dot(left, right, preferred_element_type=jnp.float32)


def dot_nt(left, right):
    return lax.dot_general(left, right, NT, preferred_element_type=jnp.float32)


def fused_kernel(
    n, m, share, pack,
    blk_ref, tok_ref, q_in, g_in, wk_ref, wv_ref,
    dq_ref, gx_ref, gwk_ref, gwv_ref,
    qg, tokf, wf, wo, kv, kvn, kt, knt, dkv, dn, pgp, pin, pga, pgo, tokd, tokn,
    gsum, rp, rin, rall, fp, fin, foreign_own, zout, zin,
    loc_sem, pair_sem, kv_credit, sent_credit, tok_sem, wz_s, wz_r, wd_s, wd_r, wx_s, wx_r, wo_sem, kv_s, kv_r,
    t1_s, t1_r, f1_s, f1_r, t2_s, t2_r, f2_s, f2_r, pp_s, pp_r, pg_s, pn_r, pc_r, po_sem,
    rf_s, rf_r, z_sem, rs_s, rs_r, ra_s, ra_r,
):
    me_dp = lax.axis_index("dp")
    me = lax.axis_index("context")
    head = lax.axis_index("head")
    other = 1 - head
    rows2, features = tok_ref.shape
    rows = rows2 // 2
    wrows = wk_ref.shape[0]
    half = n // 2
    score_scale = 1.0 / math.sqrt(HEAD_DIM)
    drains = []

    def copy_of(src, dst, send_sem, recv_sem, **device):
        return pltpu.make_async_remote_copy(
            src_ref=src, dst_ref=dst, send_sem=send_sem, recv_sem=recv_sem,
            device_id=device, device_id_type=MESH,
        )

    def put(src, dst, send_sem, recv_sem, **device):
        copy_of(src, dst, send_sem, recv_sem, **device).start()

    def put_if(condition, src, dst, send_sem, recv_sem, **device):
        pl.when(condition)(copy_of(src, dst, send_sem, recv_sem, **device).start)

    def arrived(dst, recv_sem):
        copy_of(dst, dst, loc_sem.at[0], recv_sem, head=other).wait_recv()

    def drain(whole, send_sem, condition=None):
        drains.append((condition, copy_of(whole, whole, send_sem, loc_sem.at[0], head=other)))

    def slot(src, dst):
        return lax.rem(src - dst + n - 1, n)

    def inside(place):
        return (place >= 0) & (place < n)

    def dp_slot(src, dst):
        return lax.rem(src - dst + m - 1, m)

    near = line_order(me, n)
    far = near[::-1]
    sides = (me + 1, me - 1)
    ring_peers = [lax.rem(me_dp + off, m) for off in range(1, m)]
    dp_peers = [jnp.where(k < me_dp, k, k + 1) for k in range(m - 1)]
    if m == 4:
        dp_peers = [me_dp + 1 - 2 * lax.rem(me_dp, 2), lax.rem(me_dp + 2, 4), 3 - me_dp]

    two_step = m == 4 and share % 32 == 0
    if two_step:
        low = lax.rem(me_dp, 2)
        w_peers = [(0, me_dp + 1 - 2 * low), (1, lax.rem(me_dp + 2, 4))]
    else:
        w_peers = list(enumerate(ring_peers))

    w_copies = [
        pltpu.make_async_copy(wk_ref, wf.at[me, :, pl.ds(0, HEAD_DIM)], loc_sem.at[0]),
        pltpu.make_async_copy(wv_ref, wf.at[me, :, pl.ds(HEAD_DIM, HEAD_DIM)], loc_sem.at[0]),
    ]
    own_half = pltpu.make_async_copy(tok_ref, tokf.at[head], loc_sem.at[1])
    row_copies = [
        pltpu.make_async_copy(q_in, qg.at[0], loc_sem.at[2]),
        pltpu.make_async_copy(g_in, qg.at[1], loc_sem.at[2]),
    ]
    for copy in w_copies + [own_half] + row_copies:
        copy.start()
    barrier = pltpu.get_barrier_semaphore()
    for _, peer in near:
        pl.semaphore_signal(barrier, inc=1, device_id={"context": peer}, device_id_type=MESH)
    for peer in dp_peers:
        pl.semaphore_signal(barrier, inc=1, device_id={"dp": peer}, device_id_type=MESH)
    pl.semaphore_signal(barrier, inc=1, device_id={"head": other}, device_id_type=MESH)
    pl.semaphore_wait(barrier, n + m - 1)

    def cores_meet():
        pl.semaphore_signal(pair_sem, inc=1, device_id={"head": other}, device_id_type=MESH)
        pl.semaphore_wait(pair_sem, 1)

    shared_base = pl.multiple_of(me_dp * share, 16)
    chunks = 2 if two_step else 1
    piece_rows = share // chunks

    def w_piece(owner, base, chunk):
        return wf.at[owner, pl.ds(pl.multiple_of(base + chunk * piece_rows, 16), piece_rows)]

    direct_rows = wrows - m * share
    direct = pl.ds(m * share, direct_rows)
    pltpu.make_async_copy(wf.at[me], wf.at[me], loc_sem.at[0]).wait()
    share_rows = wf.at[0, pl.ds(0, share)]
    for chunk in range(chunks):
        part = w_piece(me, shared_base, chunk)
        for at, peer in enumerate(sides):
            put_if(inside(peer), part, part, wz_s.at[at], wz_r.at[slot(me, peer), chunk], context=peer)
    for at, peer in enumerate(sides):
        drain(share_rows, wz_s.at[at], inside(peer))
    own_half.wait()
    put(tokf.at[head], tokf.at[head], tok_sem.at[0], tok_sem.at[1], head=other)
    drain(tokf.at[head], tok_sem.at[0])
    if direct_rows:
        for k, peer in near:
            part = wf.at[me, direct]
            put(part, part, wd_s.at[k - 1], wd_r.at[slot(me, peer)], context=peer)
            drain(part, wd_s.at[k - 1])

    def token_block(owner):
        column = pl.multiple_of(lax.rem(owner, half) * wrows, 128)
        return owner // half, pl.ds(column, wrows)

    quarter = rows // 4
    base = me // half * half
    place = me - base
    mates = [base + lax.rem(place + k, half) for k in range(1, half)]
    cross = [jnp.where(me < half, half + k, half - 1 - k) for k in range(half)]
    partner = lax.rem(me + half, n)
    outer = (me == 0) | (me == n - 1)
    inner = (me > 0) & (me < n - 1)

    def mate_slot(src, dst):
        return lax.rem(src - dst + half - 1, half)

    def cross_rows(core, part):
        return pl.ds(pl.multiple_of(core * 2 * quarter + part * quarter, 16), quarter)

    def mate_rows(core, part):
        if part == 0:
            return pl.ds(pl.multiple_of(core * rows, 16), rows)
        return pl.ds(pl.multiple_of(core * 2 * quarter, 16), 2 * quarter)

    def cross_copy(part, peer):
        span = cross_rows(head, part)
        side, columns = token_block(peer)
        return copy_of(
            tokf.at[side, span, columns], tokd.at[me, span],
            t1_s.at[part], t1_r.at[part, lax.rem(me, half)], context=peer,
        )

    def mate_copy(part, peer):
        if part == 0:
            side, columns = token_block(peer)
            span = mate_rows(head, 0)
            held = tokd.at[me, span]
        else:
            side, columns = token_block(lax.rem(peer + half, n))
            span = pl.ds(pl.multiple_of(rows + head * 2 * quarter, 16), 2 * quarter)
            held = tokn.at[place, mate_rows(head, 1)]
        return copy_of(
            tokf.at[side, span, columns], held,
            t2_s.at[part], t2_r.at[part, mate_slot(me, peer)], context=peer,
        )

    my_side, my_columns = token_block(me)

    def w_forward(src):
        for dp_at, peer in w_peers:
            part = w_piece(src, peer * share, dp_at)
            arrived(part, wx_r.at[slot(src, me), 2 * dp_at + dp_at])
            to = w_peers[1 - dp_at][1]
            put(part, part, wx_s.at[slot(src, me)], wx_r.at[slot(src, me), 4 + dp_at], dp=to)

    for k, src in near:
        onward = jnp.where(src > me, me - 1, me + 1)
        for chunk in range(chunks):
            part = w_piece(src, shared_base, chunk)
            arrived(part, wz_r.at[slot(src, me), chunk])
            put_if(inside(onward), part, part, wz_s.at[1 + k], wz_r.at[slot(src, onward), chunk], context=onward)
            for dp_at, peer in w_peers:
                put(part, part, wx_s.at[slot(src, me)], wx_r.at[slot(src, me), chunks * dp_at + chunk], dp=peer)
        drain(share_rows, wz_s.at[1 + k], inside(onward))
        drain(wf.at[0, pl.ds(0, (m - 1) * share)], wx_s.at[slot(src, me)])
        if k == 1:
            arrived(tokf.at[other], tok_sem.at[1])
            for peer in mates:
                for part in range(2):
                    pl.when(outer)(mate_copy(part, peer).start)
        if two_step and k > 1:
            w_forward(near[k - 2][1])
    cores_meet()
    for peer in cross[::-1]:
        cross_copy(0, peer).start()
    for peer in cross[::-1]:
        pl.when(peer < me)(cross_copy(1, peer).start)
    for peer in mates:
        pl.when(inner)(mate_copy(1, peer).start)
        pl.when((peer < me) & inner)(mate_copy(0, peer).start)
    own_tokens = pltpu.make_async_copy(tokf.at[my_side, :, my_columns], tokd.at[me], loc_sem.at[3])
    own_tokens.start()
    for part in range(2):
        held = tokd.at[pl.ds(0, half), pl.ds(0, quarter)]
        drain(held, t1_s.at[part])
        drain(held, f1_s.at[part])
    for part, held in enumerate((tokd.at[pl.ds(0, half - 1), pl.ds(0, rows)], tokn.at[pl.ds(0, half - 1), pl.ds(0, 2 * quarter)])):
        drain(held, t2_s.at[part])
        drain(held, f2_s.at[part])
    if two_step:
        w_forward(near[-1][1])

    projected = dot(tokf[my_side, :, my_columns], wf[me])
    for k, src in near:
        if direct_rows:
            arrived(wf.at[src, direct], wd_r.at[slot(src, me)])
        if two_step:
            for dp_at, peer in w_peers:
                part = w_piece(src, peer * share, 1 - dp_at)
                arrived(part, wx_r.at[slot(src, me), 2 * dp_at + 1 - dp_at])
                part = w_piece(src, (3 - me_dp) * share, dp_at)
                arrived(part, wx_r.at[slot(src, me), 4 + dp_at])
        else:
            for off in range(1, m):
                part = w_piece(src, lax.rem(me_dp + m - off, m) * share, 0)
                arrived(part, wx_r.at[slot(src, me), off - 1])
        side, columns = token_block(src)
        projected += dot(tokf[side, :, columns], wf[src])
    pairs = projected.astype(jnp.bfloat16)
    my_rows = pl.ds(pl.multiple_of(me * rows, rows), rows)
    kv[my_rows, :] = pairs[:rows]
    kvn[...] = pairs[rows:]
    for k, peer in far:
        put_if(peer > me, kv.at[my_rows], kv.at[my_rows], kv_s.at[k - 1], kv_r.at[slot(me, peer)], context=peer)
        drain(kv.at[my_rows], kv_s.at[k - 1], peer > me)
    put(wf.at[pl.ds(other * half, half)], wo, wo_sem.at[0], wo_sem.at[1], head=other)
    drain(wo, wo_sem.at[0])

    block = blk_ref[0]
    total_rows = n * rows
    lane = lax.broadcasted_iota(jnp.int32, (1, pack * rows2), 1)
    noisy_lane = lane >= pack * rows
    position = me * rows + lane % rows
    block_start = position & (-block)
    limit = jnp.where(noisy_lane, block_start, block_start + block)
    dkv[...] = jnp.zeros_like(dkv)
    dn[...] = jnp.zeros_like(dn)
    knt[...] = kvn[:, :HEAD_DIM].T
    pltpu.make_async_copy(qg, qg, loc_sem.at[2]).wait()
    for k, src in near:
        span = pl.ds(pl.multiple_of(src * rows, rows), rows)

        @pl.when(src < me)
        def _(span=span, src=src):
            arrived(kv.at[span], kv_r.at[slot(src, me)])

        @pl.when(src > me)
        def _(span=span):
            kv[span, :] = jnp.zeros((rows, 2 * HEAD_DIM), jnp.bfloat16)
    for _, peer in near:

        @pl.when(peer < me)
        def _(peer=peer):
            pl.semaphore_signal(kv_credit, inc=1, device_id={"context": peer}, device_id_type=MESH)

    kt[...] = kv[:, :HEAD_DIM].T

    steps = 4 if n % 4 == 0 else 1
    step_rows = total_rows // steps

    def head_turns(first, last):
        for step in range(steps):

            @pl.when(me // (n // steps) == step)
            def _(step=step):
                turn_of = functools.partial(head_turn, (step + 1) * step_rows)
                lax.fori_loop(first, last, turn_of, 0)

    wide = pack * rows
    exp2_scale = score_scale * math.log2(math.e)

    def head_turn(extent, turn, carry):
        open_rows = extent - step_rows
        spans = [
            pl.ds(pl.multiple_of((turn * pack + at) * HEAD_DIM, HEAD_DIM), HEAD_DIM) for at in range(pack)
        ]

        def stacked(which):
            held = [qg[which, :, span] for span in spans]
            return jnp.concatenate([x[:rows] for x in held] + [x[rows:] for x in held], axis=0)

        q = stacked(0)
        g = stacked(1)
        keys = kv[:extent, :HEAD_DIM]
        values = kv[:extent, HEAD_DIM:]
        own_keys = kvn[:, :HEAD_DIM]
        own_values = kvn[:, HEAD_DIM:]
        key_pos = open_rows + lax.broadcasted_iota(jnp.int32, (step_rows, 2 * wide), 0)
        near_key = lax.broadcasted_iota(jnp.int32, (rows, wide), 0)
        near_row = lax.broadcasted_iota(jnp.int32, (rows, wide), 1) % rows
        same = (near_key ^ near_row) < block
        s = dot_nt(keys, q)
        s_edge = jnp.where(key_pos < limit, s[open_rows:], MASKED)
        s = jnp.concatenate([s[:open_rows], s_edge], axis=0) if open_rows else s_edge
        s_own = jnp.where(same, dot_nt(own_keys, q[wide:]), MASKED)
        peak = jnp.max(s, axis=0, keepdims=True)
        peak_own = jnp.maximum(peak[:, wide:], jnp.max(s_own, axis=0, keepdims=True))
        peak = jnp.concatenate([peak[:, :wide], peak_own], axis=1)
        e = jnp.exp2((s - peak) * exp2_scale)
        e_own = jnp.exp2((s_own - peak_own) * exp2_scale)
        total = jnp.sum(e, axis=0, keepdims=True)
        total_own = total[:, wide:] + jnp.sum(e_own, axis=0, keepdims=True)
        inverse = 1.0 / jnp.concatenate([total[:, :wide], total_own], axis=1)
        p = e * inverse
        p_own = e_own * inverse[:, wide:]
        p_half = p.astype(jnp.bfloat16)
        p_half_own = p_own.astype(jnp.bfloat16)
        weighted = p * dot_nt(values, g)
        weighted_own = p_own * dot_nt(own_values, g[wide:])
        delta = jnp.sum(weighted, axis=0, keepdims=True)
        delta_own = delta[:, wide:] + jnp.sum(weighted_own, axis=0, keepdims=True)
        delta = jnp.concatenate([delta[:, :wide], delta_own], axis=1)
        ds = (weighted - p * delta).astype(jnp.bfloat16)
        ds_own = (weighted_own - p_own * delta_own).astype(jnp.bfloat16)
        dkv[:extent, :HEAD_DIM] += dot(ds, q)
        dkv[:extent, HEAD_DIM:] += dot(p_half, g)
        dn[:, :HEAD_DIM] += dot(ds_own, q[wide:])
        dn[:, HEAD_DIM:] += dot(p_half_own, g[wide:])
        dq = dot(kt[:, :extent], ds)
        dq_own = dq[:, wide:] + dot(knt[...], ds_own)
        for at, span in enumerate(spans):
            lanes = slice(at * rows, (at + 1) * rows)
            dq_ref[:rows, span] = (dq[:, lanes] * score_scale).T.astype(jnp.bfloat16)
            dq_ref[rows:, span] = (dq_own[:, lanes] * score_scale).T.astype(jnp.bfloat16)
        return carry

    turns = qg.shape[2] // HEAD_DIM // pack
    head_turns(0, turns // 2)

    @pl.when(me < n - 1)
    def _():
        pl.semaphore_wait(kv_credit, n - 1 - me)

    for peer in cross[::-1]:
        pl.when(peer > me)(cross_copy(1, peer).start)
    head_turns(turns // 2, turns)

    pair_scale = jnp.where(
        lax.broadcasted_iota(jnp.int32, (1, 2 * HEAD_DIM), 1) < HEAD_DIM, score_scale, 1.0
    )
    clean, noisy = pl.ds(0, rows), pl.ds(rows, rows)
    pga[me, noisy] = (dn[...] * pair_scale).astype(jnp.bfloat16)
    for block_at in range(n):
        pgp[block_at] = (dkv[block_at * rows : (block_at + 1) * rows] * pair_scale).astype(jnp.bfloat16)
    for at, (k, peer) in enumerate(far):
        if at == n - 2:
            for mate in mates:
                part = pga.at[me, noisy]
                put(part, part, pg_s.at[0], pn_r.at[mate_slot(me, mate)], context=mate)
        put_if(peer < me, pgp.at[peer], pin.at[me], pp_s.at[k - 1], pp_r.at[slot(me, peer)], context=peer)


    def clean_copy(peer):
        part = pga.at[me, clean]
        return copy_of(part, part, pg_s.at[1], pc_r.at[slot(me, peer)], context=peer)

    for peer in mates:
        pl.when((peer > me) & inner)(mate_copy(0, peer).start)
    put(pga.at[me, noisy], pgo.at[noisy], po_sem.at[0], po_sem.at[1], head=other)
    dkv[my_rows, :] *= pair_scale

    def cross_onward(src, part):
        held = tokd.at[src, cross_rows(head, part)]
        arrived(held, t1_r.at[part, lax.rem(src, half)])
        put(held, held, f1_s.at[part], f1_r.at[part, lax.rem(src, half)], head=other)

    def mate_held(src, core, part):
        return tokd.at[src, mate_rows(core, 0)] if part == 0 else tokn.at[src - base, mate_rows(core, 1)]

    def mate_onward(src, part):
        held = mate_held(src, head, part)
        arrived(held, t2_r.at[part, mate_slot(src, me)])
        put(held, held, f2_s.at[part], f2_r.at[part, mate_slot(src, me)], head=other)

    for src in mates:
        mate_onward(src, 1)
    for src in cross:
        cross_onward(src, 0)
    for k, peer in near:
        sent = copy_of(pgp.at[peer], pgp.at[peer], pp_s.at[k - 1], loc_sem.at[0], head=other)
        pl.when(peer < me)(sent.wait_send)
    for _, peer in near:

        @pl.when((peer > me) & (me > 0))
        def _(peer=peer):
            pl.semaphore_signal(sent_credit, inc=1, device_id={"context": peer}, device_id_type=MESH)

    foreign_side, foreign_columns = token_block(partner)
    gf = dot(pga[me, noisy].T, tokf[foreign_side, rows:, foreign_columns])
    for src in mates:
        arrived(mate_held(src, other, 1), f2_r.at[1, mate_slot(src, me)])
        arrived(pga.at[src, noisy], pn_r.at[mate_slot(src, me)])
        gf += dot(pga[src, noisy].T, tokn[src - base])
    slab = gf.shape[0] // m
    for at in range(m):
        gsum[at] = gf[at * slab : (at + 1) * slab]
        fp[at] = gf[at * slab : (at + 1) * slab].astype(jnp.bfloat16)
    foreign_own[...] = gsum[me_dp]
    for peer in dp_peers:
        put(fp.at[peer], fin.at[me_dp], rf_s.at[0], rf_r.at[dp_slot(me_dp, peer)], dp=peer)
    drain(fp.at[pl.ds(0, m - 1)], rf_s.at[0])
    for k, src in near:

        @pl.when(src > me)
        def _(src=src):
            arrived(pin.at[src], pp_r.at[slot(src, me)])
            dkv[my_rows, :] += pin[src].astype(jnp.float32)

    pga[me, clean] = dkv[my_rows, :].astype(jnp.bfloat16)
    for k, peer in far:
        pl.when(peer > me)(clean_copy(peer).start)

    @pl.when(me > 1)
    def _():
        pl.semaphore_wait(sent_credit, me - 1)

    for k, peer in far:
        pl.when((peer < me))(clean_copy(peer).start)


    put(pga.at[me, clean], pgo.at[clean], po_sem.at[0], po_sem.at[2], head=other)
    drain(pga.at[pl.ds(0, half - 1), noisy], pg_s.at[0])
    drain(pga.at[pl.ds(0, n - 1), clean], pg_s.at[1])
    drain(pga.at[me], po_sem.at[0])

    own_tokens.wait()
    for src in mates:
        mate_onward(src, 0)
    for src in cross:
        cross_onward(src, 1)
    gw = dot(pga[me].T, tokd[me])
    for src in mates:
        arrived(mate_held(src, other, 0), f2_r.at[0, mate_slot(src, me)])
        arrived(pga.at[src, clean], pc_r.at[slot(src, me)])
        gw += dot(pga[src].T, tokd[src])
    for src in cross:
        for part in range(2):
            arrived(tokd.at[src, cross_rows(other, part)], f1_r.at[part, lax.rem(src, half)])
        arrived(pga.at[src, clean], pc_r.at[slot(src, me)])
        gw += dot(pga[src, clean].T, tokd[src, clean])

    for at in range(m):
        gsum[at] = gw[at * slab : (at + 1) * slab]
        rp[at] = gw[at * slab : (at + 1) * slab].astype(jnp.bfloat16)
    parts = 2 if slab % 32 == 0 else 1

    def slab_part(part):
        return pl.ds(part * (slab // parts), slab // parts)

    for part in range(parts):
        span = slab_part(part)
        for peer in dp_peers:
            put(rp.at[peer, span], rin.at[me_dp, span], rs_s.at[0], rs_r.at[part, dp_slot(me_dp, peer)], dp=peer)
    drain(rp.at[pl.ds(0, m - 1)], rs_s.at[0])
    foreign_sum = foreign_own[...]
    for src in dp_peers:
        arrived(fin.at[src], rf_r.at[dp_slot(src, me_dp)])
        foreign_sum += fin[src].astype(jnp.float32)
    zout[...] = foreign_sum.astype(jnp.bfloat16)
    for part in range(parts):
        span = slab_part(part)
        put(zout.at[span], zin.at[span], z_sem.at[0], z_sem.at[1 + part], context=partner)
    drain(zout, z_sem.at[0])
    arrived(wo, wo_sem.at[1])
    arrived(pgo.at[noisy], po_sem.at[1])
    arrived(pgo.at[clean], po_sem.at[2])
    for at in range(half):
        gx_ref[:, at * wrows : (at + 1) * wrows] = (
            dot_nt(pga[me], wf[head * half + at]) + dot_nt(pgo[...], wo[at])
        ).astype(jnp.bfloat16)

    for part in range(parts):
        span = slab_part(part)
        slab_sum = gsum[me_dp, span]
        for src in dp_peers:
            arrived(rin.at[src, span], rs_r.at[part, dp_slot(src, me_dp)])
            slab_sum += rin[src, span].astype(jnp.float32)
        arrived(zin.at[span], z_sem.at[1 + part])
        slab_sum += zin[span].astype(jnp.float32)
        rall[me_dp, span] = slab_sum.astype(jnp.bfloat16)
        for peer in dp_peers:
            held = rall.at[me_dp, span]
            put(held, held, ra_s.at[0], ra_r.at[part, dp_slot(me_dp, peer)], dp=peer)
    drain(rall.at[pl.ds(0, m - 1)], ra_s.at[0])
    for part in range(parts):
        span = slab_part(part)
        for src in dp_peers:
            arrived(rall.at[src, span], ra_r.at[part, dp_slot(src, me_dp)])
    for at in range(m):
        gsum[at] = rall[at].astype(jnp.float32)
    gwk_ref[...] = gsum[: m // 2].reshape(HEAD_DIM, wrows).T
    gwv_ref[...] = gsum[m // 2 :].reshape(HEAD_DIM, wrows).T
    for condition, copy in drains:
        if condition is None:
            copy.wait_send()
        else:
            pl.when(condition)(copy.wait_send)


def store_kernel(dq_in, gx_in, gwk_in, gwv_in, dq_out, gx_out, gwk_out, gwv_out, sem):
    pairs = ((gx_in, gx_out), (dq_in, dq_out), (gwk_in, gwk_out), (gwv_in, gwv_out))
    copies = [pltpu.make_async_copy(src, dst, sem.at[at]) for at, (src, dst) in enumerate(pairs)]
    for copy in copies:
        copy.start()
    for copy in copies:
        copy.wait()


def per_device(tokens, queries, grad_out, w_key, w_value, block_len):
    n = lax.axis_size("context")
    m = lax.axis_size("dp")
    rows = tokens.shape[2]
    features = tokens.shape[3]
    wrows, width = w_key.shape
    q_width = queries.shape[3]
    share = wrows // m // 16 * 16
    direct_slots = n - 1 if wrows > m * share else 1
    half = n // 2
    pair = 2 * width
    bf16, f32 = jnp.bfloat16, jnp.float32
    vmem = pl.BlockSpec(memory_space=pltpu.VMEM)
    dma = pltpu.SemaphoreType.DMA
    heads = q_width // HEAD_DIM
    pack = math.gcd(heads, max(1, min(4, 2048 // (n * rows))))
    hbm = pl.BlockSpec(memory_space=pltpu.HBM)
    slab = pair // m
    results = (
        ((2 * rows, q_width), bf16),
        ((2 * rows, features), bf16),
        ((wrows, width), f32),
        ((wrows, width), f32),
    )
    dq, gx, gwk, gwv = pl.pallas_call(
        functools.partial(fused_kernel, n, m, share, pack),
        out_shape=tuple(pltpu.VMEM(*result) for result in results),
        in_specs=[pl.BlockSpec(memory_space=pltpu.SMEM)] + [hbm] * 5,
        out_specs=(vmem, vmem, vmem, vmem),
        scratch_shapes=[
            pltpu.VMEM((2, 2 * rows, q_width), bf16),
            pltpu.VMEM((2, 2 * rows, features), bf16),
            pltpu.VMEM((n, wrows, pair), bf16),
            pltpu.VMEM((half, wrows, pair), bf16),
            pltpu.VMEM((n * rows, pair), bf16),
            pltpu.VMEM((rows, pair), bf16),
            pltpu.VMEM((width, n * rows), bf16),
            pltpu.VMEM((width, rows), bf16),
            pltpu.VMEM((n * rows, pair), f32),
            pltpu.VMEM((rows, pair), f32),
            pltpu.VMEM((n, rows, pair), bf16),
            pltpu.VMEM((n, rows, pair), bf16),
            pltpu.VMEM((n, 2 * rows, pair), bf16),
            pltpu.VMEM((2 * rows, pair), bf16),
            pltpu.VMEM((n, 2 * rows, wrows), bf16),
            pltpu.VMEM((half, rows, wrows), bf16),
            pltpu.VMEM((m, slab, wrows), f32),
            pltpu.VMEM((m, slab, wrows), bf16),
            pltpu.VMEM((m, slab, wrows), bf16),
            pltpu.VMEM((m, slab, wrows), bf16),
            pltpu.VMEM((m, slab, wrows), bf16),
            pltpu.VMEM((m, slab, wrows), bf16),
            pltpu.VMEM((slab, wrows), f32),
            pltpu.VMEM((slab, wrows), bf16),
            pltpu.VMEM((slab, wrows), bf16),
            dma((4,)), pltpu.SemaphoreType.REGULAR, pltpu.SemaphoreType.REGULAR, pltpu.SemaphoreType.REGULAR, dma((2,)),
            dma((n + 1,)), dma((n - 1, 2)), dma((direct_slots,)), dma((direct_slots,)),
            dma((n - 1,)), dma((n - 1, max(6, m - 1))), dma((2,)), dma((n - 1,)), dma((n - 1,)),
            dma((2,)), dma((2, half)), dma((2,)), dma((2, half)),
            dma((2,)), dma((2, half - 1)), dma((2,)), dma((2, half - 1)), dma((n - 1,)), dma((n - 1,)),
            dma((2,)), dma((half - 1,)), dma((n - 1,)), dma((3,)),
            dma((1,)), dma((m - 1,)), dma((3,)), dma((1,)), dma((2, m - 1)), dma((1,)), dma((2, m - 1)),
        ],
        compiler_params=pltpu.CompilerParams(
            collective_id=0, has_side_effects=True, vmem_limit_bytes=VMEM_LIMIT
        ),
    )(
        block_len,
        tokens.reshape(2 * rows, features),
        queries.reshape(2 * rows, q_width),
        grad_out.reshape(2 * rows, q_width),
        w_key,
        w_value,
    )
    dq, gx, gwk, gwv = pl.pallas_call(
        store_kernel,
        out_shape=tuple(jax.ShapeDtypeStruct(*result) for result in results),
        in_specs=[vmem] * 4,
        out_specs=(hbm, hbm, hbm, hbm),
        scratch_shapes=[dma((4,))],
    )(*(pltpu.with_memory_space_constraint(x, pltpu.VMEM) for x in (dq, gx, gwk, gwv)))
    return (
        dq.reshape(queries.shape),
        gx.reshape(tokens.shape),
        gwk,
        gwv,
    )


def solution(mesh):
    placed = (
        P("dp", None, "context", "head"),
        P("dp", None, "context", "head"),
        P("dp", None, "context", "head"),
        P("context", "head"),
        P("context", "head"),
        P("dp"),
    )
    return jax.shard_map(
        per_device,
        mesh=mesh,
        in_specs=placed,
        out_specs=(
            P("dp", None, "context", "head"),
            P("dp", None, "context", "head"),
            P("context", "head"),
            P("context", "head"),
        ),
        check_vma=False,
    )
```
